32 devices in a mesh: clu: 16 (over z, x, core), doc: 2 (over y).
Axes of the slice: x: 2, y: 2, z: 4, core: 2. Of those that a mesh axis runs over, the one named last changes fastest.
Arguments:
- docs: bfloat16 [8192, 768], P(('clu', 'doc')), may hold values from -6 to 6
- centroids: bfloat16 [5504, 768], P('doc', 'clu'), may hold values from -6 to 6
- assigned: int32 [8192], P(('clu', 'doc')), may hold values from 0 to 5503
Outputs:
- nearest: float32 [8192], P(('clu', 'doc'))
- assigned_dist: float32 [8192], P(('clu', 'doc'))
The draws below stay inside these ranges and needn't reach their ends.
Inputs may be any that keep to these rules, and one draw needn't show every extreme that they name: `assigned`: cluster ids.
All inputs are finite; a program needn't handle non-finite values.
Results may differ from the reference program's by a relative error of at most 0.0003.
Values may be sent and summed in bfloat16 or wider, within the bound.
A program may use at most 64 MiB of HBM per device.

```python
import jax
import jax.numpy as jnp
from jax import lax

D = 768
K = 5504
N = 8192
N_CLU = 16


def touch_ends(entries, stream_key, least, top_value):
    longest = entries.shape.index(max(entries.shape))
    spots = []
    for shift in (0, 1):
        where = [jax.random.randint(jax.random.fold_in(stream_key, axis), (), 0, length) for axis, length in enumerate(entries.shape)]
        where[longest] = (where[longest] + shift) % entries.shape[longest]
        spots.append(tuple(where))
    return entries.at[spots[0]].set(least).at[spots[1]].set(top_value)


def block_scale(key, dims, pieces, least, largest):
    def one(dim, blocks):
        steps = jax.random.uniform(jax.random.fold_in(jax.random.fold_in(key, 6), dim), (blocks,), jnp.float32, least / len(pieces), largest / len(pieces))
        return jnp.repeat(jnp.exp(steps), dims[dim] // blocks).reshape((-1,) + (1,) * (len(dims) - dim - 1))

    gain = one(*pieces[0])
    for cut in pieces[1:]:
        gain = gain * one(*cut)
    return gain


def centred(own_key, dims, spread, bound, shards=(), dtype=jnp.bfloat16):
    level = block_scale(own_key, dims, shards, -0.22, 0.18) if shards else 1.0
    values = jax.random.normal(own_key, dims, jnp.float32) * spread * level
    return jnp.minimum(jnp.maximum(values, -bound), bound).astype(dtype)


def setup_inputs(seed: int = 0) -> dict:
    splits = jax.random.split(jax.random.key(seed), 4)
    return {
        "docs": centred(splits[0], (N, D), 1.0, 6.0, ((0, 32),)),
        "centroids": centred(splits[1], (K, D), 1.0, 6.0, ((0, 2), (1, 16))),
        "assigned": touch_ends(jax.random.randint(splits[2], (N,), 0, K), jax.random.fold_in(splits[2], 1), 0, K - 1).astype(jnp.int32),
    }


epsilon = 1e-06

def reference(docs, centroids, assigned):
    cent_wide = centroids.astype(jnp.float32)
    scale_c = lax.rsqrt(lax.optimization_barrier(jnp.sum(cent_wide * cent_wide, 1)) + epsilon)
    features = docs.shape[1]

    def score_block(inputs):
        doc_rows, doc_ids = inputs
        row_wide = doc_rows.astype(jnp.float32)
        scale_x = lax.rsqrt(lax.optimization_barrier(jnp.sum(row_wide * row_wide, 1)) + epsilon)
        products = jnp.dot(doc_rows, centroids.T, preferred_element_type=jnp.float32)
        distance = 1.0 - products * scale_x[:, None] * scale_c[None, :]
        nearest = lax.optimization_barrier(jnp.min(distance, 1))
        chosen = jnp.take_along_axis(distance, doc_ids[:, None].astype(jnp.int32), axis=1)[:, 0]
        return (nearest, chosen)
    nearest, chosen = lax.map(score_block, (docs.reshape(N_CLU, -1, features), assigned.reshape(N_CLU, -1)))
    return (nearest.reshape(-1), chosen.reshape(-1))
```

```python
import functools

import jax
import jax.numpy as jnp
from jax import lax
from jax.experimental import pallas as pl
from jax.experimental.pallas import tpu as pltpu
from jax.sharding import PartitionSpec as P

epsilon = 1e-06
PIECES = 4
ROWS = 64
MESH = pl.DeviceIdType.MESH


def chip_at(pos, n):
    half = n // 2
    return jnp.where(pos < half, 2 * pos, 2 * (n - 1 - pos) + 1)


def cut(width):
    tiles = (width + 127) // 128
    ends = [min(-(-tiles * (c + 1) // PIECES) * 128, width) for c in range(PIECES)]
    return tuple((a, b - a) for a, b in zip([0] + ends[:-1], ends))


def kernel(n, nd, feat, docs_in, cents_in, ids_in, near_out, chosen_out,
           buf, docs_all, ids_all, dp_a, dp_b, dp_c, acc, idb, mx, ch, csq, scale, res, got,
           local_sem, ring_send, pair_send, recv, docs_send, docs_recv, ids_send, ids_recv,
           res_send, res_recv):
    hops = n // 2
    fp = cents_in.shape[0]
    width = cents_in.shape[1]
    rows_dev = docs_in.shape[0]
    chunks = cut(width)
    half = len(chunks) // 2

    clu, doc = lax.axis_index("clu"), lax.axis_index("doc")
    core, chip = lax.rem(clu, 2), lax.div(clu, 2)
    z, x = lax.div(chip, 2), lax.rem(chip, 2)
    pos = jnp.where(x == 0, z, n - 1 - z)
    right = chip_at(lax.rem(pos + 1, n), n) * 2 + core
    left = chip_at(lax.rem(pos + n - 1, n), n) * 2 + core
    partner = chip * 2 + (1 - core)

    own_c = pltpu.make_async_copy(cents_in, buf.at[pl.ds(0, fp), :], local_sem.at[0])
    own_d = pltpu.make_async_copy(docs_in, docs_all.at[0], local_sem.at[1])
    own_i = pltpu.make_async_copy(ids_in, ids_all.at[0], local_sem.at[2])
    own_c.start()
    own_d.start()
    own_i.start()

    barrier = pltpu.get_barrier_semaphore()
    for peer in (left, right, partner):
        pl.semaphore_signal(barrier, inc=1, device_id={"clu": peer}, device_id_type=MESH)
    for k in range(1, nd):
        pl.semaphore_signal(barrier, inc=1, device_id={"doc": lax.rem(doc + k, nd)}, device_id_type=MESH)
    pl.semaphore_wait(barrier, 3 + nd - 1)

    def slot(way, h):
        if h == 0:
            return 0
        if h == hops:
            return n - 1
        return 2 * h - 1 if way == 0 else 2 * h

    def piece(s, m, c):
        return buf.at[pl.ds((2 * s + m) * fp, fp), pl.ds(*chunks[c])]

    def reach(way, c):
        return hops if way == c // half else hops - 1

    sent = []

    def ring(way, h, c):
        s, t = slot(way, h), slot(way, h + 1)
        copy = pltpu.make_async_remote_copy(
            src_ref=piece(s, 0, c), dst_ref=piece(t, 0, c),
            send_sem=ring_send.at[way, h, c], recv_sem=recv.at[t, 0, c],
            device_id={"clu": right if way == 0 else left}, device_id_type=MESH)
        copy.start()
        sent.append(copy)

    def share(s, c):
        copy = pltpu.make_async_remote_copy(
            src_ref=piece(s, 0, c), dst_ref=piece(s, 1, c),
            send_sem=pair_send.at[s, c], recv_sem=recv.at[s, 1, c],
            device_id={"clu": partner}, device_id_type=MESH)
        copy.start()
        sent.append(copy)

    def landed(s, m, c):
        pltpu.make_async_remote_copy(
            src_ref=piece(s, m, c), dst_ref=piece(s, m, c),
            send_sem=pair_send.at[s, c], recv_sem=recv.at[s, m, c],
            device_id={"clu": partner}, device_id_type=MESH).wait_recv()

    own_c.wait()
    for i in range(PIECES):
        ring(0, 0, i)
        ring(1, 0, (i + half) % PIECES)
    for c in range(PIECES):
        share(0, c)
    own_d.wait()
    own_i.wait()
    doc_copies = []
    for k in range(1, nd):
        mate = lax.rem(doc + k, nd)
        for ref, ss, rs in ((ids_all, ids_send, ids_recv), (docs_all, docs_send, docs_recv)):
            copy = pltpu.make_async_remote_copy(
                src_ref=ref.at[0], dst_ref=ref.at[k], send_sem=ss.at[k], recv_sem=rs.at[k],
                device_id={"doc": mate}, device_id_type=MESH)
            copy.start()
            doc_copies.append(copy)

    def owner(s):
        if s == 0:
            p = pos
        elif s == n - 1:
            p = pos + hops
        elif s % 2:
            p = pos + n - (s + 1) // 2
        else:
            p = pos + s // 2
        return chip_at(lax.rem(p, n), n)

    ranges = ((0, n - 3), (n - 3, n - 1), (n - 1, n))
    spread = (dp_a, dp_b, dp_c)

    def permute(k):
        rows = docs_all[k]
        for (first, last), out in zip(ranges, spread):
            wide = out.shape[1]
            lane = lax.broadcasted_iota(jnp.int32, (1, wide), 1)
            target = jnp.full((1, wide), -1, jnp.int32)
            for s in range(first, last):
                chip_s = owner(s)
                for m in (0, 1):
                    part = chip_s * 2 + (core if m == 0 else 1 - core)
                    start = (2 * (s - first) + m) * fp
                    inside = (lane >= start) & (lane < start + feat)
                    target = jnp.where(inside, lane - start + part * feat, target)
            source = lax.broadcasted_iota(jnp.int32, (rows.shape[1], wide), 0)
            mover = jnp.where(source == target, 1.0, 0.0).astype(jnp.bfloat16)
            out[pl.ds(k * rows_dev, rows_dev), :] = jnp.dot(
                rows, mover, preferred_element_type=jnp.float32).astype(jnp.bfloat16)

    def prepare_ids(k):
        base = doc * width
        ids = ids_all[k] - base
        ids = jnp.where((ids >= 0) & (ids < width), ids, -1)
        full = jnp.broadcast_to(ids, (128, rows_dev)).T
        lanes = lax.broadcasted_iota(jnp.int32, (rows_dev, 128), 1)
        idb[pl.ds(k * rows_dev, rows_dev), :] = jnp.where(full >= 0, full - lanes, -(2**20))

    def phase(index, c):
        first, last = ranges[index]
        start, depth = 2 * first * fp, 2 * (last - first) * fp
        cols = pl.ds(*chunks[c])
        block = buf[pl.ds(start, depth), cols]
        prod = jnp.dot(spread[index][...], block, preferred_element_type=jnp.float32)
        w32 = block.astype(jnp.float32)
        sq = jnp.sum((w32 * w32).reshape(depth // 8, 8, chunks[c][1]), 0)
        if index == 0:
            acc[:, cols] = prod
            csq[:, cols] = sq
        else:
            acc[:, cols] += prod
            csq[:, cols] += sq

    tail = pl.ds(2 * (n - 1) * fp, 2 * fp)

    def finish_scale(c):
        cols = pl.ds(*chunks[c])
        w32 = buf[tail, cols].astype(jnp.float32)
        sq = jnp.sum((w32 * w32).reshape(2 * fp // 8, 8, chunks[c][1]), 0) + csq[:, cols]
        scale[:, cols] = lax.rsqrt(jnp.sum(sq, 0, keepdims=True) + epsilon)

    def final(k, c):
        start, wide = chunks[c]
        prod = jnp.dot(dp_c[pl.ds(k * rows_dev, rows_dev), :], buf[tail, pl.ds(start, wide)],
                       preferred_element_type=jnp.float32)
        for r in range(0, rows_dev, ROWS):
            rs = pl.ds(k * rows_dev + r, ROWS)
            top, hit = mx[rs, :], ch[rs, :]
            ids = idb[rs, :]
            for a in range(0, wide, 128):
                w = min(128, wide - a)
                cols = pl.ds(start + a, w)
                v = (acc[rs, cols] + prod[r:r + ROWS, a:a + w]) * scale[:, cols]
                if w == 128:
                    top = jnp.maximum(top, v)
                    hit = jnp.where(ids == start + a, v, hit)
                else:
                    mx[rs, :] = top
                    ch[rs, :] = hit
                    mx[rs, pl.ds(0, w)] = jnp.maximum(mx[rs, pl.ds(0, w)], v)
                    ch[rs, pl.ds(0, w)] = jnp.where(idb[rs, pl.ds(0, w)] == start + a, v, ch[rs, pl.ds(0, w)])
            if wide % 128 == 0:
                mx[rs, :] = top
                ch[rs, :] = hit

    def reduced(k):
        rs = pl.ds(k * rows_dev, rows_dev)
        return (jnp.max(mx[rs, :].T, 0, keepdims=True), jnp.sum(ch[rs, :].T, 0, keepdims=True))

    mx[...] = jnp.full(mx.shape, -3.0e38, jnp.float32)
    ch[...] = jnp.zeros(ch.shape, jnp.float32)
    permute(0)
    prepare_ids(0)
    wide = docs_all[0].astype(jnp.float32)
    squares = wide * wide
    total = squares[:, 0:128]
    for a in range(128, wide.shape[1], 128):
        total = total + squares[:, a:a + 128]
    scale_x = lax.rsqrt(jnp.sum(total.T, 0, keepdims=True) + epsilon)

    def step(way, h, c):
        s = slot(way, h)
        landed(s, 0, c)
        if h < reach(way, c):
            ring(way, h, c)
        share(s, c)

    def pair(h, i):
        step(0, h, i)
        step(1, h, (i + half) % PIECES)

    def partners(slots, c):
        for s in slots:
            landed(s, 1, c)

    early, late = range(n - 3), (n - 3, n - 2)
    order = [j // 2 + half * (j % 2) for j in range(PIECES)]
    for h in range(1, hops):
        for i in range(PIECES):
            pair(h, i)
            if h == hops - 2 and i == half:
                for copy in doc_copies:
                    copy.wait()
                for k in range(1, nd):
                    permute(k)
                    prepare_ids(k)
            if h == hops - 1:
                c = order[i]
                partners(early, c)
                phase(0, c)
    for c in order[:half]:
        partners(late, c)
        phase(1, c)
    for i in range(half):
        for way in (0, 1):
            c = i + half * way
            landed(n - 1, 0, c)
            share(n - 1, c)
    for c in order[half:]:
        partners(late, c)
        phase(1, c)
    for c in order[:-2]:
        landed(n - 1, 1, c)
        finish_scale(c)
        for k in range(nd):
            final(k, c)
    for c in order[-2:]:
        landed(n - 1, 1, c)
        finish_scale(c)

    returns = []
    for k in range(1, nd):
        for c in order[-2:]:
            final(k, c)
        best, chosen = reduced(k)
        res[k, 0:1, :] = best
        res[k, 1:2, :] = chosen
        copy = pltpu.make_async_remote_copy(
            src_ref=res.at[k], dst_ref=got.at[k], send_sem=res_send.at[k], recv_sem=res_recv.at[k],
            device_id={"doc": lax.rem(doc + nd - k, nd)}, device_id_type=MESH)
        copy.start()
        returns.append(copy)
    for c in order[-2:]:
        final(0, c)
    best, chosen = reduced(0)
    for k in range(1, nd):
        returns[k - 1].wait()
        best = jnp.maximum(best, got[k, 0:1, :])
        chosen = chosen + got[k, 1:2, :]
    near_out[...] = best * scale_x
    chosen_out[...] = chosen * scale_x
    for copy in sent:
        copy.wait_send()


def layer_kernel(nz, feat, docs_in, cents_in, ids_in, near_out, chosen_out,
                 own, raw, buf, docs, ids, acc, idb, csq, scale, res, got,
                 local_sem, c_send, c_recv, z_send, d_send, d_recv, i_send, i_recv, r_send, r_recv):
    width = cents_in.shape[1]
    rows_dev, depth = docs_in.shape
    tiles = own.shape[1] // 128
    per = tiles // 2
    small = per // 2
    big = per - small
    wide = big * 128
    full = width // 128 * 128
    late = -(-4 * feat // 256) * 256
    early = depth - late
    a = rows_dev * 3 // 8 // 16 * 16
    b = (rows_dev - a) // 32 * 16
    spans = ((0, a), (a, b), (a + b, rows_dev - a - b))

    clu, doc = lax.axis_index("clu"), lax.axis_index("doc")
    core, chip = lax.rem(clu, 2), lax.div(clu, 2)
    z, x = lax.div(chip, 2), lax.rem(chip, 2)
    upper = z >= nz // 2

    def device(r, dz=0):
        dx, dy, dc = r // 4, r // 2 % 2, r % 2
        there = ((z + dz) * 2 + (1 - x if dx else x)) * 2 + (1 - core if dc else core)
        return {"clu": there, "doc": 1 - doc if dy else doc}

    def when(cond, body):
        if cond is None:
            body()
        else:
            pl.when(cond)(body)

    def both(p, q):
        return q if p is None else p if q is None else p & q

    sizes = ((None, big),) if big == small else ((1, big), (0, small))

    def sized(c, cond, body):
        for value, count in sizes:
            when(both(cond, None if value is None else c == value), functools.partial(body, count * 128))

    own_copy = pltpu.make_async_copy(cents_in.at[:, pl.ds(0, full)], own.at[:, pl.ds(0, full)], local_sem.at[0])
    docs_copy = pltpu.make_async_copy(docs_in, docs.at[0], local_sem.at[1])
    ids_copy = pltpu.make_async_copy(ids_in, ids.at[0], local_sem.at[2])
    own_copy.start()
    if full < width:
        raw_copy = pltpu.make_async_copy(cents_in.at[:, pl.ds(full, width - full)], raw, local_sem.at[3])
        raw_copy.start()
    docs_copy.start()
    ids_copy.start()

    above, below = z < nz - 1, z > 0
    barrier = pltpu.get_barrier_semaphore()

    def greet(to):
        pl.semaphore_signal(barrier, inc=1, device_id=to, device_id_type=MESH)

    pl.when(above)(lambda: greet(device(0, 1)))
    pl.when(below)(lambda: greet(device(0, -1)))
    for r in (4, 5, 2, 1):
        greet(device(r))
    if small < big:
        @pl.when(core == 0)
        def _():
            buf[:, pl.ds(small * 128, 128)] = jnp.zeros((buf.shape[0], 128), buf.dtype)
    if full < width:
        raw_copy.wait()
        own[:, pl.ds(full, 128)] = jnp.concatenate(
            [raw[...], jnp.zeros((feat, full + 128 - width), raw.dtype)], axis=1)
    own_copy.wait()
    docs_copy.wait()
    ids_copy.wait()
    pl.semaphore_wait(barrier, 4 + above.astype(jnp.int32) + below.astype(jnp.int32))

    pending = []

    def start(make, cond=None):
        when(cond, lambda: make().start())
        pending.append((cond, make))

    def start_sized(make, c, cond=None):
        sized(c, cond, lambda w: make(w).start())
        pending.append((c, cond, make))

    def remote(src, dst, ss, rs, to):
        return pltpu.make_async_remote_copy(
            src_ref=src, dst_ref=dst, send_sem=ss, recv_sem=rs, device_id=to, device_id_type=MESH)

    near = (0, 1, 4, 5)

    def source(layer, j):
        r = near[j]
        there = (layer * 2 + (1 - x if r // 4 else x)) * 2 + (1 - core if r % 2 else core)
        return pl.ds(pl.multiple_of(there * feat, 16), feat)

    def columns(r, w):
        xd = 1 - x if r // 4 else x
        cd = 1 - core if r % 2 else core
        return pl.ds(pl.multiple_of((xd * per + cd * small) * 128, 128), w)

    mine = source(z, 0)

    def exchange(j):
        r = near[j]
        start_sized(lambda w: remote(own.at[:, columns(r, w)], buf.at[mine, pl.ds(0, w)],
                                     c_send.at[j], c_recv.at[z, j], device(r)),
                    1 - core if r % 2 else core)

    def landed(layer, j, cond=None):
        rows = source(layer, j)
        sized(core, cond, lambda w: remote(
            buf.at[rows, pl.ds(0, w)], buf.at[rows, pl.ds(0, w)], c_send.at[j], c_recv.at[layer, j],
            device(1)).wait_recv())

    def climb(layer, j, way, s, cond):
        rows = source(layer, j)
        src = (lambda w: own.at[:, columns(0, w)]) if s == 0 and j == 0 else (lambda w: buf.at[rows, pl.ds(0, w)])
        start_sized(lambda w: remote(src(w), buf.at[rows, pl.ds(0, w)], z_send.at[way, s, j],
                                     c_recv.at[layer, j], device(0, 1 - 2 * way)), core, cond)

    def spread(j):
        if j:
            landed(z, j)
        climb(z, j, 0, 0, above)
        climb(z, j, 1, 0, below)

    def relay(s, j):
        up, down = z >= s, z + s < nz
        landed(z - s, j, up)
        if s < nz - 1:
            climb(z - s, j, 0, s, up & above)
        landed(z + s, j, down)
        if s < nz - 1:
            climb(z + s, j, 1, s, down & below)

    def part(slot, p):
        return docs.at[slot, pl.ds(*spans[p]), :]

    def send_docs(src_slot, p, dst_slot, r):
        start(lambda: remote(part(src_slot, p), part(dst_slot, p), d_send.at[dst_slot, p],
                             d_recv.at[dst_slot, p], device(r)))

    def send_ids(src_slot, dst_slot, r):
        start(lambda: remote(ids.at[src_slot], ids.at[dst_slot], i_send.at[dst_slot],
                             i_recv.at[dst_slot], device(r)))

    def have_docs(slot, p):
        remote(part(slot, p), part(slot, p), d_send.at[slot, p], d_recv.at[slot, p], device(1)).wait_recv()

    def have_ids(slot):
        remote(ids.at[slot], ids.at[slot], i_send.at[slot], i_recv.at[slot], device(1)).wait_recv()

    def share(slot, p):
        send_docs(slot, p, slot + 1, 1)

    spread(0)
    for j in (1, 2, 3):
        exchange(j)
    send_ids(0, 2, 2)
    for p in (0, 1, 2):
        send_docs(0, p, 2, 2)
    send_ids(0, 4, 4)
    for p in (1, 2, 0):
        send_docs(0, p, 4, 4)
    send_ids(0, 1, 1)
    for p in (0, 1, 2):
        send_docs(0, p, 1, 1)

    part_cols = jnp.where(core == 1, big, small) * 128
    first = (x * per + core * small) * 128
    base = doc * width + first
    reach = jnp.minimum(part_cols, width - first)
    lanes = lax.broadcasted_iota(jnp.int32, (rows_dev, 128), 1)

    def prepare_ids(slot):
        rel = ids[slot] - base
        rel = jnp.where((rel >= 0) & (rel < reach), rel, -1)
        tall = jnp.broadcast_to(rel, (128, rows_dev)).T
        idb[slot] = jnp.where(tall >= 0, tall - lanes, -(2**20))

    buf[mine, pl.ds(0, small * 128)] = own[:, columns(0, small * 128)]
    if small < big:
        @pl.when(core == 1)
        def _():
            start_col = pl.multiple_of((x * per + 2 * small) * 128, 128)
            buf[mine, pl.ds(small * 128, 128)] = own[:, pl.ds(start_col, 128)]

    spread(1)
    prepare_ids(0)
    spread(2)
    relay(1, 0)
    spread(3)
    relay(1, 1)
    have_docs(2, 0)
    send_docs(2, 0, 6, 4)
    share(2, 0)
    have_ids(4)
    send_ids(4, 6, 2)
    send_ids(4, 5, 1)
    have_ids(2)
    send_ids(2, 3, 1)
    relay(1, 2)
    have_docs(4, 1)
    send_docs(4, 1, 6, 2)
    share(4, 1)
    relay(1, 3)
    have_docs(2, 1)
    share(2, 1)
    for s in range(2, nz - 1):
        relay(s, 0)
    have_docs(4, 2)
    send_docs(4, 2, 6, 2)
    share(4, 2)
    have_docs(2, 2)
    share(2, 2)
    have_ids(6)
    send_ids(6, 7, 1)
    for slot in (1, 2, 3, 4, 5, 6, 7):
        if slot in (1, 3, 5, 7):
            have_ids(slot)
        prepare_ids(slot)
    for s in range(2, nz - 1):
        for j in (1, 2, 3):
            relay(s, j)

    early_at = pl.multiple_of(jnp.where(upper, late, 0), 256)
    late_at = pl.multiple_of(jnp.where(upper, 0, early), 256)

    def squares(at, count):
        w32 = buf[pl.ds(at, count), :].astype(jnp.float32)
        return jnp.sum((w32 * w32).reshape(count // 8, 8, wide), 0)

    def begin(slot):
        acc[slot] = jnp.dot(docs[slot, :, pl.ds(early_at, early)], buf[pl.ds(early_at, early), :],
                            preferred_element_type=jnp.float32)

    csq[...] = squares(early_at, early)
    begin(0)
    for p in (0, 1, 2):
        have_docs(1, p)
    begin(1)
    begin(2)
    have_docs(4, 0)
    share(4, 0)
    for p in (0, 1, 2):
        have_docs(3, p)
    begin(3)
    begin(4)
    for p in (1, 2, 0):
        have_docs(6, p)
        share(6, p)
    for p in (1, 2, 0):
        have_docs(5, p)
    begin(5)
    begin(6)
    for p in (1, 2, 0):
        have_docs(7, p)
    begin(7)
    for j in (0, 1, 2, 3):
        relay(nz - 1, j)

    total = jnp.sum(csq[...] + squares(late_at, late), 0, keepdims=True)
    scale[...] = lax.rsqrt(total + epsilon)
    lane = lax.broadcasted_iota(jnp.int32, (1, 128), 1)

    def finish(slot):
        prod = jnp.dot(docs[slot, :, pl.ds(late_at, late)], buf[pl.ds(late_at, late), :],
                       preferred_element_type=jnp.float32)
        tops, hits = [], []
        for r in range(0, rows_dev, ROWS):
            rs = pl.ds(r, ROWS)
            top = jnp.full((ROWS, 128), -3.0e38, jnp.float32)
            hit = jnp.zeros((ROWS, 128), jnp.float32)
            where_id = idb[slot, rs, :]
            for c in range(0, wide, 128):
                cols = pl.ds(c, 128)
                v = (acc[slot, rs, cols] + prod[r:r + ROWS, c:c + 128]) * scale[:, cols]
                hit = jnp.where(where_id == c, v, hit)
                if c + 128 > small * 128 or (c + 128 == small * 128 and small == big):
                    v = jnp.where(lane < reach - c, v, -3.0e38)
                top = jnp.maximum(top, v)
            tops.append(top)
            hits.append(hit)
        return (jnp.max(jnp.concatenate(tops, 0).T, 0, keepdims=True),
                jnp.sum(jnp.concatenate(hits, 0).T, 0, keepdims=True))

    for slot in (7, 6, 3, 2, 5, 4, 1):
        best, chosen = finish(slot)
        res[slot, 0:1, :] = best
        res[slot, 1:2, :] = chosen
        start(lambda slot=slot: remote(res.at[slot], got.at[slot], r_send.at[slot], r_recv.at[slot], device(slot)))
    best, chosen = finish(0)
    x32 = docs[0].astype(jnp.float32)
    sq = x32 * x32
    total = sq[:, 0:128]
    for c in range(128, depth, 128):
        total = total + sq[:, c:c + 128]
    scale_x = lax.rsqrt(jnp.sum(total.T, 0, keepdims=True) + epsilon)
    for slot in (1, 4, 5, 2, 3, 6, 7):
        remote(res.at[slot], got.at[slot], r_send.at[slot], r_recv.at[slot], device(slot)).wait_recv()
        best = jnp.maximum(best, got[slot, 0:1, :])
        chosen = chosen + got[slot, 1:2, :]
    near_out[...] = best * scale_x
    chosen_out[...] = chosen * scale_x
    for entry in pending:
        if len(entry) == 2:
            cond, make = entry
            when(cond, lambda: make().wait_send())
        else:
            c, cond, make = entry
            sized(c, cond, lambda w: make(w).wait_send())


def by_layers(docs, centroids, assigned):
    nz = lax.axis_size("clu") // 4
    rows_dev, depth = docs.shape
    width, feat = centroids.shape
    tiles = -(-width // 128)
    wide = (tiles // 2 - tiles // 4) * 128
    any_space = pl.BlockSpec(memory_space=pl.ANY)
    vmem = pl.BlockSpec(memory_space=pltpu.VMEM)
    dma = pltpu.SemaphoreType.DMA
    line = jax.ShapeDtypeStruct((1, rows_dev), jnp.float32)
    near, chosen = pl.pallas_call(
        functools.partial(layer_kernel, nz, feat),
        out_shape=(line, line),
        in_specs=[any_space] * 3,
        out_specs=(vmem, vmem),
        scratch_shapes=[
            pltpu.VMEM((feat, tiles * 128), jnp.bfloat16),
            pltpu.VMEM((feat, width % 128 or 128), jnp.bfloat16),
            pltpu.VMEM((depth, wide), jnp.bfloat16),
            pltpu.VMEM((8, rows_dev, depth), jnp.bfloat16),
            pltpu.VMEM((8, 1, rows_dev), jnp.int32),
            pltpu.VMEM((8, rows_dev, wide), jnp.float32),
            pltpu.VMEM((8, rows_dev, 128), jnp.int32),
            pltpu.VMEM((8, wide), jnp.float32),
            pltpu.VMEM((1, wide), jnp.float32),
            pltpu.VMEM((8, 2, rows_dev), jnp.float32),
            pltpu.VMEM((8, 2, rows_dev), jnp.float32),
            dma((4,)),
            dma((4,)), dma((nz, 4)), dma((2, nz, 4)),
            dma((8, 3)), dma((8, 3)), dma((8,)), dma((8,)), dma((8,)), dma((8,)),
        ],
        compiler_params=pltpu.CompilerParams(collective_id=0, has_side_effects=True),
        name="layer_distances",
    )(docs, centroids.T, assigned.reshape(1, rows_dev))
    return 1.0 - near.reshape(rows_dev), 1.0 - chosen.reshape(rows_dev)


def fits_layers(docs, centroids):
    tiles = -(-centroids.shape[0] // 128)
    n_clu, feat = lax.axis_size("clu"), centroids.shape[1]
    return (lax.axis_size("doc") == 2 and n_clu % 8 == 0 and tiles % 2 == 0 and tiles >= 4
            and feat % 16 == 0 and docs.shape[0] % 128 == 0 and docs.shape[1] % 256 == 0
            and docs.shape[1] > 4 * feat + 255)


def on_device(docs, centroids, assigned):
    if fits_layers(docs, centroids):
        return by_layers(docs, centroids, assigned)
    n_clu, nd = lax.axis_size("clu"), lax.axis_size("doc")
    n = n_clu // 2
    rows_dev, depth = docs.shape
    width, feat = centroids.shape
    fp = (feat + 15) // 16 * 16
    cents = centroids.T
    if fp != feat:
        cents = jnp.pad(cents, ((0, fp - feat), (0, 0)))
    rows = nd * rows_dev
    any_space = pl.BlockSpec(memory_space=pl.ANY)
    vmem = pl.BlockSpec(memory_space=pltpu.VMEM)
    dma = pltpu.SemaphoreType.DMA
    hops = n // 2
    line = jax.ShapeDtypeStruct((1, rows_dev), jnp.float32)
    near, chosen = pl.pallas_call(
        functools.partial(kernel, n, nd, feat),
        out_shape=(line, line),
        in_specs=[any_space] * 3,
        out_specs=(vmem, vmem),
        scratch_shapes=[
            pltpu.VMEM((n_clu * fp, width), jnp.bfloat16),
            pltpu.VMEM((nd, rows_dev, depth), jnp.bfloat16),
            pltpu.VMEM((nd, 1, rows_dev), jnp.int32),
            pltpu.VMEM((rows, (n - 3) * 2 * fp), jnp.bfloat16),
            pltpu.VMEM((rows, 4 * fp), jnp.bfloat16),
            pltpu.VMEM((rows, 2 * fp), jnp.bfloat16),
            pltpu.VMEM((rows, width), jnp.float32),
            pltpu.VMEM((rows, 128), jnp.int32),
            pltpu.VMEM((rows, 128), jnp.float32),
            pltpu.VMEM((rows, 128), jnp.float32),
            pltpu.VMEM((8, width), jnp.float32),
            pltpu.VMEM((1, width), jnp.float32),
            pltpu.VMEM((nd, 2, rows_dev), jnp.float32),
            pltpu.VMEM((nd, 2, rows_dev), jnp.float32),
            dma((3,)),
            dma((2, hops, PIECES)),
            dma((n, PIECES)),
            dma((n, 2, PIECES)),
            dma((nd,)), dma((nd,)), dma((nd,)), dma((nd,)), dma((nd,)), dma((nd,)),
        ],
        compiler_params=pltpu.CompilerParams(collective_id=0, has_side_effects=True),
        name="ring_distances",
    )(docs, cents, assigned.reshape(1, rows_dev))
    return 1.0 - near.reshape(rows_dev), 1.0 - chosen.reshape(rows_dev)


def solution(mesh):
    placed = (P(("clu", "doc"), None), P("doc", "clu"), P(("clu", "doc")))
    return jax.shard_map(
        on_device,
        mesh=mesh,
        in_specs=placed,
        out_specs=(P(("clu", "doc")), P(("clu", "doc"))),
        check_vma=False,
    )
```

```python
import functools

import jax
import jax.numpy as jnp
from jax import lax
from jax.experimental import pallas as pl
from jax.experimental.pallas import tpu as pltpu
from jax.sharding import PartitionSpec as P

epsilon = 1e-06
PIECES = 4
ROWS = 64
MESH = pl.DeviceIdType.MESH


def chip_at(pos, n):
    half = n // 2
    return jnp.where(pos < half, 2 * pos, 2 * (n - 1 - pos) + 1)


def cut(width):
    tiles = (width + 127) // 128
    ends = [min(-(-tiles * (c + 1) // PIECES) * 128, width) for c in range(PIECES)]
    return tuple((a, b - a) for a, b in zip([0] + ends[:-1], ends))


def kernel(n, nd, feat, docs_in, cents_in, ids_in, near_out, chosen_out,
           buf, docs_all, ids_all, dp_a, dp_b, dp_c, acc, idb, mx, ch, csq, scale, res, got,
           local_sem, ring_send, pair_send, recv, docs_send, docs_recv, ids_send, ids_recv,
           res_send, res_recv):
    hops = n // 2
    fp = cents_in.shape[0]
    width = cents_in.shape[1]
    rows_dev = docs_in.shape[0]
    chunks = cut(width)
    half = len(chunks) // 2

    clu, doc = lax.axis_index("clu"), lax.axis_index("doc")
    core, chip = lax.rem(clu, 2), lax.div(clu, 2)
    z, x = lax.div(chip, 2), lax.rem(chip, 2)
    pos = jnp.where(x == 0, z, n - 1 - z)
    right = chip_at(lax.rem(pos + 1, n), n) * 2 + core
    left = chip_at(lax.rem(pos + n - 1, n), n) * 2 + core
    partner = chip * 2 + (1 - core)

    own_c = pltpu.make_async_copy(cents_in, buf.at[pl.ds(0, fp), :], local_sem.at[0])
    own_d = pltpu.make_async_copy(docs_in, docs_all.at[0], local_sem.at[1])
    own_i = pltpu.make_async_copy(ids_in, ids_all.at[0], local_sem.at[2])
    own_c.start()
    own_d.start()
    own_i.start()

    barrier = pltpu.get_barrier_semaphore()
    for peer in (left, right, partner):
        pl.semaphore_signal(barrier, inc=1, device_id={"clu": peer}, device_id_type=MESH)
    for k in range(1, nd):
        pl.semaphore_signal(barrier, inc=1, device_id={"doc": lax.rem(doc + k, nd)}, device_id_type=MESH)
    pl.semaphore_wait(barrier, 3 + nd - 1)

    def slot(way, h):
        if h == 0:
            return 0
        if h == hops:
            return n - 1
        return 2 * h - 1 if way == 0 else 2 * h

    def piece(s, m, c):
        return buf.at[pl.ds((2 * s + m) * fp, fp), pl.ds(*chunks[c])]

    def reach(way, c):
        return hops if way == c // half else hops - 1

    sent = []

    def ring(way, h, c):
        s, t = slot(way, h), slot(way, h + 1)
        copy = pltpu.make_async_remote_copy(
            src_ref=piece(s, 0, c), dst_ref=piece(t, 0, c),
            send_sem=ring_send.at[way, h, c], recv_sem=recv.at[t, 0, c],
            device_id={"clu": right if way == 0 else left}, device_id_type=MESH)
        copy.start()
        sent.append(copy)

    def share(s, c):
        copy = pltpu.make_async_remote_copy(
            src_ref=piece(s, 0, c), dst_ref=piece(s, 1, c),
            send_sem=pair_send.at[s, c], recv_sem=recv.at[s, 1, c],
            device_id={"clu": partner}, device_id_type=MESH)
        copy.start()
        sent.append(copy)

    def landed(s, m, c):
        pltpu.make_async_remote_copy(
            src_ref=piece(s, m, c), dst_ref=piece(s, m, c),
            send_sem=pair_send.at[s, c], recv_sem=recv.at[s, m, c],
            device_id={"clu": partner}, device_id_type=MESH).wait_recv()

    own_c.wait()
    for i in range(PIECES):
        ring(0, 0, i)
        ring(1, 0, (i + half) % PIECES)
    for c in range(PIECES):
        share(0, c)
    own_d.wait()
    own_i.wait()
    doc_copies = []
    for k in range(1, nd):
        mate = lax.rem(doc + k, nd)
        for ref, ss, rs in ((ids_all, ids_send, ids_recv), (docs_all, docs_send, docs_recv)):
            copy = pltpu.make_async_remote_copy(
                src_ref=ref.at[0], dst_ref=ref.at[k], send_sem=ss.at[k], recv_sem=rs.at[k],
                device_id={"doc": mate}, device_id_type=MESH)
            copy.start()
            doc_copies.append(copy)

    def owner(s):
        if s == 0:
            p = pos
        elif s == n - 1:
            p = pos + hops
        elif s % 2:
            p = pos + n - (s + 1) // 2
        else:
            p = pos + s // 2
        return chip_at(lax.rem(p, n), n)

    ranges = ((0, n - 3), (n - 3, n - 1), (n - 1, n))
    spread = (dp_a, dp_b, dp_c)

    def permute(k):
        rows = docs_all[k]
        for (first, last), out in zip(ranges, spread):
            wide = out.shape[1]
            lane = lax.broadcasted_iota(jnp.int32, (1, wide), 1)
            target = jnp.full((1, wide), -1, jnp.int32)
            for s in range(first, last):
                chip_s = owner(s)
                for m in (0, 1):
                    part = chip_s * 2 + (core if m == 0 else 1 - core)
                    start = (2 * (s - first) + m) * fp
                    inside = (lane >= start) & (lane < start + feat)
                    target = jnp.where(inside, lane - start + part * feat, target)
            source = lax.broadcasted_iota(jnp.int32, (rows.shape[1], wide), 0)
            mover = jnp.where(source == target, 1.0, 0.0).astype(jnp.bfloat16)
            out[pl.ds(k * rows_dev, rows_dev), :] = jnp.dot(
                rows, mover, preferred_element_type=jnp.float32).astype(jnp.bfloat16)

    def prepare_ids(k):
        base = doc * width
        ids = ids_all[k] - base
        ids = jnp.where((ids >= 0) & (ids < width), ids, -1)
        full = jnp.broadcast_to(ids, (128, rows_dev)).T
        lanes = lax.broadcasted_iota(jnp.int32, (rows_dev, 128), 1)
        idb[pl.ds(k * rows_dev, rows_dev), :] = jnp.where(full >= 0, full - lanes, -(2**20))

    def phase(index, c):
        first, last = ranges[index]
        start, depth = 2 * first * fp, 2 * (last - first) * fp
        cols = pl.ds(*chunks[c])
        block = buf[pl.ds(start, depth), cols]
        prod = jnp.dot(spread[index][...], block, preferred_element_type=jnp.float32)
        w32 = block.astype(jnp.float32)
        sq = jnp.sum((w32 * w32).reshape(depth // 8, 8, chunks[c][1]), 0)
        if index == 0:
            acc[:, cols] = prod
            csq[:, cols] = sq
        else:
            acc[:, cols] += prod
            csq[:, cols] += sq

    tail = pl.ds(2 * (n - 1) * fp, 2 * fp)

    def finish_scale(c):
        cols = pl.ds(*chunks[c])
        w32 = buf[tail, cols].astype(jnp.float32)
        sq = jnp.sum((w32 * w32).reshape(2 * fp // 8, 8, chunks[c][1]), 0) + csq[:, cols]
        scale[:, cols] = lax.rsqrt(jnp.sum(sq, 0, keepdims=True) + epsilon)

    def final(k, c):
        start, wide = chunks[c]
        prod = jnp.dot(dp_c[pl.ds(k * rows_dev, rows_dev), :], buf[tail, pl.ds(start, wide)],
                       preferred_element_type=jnp.float32)
        for r in range(0, rows_dev, ROWS):
            rs = pl.ds(k * rows_dev + r, ROWS)
            top, hit = mx[rs, :], ch[rs, :]
            ids = idb[rs, :]
            for a in range(0, wide, 128):
                w = min(128, wide - a)
                cols = pl.ds(start + a, w)
                v = (acc[rs, cols] + prod[r:r + ROWS, a:a + w]) * scale[:, cols]
                if w == 128:
                    top = jnp.maximum(top, v)
                    hit = jnp.where(ids == start + a, v, hit)
                else:
                    mx[rs, :] = top
                    ch[rs, :] = hit
                    mx[rs, pl.ds(0, w)] = jnp.maximum(mx[rs, pl.ds(0, w)], v)
                    ch[rs, pl.ds(0, w)] = jnp.where(idb[rs, pl.ds(0, w)] == start + a, v, ch[rs, pl.ds(0, w)])
            if wide % 128 == 0:
                mx[rs, :] = top
                ch[rs, :] = hit

    def reduced(k):
        rs = pl.ds(k * rows_dev, rows_dev)
        return (jnp.max(mx[rs, :].T, 0, keepdims=True), jnp.sum(ch[rs, :].T, 0, keepdims=True))

    mx[...] = jnp.full(mx.shape, -3.0e38, jnp.float32)
    ch[...] = jnp.zeros(ch.shape, jnp.float32)
    permute(0)
    prepare_ids(0)
    wide = docs_all[0].astype(jnp.float32)
    squares = wide * wide
    total = squares[:, 0:128]
    for a in range(128, wide.shape[1], 128):
        total = total + squares[:, a:a + 128]
    scale_x = lax.rsqrt(jnp.sum(total.T, 0, keepdims=True) + epsilon)

    def step(way, h, c):
        s = slot(way, h)
        landed(s, 0, c)
        if h < reach(way, c):
            ring(way, h, c)
        share(s, c)

    def pair(h, i):
        step(0, h, i)
        step(1, h, (i + half) % PIECES)

    def partners(slots, c):
        for s in slots:
            landed(s, 1, c)

    early, late = range(n - 3), (n - 3, n - 2)
    order = [j // 2 + half * (j % 2) for j in range(PIECES)]
    for h in range(1, hops):
        for i in range(PIECES):
            pair(h, i)
            if h == hops - 2 and i == half:
                for copy in doc_copies:
                    copy.wait()
                for k in range(1, nd):
                    permute(k)
                    prepare_ids(k)
            if h == hops - 1:
                c = order[i]
                partners(early, c)
                phase(0, c)
    for c in order[:half]:
        partners(late, c)
        phase(1, c)
    for i in range(half):
        for way in (0, 1):
            c = i + half * way
            landed(n - 1, 0, c)
            share(n - 1, c)
    for c in order[half:]:
        partners(late, c)
        phase(1, c)
    for c in order[:-2]:
        landed(n - 1, 1, c)
        finish_scale(c)
        for k in range(nd):
            final(k, c)
    for c in order[-2:]:
        landed(n - 1, 1, c)
        finish_scale(c)

    returns = []
    for k in range(1, nd):
        for c in order[-2:]:
            final(k, c)
        best, chosen = reduced(k)
        res[k, 0:1, :] = best
        res[k, 1:2, :] = chosen
        copy = pltpu.make_async_remote_copy(
            src_ref=res.at[k], dst_ref=got.at[k], send_sem=res_send.at[k], recv_sem=res_recv.at[k],
            device_id={"doc": lax.rem(doc + nd - k, nd)}, device_id_type=MESH)
        copy.start()
        returns.append(copy)
    for c in order[-2:]:
        final(0, c)
    best, chosen = reduced(0)
    for k in range(1, nd):
        returns[k - 1].wait()
        best = jnp.maximum(best, got[k, 0:1, :])
        chosen = chosen + got[k, 1:2, :]
    near_out[...] = best * scale_x
    chosen_out[...] = chosen * scale_x
    for copy in sent:
        copy.wait_send()


def layer_kernel(nz, feat, docs_in, cents_in, ids_in, near_out, chosen_out,
                 own, raw, buf, docs, ids, acc, idb, mx, ch, csq, scale, res, got,
                 local_sem, c_send, c_recv, z_send, last_send, last_recv,
                 d_send, d_recv, i_send, i_recv, r_send, r_recv):
    width = cents_in.shape[1]
    rows_dev, depth = docs_in.shape
    tiles = own.shape[1] // 128
    per = tiles // 2
    small = per // 2
    big = per - small
    wide = big * 128
    full = width // 128 * 128
    late = -(-4 * feat // 256) * 256
    k1 = 8 * feat // 256 * 256
    k2 = depth - late - k1
    a = rows_dev * 5 // 16 // 16 * 16
    b = (rows_dev - a) // 32 * 16
    spans = ((0, a), (a, b), (a + b, rows_dev - a - b))
    chunks = tuple((c, min(256, wide - c)) for c in range(0, wide, 256))

    clu, doc = lax.axis_index("clu"), lax.axis_index("doc")
    core, chip = lax.rem(clu, 2), lax.div(clu, 2)
    z, x = lax.div(chip, 2), lax.rem(chip, 2)
    upper = z >= nz // 2
    out = jnp.where(upper, 1, -1)
    end = (z == 0) | (z == nz - 1)
    inner = jnp.logical_not(end)

    def device(r, dz=0):
        dx, dy, dc = r // 4, r // 2 % 2, r % 2
        there = ((z + dz) * 2 + (1 - x if dx else x)) * 2 + (1 - core if dc else core)
        return {"clu": there, "doc": 1 - doc if dy else doc}

    def when(cond, body):
        if cond is None:
            body()
        else:
            pl.when(cond)(body)

    def both(p, q):
        return q if p is None else p if q is None else p & q

    sizes = ((None, big),) if big == small else ((1, big), (0, small))

    def sized(c, cond, body):
        for value, count in sizes:
            when(both(cond, None if value is None else c == value), functools.partial(body, count * 128))

    own_copy = pltpu.make_async_copy(cents_in.at[:, pl.ds(0, full)], own.at[:, pl.ds(0, full)], local_sem.at[0])
    docs_copy = pltpu.make_async_copy(docs_in, docs.at[0], local_sem.at[1])
    ids_copy = pltpu.make_async_copy(ids_in, ids.at[0], local_sem.at[2])
    own_copy.start()
    if full < width:
        raw_copy = pltpu.make_async_copy(cents_in.at[:, pl.ds(full, width - full)], raw, local_sem.at[3])
        raw_copy.start()
    docs_copy.start()
    ids_copy.start()

    barrier = pltpu.get_barrier_semaphore()

    def greet(to):
        pl.semaphore_signal(barrier, inc=1, device_id=to, device_id_type=MESH)

    pl.when(inner)(lambda: greet(device(0, out)))
    greet(device(0, -out))
    for r in (4, 5, 2, 1):
        greet(device(r))
    if small < big:
        @pl.when(core == 0)
        def _():
            buf[:, pl.ds(small * 128, 128)] = jnp.zeros((buf.shape[0], 128), buf.dtype)
    if full < width:
        raw_copy.wait()
        own[:, pl.ds(full, 128)] = jnp.concatenate(
            [raw[...], jnp.zeros((feat, full + 128 - width), raw.dtype)], axis=1)
    own_copy.wait()
    docs_copy.wait()
    ids_copy.wait()
    pl.semaphore_wait(barrier, 5 + inner.astype(jnp.int32))

    pending = []

    def start(make, cond=None):
        when(cond, lambda: make().start())
        pending.append((cond, make))

    def start_sized(make, c, cond=None):
        sized(c, cond, lambda w: make(w).start())
        pending.append((c, cond, make))

    def remote(src, dst, ss, rs, to):
        return pltpu.make_async_remote_copy(
            src_ref=src, dst_ref=dst, send_sem=ss, recv_sem=rs, device_id=to, device_id_type=MESH)

    near = (0, 1, 4, 5)

    def source(layer, j):
        r = near[j]
        there = (layer * 2 + (1 - x if r // 4 else x)) * 2 + (1 - core if r % 2 else core)
        return pl.ds(pl.multiple_of(there * feat, 16), feat)

    def columns(r, w):
        xd = 1 - x if r // 4 else x
        cd = 1 - core if r % 2 else core
        return pl.ds(pl.multiple_of((xd * per + cd * small) * 128, 128), w)

    mine = source(z, 0)

    def exchange(j):
        r = near[j]
        start_sized(lambda w: remote(own.at[:, columns(r, w)], buf.at[mine, pl.ds(0, w)],
                                     c_send.at[j], c_recv.at[z, j], device(r)),
                    1 - core if r % 2 else core)

    def landed(layer, j, cond=None):
        rows = source(layer, j)
        sized(core, cond, lambda w: remote(
            buf.at[rows, pl.ds(0, w)], buf.at[rows, pl.ds(0, w)], c_send.at[j], c_recv.at[layer, j],
            device(1)).wait_recv())

    def carry(layer, j, way, s, cond=None):
        rows = source(layer, j)
        src = (lambda w: own.at[:, columns(0, w)]) if s == 0 and j == 0 else (lambda w: buf.at[rows, pl.ds(0, w)])
        start_sized(lambda w: remote(src(w), buf.at[rows, pl.ds(0, w)], z_send.at[way, s, j],
                                     c_recv.at[layer, j], device(0, -out if way else out)), core, cond)

    def spread(j):
        if j:
            landed(z, j)
        carry(z, j, 0, 0, inner)
        carry(z, j, 1, 0)

    def relay(j):
        landed(z - out, j)
        carry(z - out, j, 0, 1, inner)
        landed(z + out, j, inner)
        carry(z + out, j, 1, 1, inner)

    def pair(layer, k, w):
        rows = pl.ds(pl.multiple_of((layer * 2 + 1 - x) * 2 * feat, 16), 2 * feat)
        c = chunks[k][0]
        return buf.at[rows, pl.ds(c, min(w, c + chunks[k][1]) - c)]

    def relay_far(j):
        landed(z - 2 * out, j)
        if j < 2:
            carry(z - 2 * out, j, 0, 2, inner)
        elif j == 3:
            for k in range(len(chunks)):
                start_sized(lambda w, k=k: remote(
                    pair(z - 2 * out, k, w), pair(z - 2 * out, k, w), last_send.at[k], last_recv.at[k],
                    device(0, out)), core, inner)

    def last_landed(k):
        sized(core, end, lambda w: remote(
            pair(z - 3 * out, k, w), pair(z - 3 * out, k, w), last_send.at[k], last_recv.at[k],
            device(1)).wait_recv())

    def part(slot, p):
        return docs.at[slot, pl.ds(*spans[p]), :]

    def send_docs(src_slot, p, dst_slot, r):
        start(lambda: remote(part(src_slot, p), part(dst_slot, p), d_send.at[dst_slot, p],
                             d_recv.at[dst_slot, p], device(r)))

    def send_ids(src_slot, dst_slot, r):
        start(lambda: remote(ids.at[src_slot], ids.at[dst_slot], i_send.at[dst_slot],
                             i_recv.at[dst_slot], device(r)))

    def have_docs(slot, *parts):
        for p in parts:
            remote(part(slot, p), part(slot, p), d_send.at[slot, p], d_recv.at[slot, p], device(1)).wait_recv()

    def have_ids(slot):
        remote(ids.at[slot], ids.at[slot], i_send.at[slot], i_recv.at[slot], device(1)).wait_recv()

    def share(slot, p):
        send_docs(slot, p, slot + 1, 1)

    spread(0)
    for j in (1, 2, 3):
        exchange(j)
    send_ids(0, 2, 2)
    for p in (0, 1, 2):
        send_docs(0, p, 2, 2)
    send_ids(0, 4, 4)
    for p in (1, 2, 0):
        send_docs(0, p, 4, 4)
    send_ids(0, 1, 1)
    for p in (0, 1, 2):
        send_docs(0, p, 1, 1)

    part_cols = jnp.where(core == 1, big, small) * 128
    first = (x * per + core * small) * 128
    base = doc * width + first
    reach = jnp.minimum(part_cols, width - first)
    lanes = lax.broadcasted_iota(jnp.int32, (rows_dev, 128), 1)
    lane = lax.broadcasted_iota(jnp.int32, (1, 128), 1)

    def prepare_ids(slot):
        rel = ids[slot] - base
        rel = jnp.where((rel >= 0) & (rel < reach), rel, -1)
        tall = jnp.broadcast_to(rel, (128, rows_dev)).T
        idb[slot] = jnp.where(tall >= 0, tall - lanes, -(2**20))

    buf[mine, pl.ds(0, small * 128)] = own[:, columns(0, small * 128)]
    if small < big:
        @pl.when(core == 1)
        def _():
            start_col = pl.multiple_of((x * per + 2 * small) * 128, 128)
            buf[mine, pl.ds(small * 128, 128)] = own[:, pl.ds(start_col, 128)]

    k1_at = pl.multiple_of(jnp.where(upper, depth - k1, 0), 256)
    k2_at = pl.multiple_of(jnp.where(upper, late, k1), 256)
    early_at = pl.multiple_of(jnp.where(upper, late, 0), 256)
    late_at = pl.multiple_of(jnp.where(upper, 0, depth - late), 256)

    def squares(at, count, c, w):
        w32 = buf[pl.ds(at, count), pl.ds(c, w)].astype(jnp.float32)
        return jnp.sum((w32 * w32).reshape(count // 8, 8, w), 0)

    def begin(slot, count, at, deep, add=False):
        rows = docs[pl.ds(slot, count), :, pl.ds(at, deep)].reshape(count * rows_dev, deep)
        prod = jnp.dot(rows, buf[pl.ds(at, deep), :], preferred_element_type=jnp.float32)
        prod = prod.reshape(count, rows_dev, wide)
        if add:
            acc[pl.ds(slot, count)] += prod
        else:
            acc[pl.ds(slot, count)] = prod

    spread(1)
    prepare_ids(0)
    spread(2)
    relay(0)
    spread(3)
    relay(1)
    have_docs(2, 0)
    send_docs(2, 0, 6, 4)
    share(2, 0)
    have_ids(4)
    send_ids(4, 6, 2)
    send_ids(4, 5, 1)
    have_ids(2)
    send_ids(2, 3, 1)
    relay(2)
    have_docs(4, 1)
    send_docs(4, 1, 6, 2)
    share(4, 1)
    have_docs(2, 1)
    share(2, 1)
    relay(3)
    relay_far(0)
    have_docs(4, 2)
    send_docs(4, 2, 6, 2)
    share(4, 2)
    have_docs(2, 2)
    share(2, 2)
    have_ids(6)
    send_ids(6, 7, 1)
    have_docs(1, 0, 1, 2)
    begin(0, 2, k1_at, k1)
    relay_far(1)
    for slot in (1, 2, 3, 4, 5, 6, 7):
        if slot in (1, 3, 5, 7):
            have_ids(slot)
        prepare_ids(slot)
    have_docs(4, 0)
    share(4, 0)
    relay_far(2)
    have_docs(3, 0, 1, 2)
    begin(2, 2, k1_at, k1)
    csq[...] = squares(k1_at, k1, 0, wide)
    relay_far(3)
    begin(0, 2, k2_at, k2, True)
    begin(2, 2, k2_at, k2, True)
    csq[...] += squares(k2_at, k2, 0, wide)
    have_docs(5, 1, 2, 0)
    begin(4, 2, early_at, k1 + k2)
    for p in (1, 2, 0):
        have_docs(6, p)
        share(6, p)
    begin(6, 1, early_at, k1 + k2)

    def scales(k):
        c, w = chunks[k]
        total = jnp.sum(csq[:, pl.ds(c, w)] + squares(late_at, late, c, w), 0, keepdims=True)
        scale[:, pl.ds(c, w)] = lax.rsqrt(total + epsilon)

    def stage(k, slot):
        c0, w = chunks[k]
        rows = docs[pl.ds(slot, 2), :, pl.ds(late_at, late)].reshape(2 * rows_dev, late)
        prod = jnp.dot(rows, buf[pl.ds(late_at, late), pl.ds(c0, w)], preferred_element_type=jnp.float32)
        for half in (0, 1):
            for r in range(0, rows_dev, ROWS):
                rs = pl.ds(r, ROWS)
                at = half * rows_dev + r
                if k:
                    top, hit = mx[slot + half, rs, :], ch[slot + half, rs, :]
                else:
                    top = jnp.full((ROWS, 128), -3.0e38, jnp.float32)
                    hit = jnp.zeros((ROWS, 128), jnp.float32)
                where_id = idb[slot + half, rs, :]
                for c in range(0, w, 128):
                    cols = pl.ds(c0 + c, 128)
                    v = (acc[slot + half, rs, cols] + prod[at:at + ROWS, c:c + 128]) * scale[:, cols]
                    hit = jnp.where(where_id == c0 + c, v, hit)
                    if c0 + c + 128 > small * 128 or (c0 + c + 128 == small * 128 and small == big):
                        v = jnp.where(lane < reach - (c0 + c), v, -3.0e38)
                    top = jnp.maximum(top, v)
                mx[slot + half, rs, :] = top
                ch[slot + half, rs, :] = hit

    def reduced(slot):
        return (jnp.max(mx[slot].T, 0, keepdims=True), jnp.sum(ch[slot].T, 0, keepdims=True))

    def give(slot):
        best, chosen = reduced(slot)
        res[slot, 0:1, :] = best
        res[slot, 1:2, :] = chosen
        start(lambda: remote(res.at[slot], got.at[slot], r_send.at[slot], r_recv.at[slot], device(slot)))

    landed(z - 3 * out, 0, end)
    landed(z - 3 * out, 1, end)
    final = len(chunks) - 1
    for k in range(final):
        last_landed(k)
        scales(k)
        for slot in (0, 2, 4):
            stage(k, slot)
        if k == 0:
            have_docs(7, 1, 2, 0)
            begin(7, 1, early_at, k1 + k2)
        stage(k, 6)
    last_landed(final)
    scales(final)
    stage(final, 6)
    stage(final, 2)
    give(7)
    give(6)
    stage(final, 4)
    give(3)
    give(2)
    stage(final, 0)
    give(5)
    give(4)
    give(1)
    best, chosen = reduced(0)
    x32 = docs[0].astype(jnp.float32)
    sq = x32 * x32
    total = sq[:, 0:128]
    for c in range(128, depth, 128):
        total = total + sq[:, c:c + 128]
    scale_x = lax.rsqrt(jnp.sum(total.T, 0, keepdims=True) + epsilon)
    for slot in (1, 4, 5, 2, 3, 6, 7):
        remote(res.at[slot], got.at[slot], r_send.at[slot], r_recv.at[slot], device(slot)).wait_recv()
        best = jnp.maximum(best, got[slot, 0:1, :])
        chosen = chosen + got[slot, 1:2, :]
    near_out[...] = best * scale_x
    chosen_out[...] = chosen * scale_x
    for entry in pending:
        if len(entry) == 2:
            cond, make = entry
            when(cond, lambda: make().wait_send())
        else:
            c, cond, make = entry
            sized(c, cond, lambda w: make(w).wait_send())


def by_layers(docs, centroids, assigned):
    nz = lax.axis_size("clu") // 4
    rows_dev, depth = docs.shape
    width, feat = centroids.shape
    tiles = -(-width // 128)
    wide = (tiles // 2 - tiles // 4) * 128
    any_space = pl.BlockSpec(memory_space=pl.ANY)
    vmem = pl.BlockSpec(memory_space=pltpu.VMEM)
    dma = pltpu.SemaphoreType.DMA
    line = pltpu.VMEM((1, rows_dev), jnp.float32)
    near, chosen = pl.pallas_call(
        functools.partial(layer_kernel, nz, feat),
        out_shape=(line, line),
        in_specs=[any_space] * 3,
        out_specs=(vmem, vmem),
        scratch_shapes=[
            pltpu.VMEM((feat, tiles * 128), jnp.bfloat16),
            pltpu.VMEM((feat, width % 128 or 128), jnp.bfloat16),
            pltpu.VMEM((depth, wide), jnp.bfloat16),
            pltpu.VMEM((8, rows_dev, depth), jnp.bfloat16),
            pltpu.VMEM((8, 1, rows_dev), jnp.int32),
            pltpu.VMEM((8, rows_dev, wide), jnp.float32),
            pltpu.VMEM((8, rows_dev, 128), jnp.int32),
            pltpu.VMEM((8, rows_dev, 128), jnp.float32),
            pltpu.VMEM((8, rows_dev, 128), jnp.float32),
            pltpu.VMEM((8, wide), jnp.float32),
            pltpu.VMEM((1, wide), jnp.float32),
            pltpu.VMEM((8, 2, rows_dev), jnp.float32),
            pltpu.VMEM((8, 2, rows_dev), jnp.float32),
            dma((4,)),
            dma((4,)), dma((nz, 4)), dma((2, 3, 4)), dma((-(-wide // 256),)), dma((-(-wide // 256),)),
            dma((8, 3)), dma((8, 3)), dma((8,)), dma((8,)), dma((8,)), dma((8,)),
        ],
        compiler_params=pltpu.CompilerParams(collective_id=0, has_side_effects=True),
        name="layer_distances",
    )(docs, centroids.T, assigned.reshape(1, rows_dev))
    return 1.0 - near.reshape(rows_dev), 1.0 - chosen.reshape(rows_dev)


def fits_layers(docs, centroids):
    tiles = -(-centroids.shape[0] // 128)
    n_clu, feat = lax.axis_size("clu"), centroids.shape[1]
    return (lax.axis_size("doc") == 2 and n_clu == 16 and tiles % 2 == 0 and tiles >= 4
            and feat % 16 == 0 and docs.shape[0] % 128 == 0 and docs.shape[1] % 256 == 0
            and docs.shape[1] == n_clu * feat and 8 * feat >= 256)


def on_device(docs, centroids, assigned):
    if fits_layers(docs, centroids):
        return by_layers(docs, centroids, assigned)
    n_clu, nd = lax.axis_size("clu"), lax.axis_size("doc")
    n = n_clu // 2
    rows_dev, depth = docs.shape
    width, feat = centroids.shape
    fp = (feat + 15) // 16 * 16
    cents = centroids.T
    if fp != feat:
        cents = jnp.pad(cents, ((0, fp - feat), (0, 0)))
    rows = nd * rows_dev
    any_space = pl.BlockSpec(memory_space=pl.ANY)
    vmem = pl.BlockSpec(memory_space=pltpu.VMEM)
    dma = pltpu.SemaphoreType.DMA
    hops = n // 2
    line = jax.ShapeDtypeStruct((1, rows_dev), jnp.float32)
    near, chosen = pl.pallas_call(
        functools.partial(kernel, n, nd, feat),
        out_shape=(line, line),
        in_specs=[any_space] * 3,
        out_specs=(vmem, vmem),
        scratch_shapes=[
            pltpu.VMEM((n_clu * fp, width), jnp.bfloat16),
            pltpu.VMEM((nd, rows_dev, depth), jnp.bfloat16),
            pltpu.VMEM((nd, 1, rows_dev), jnp.int32),
            pltpu.VMEM((rows, (n - 3) * 2 * fp), jnp.bfloat16),
            pltpu.VMEM((rows, 4 * fp), jnp.bfloat16),
            pltpu.VMEM((rows, 2 * fp), jnp.bfloat16),
            pltpu.VMEM((rows, width), jnp.float32),
            pltpu.VMEM((rows, 128), jnp.int32),
            pltpu.VMEM((rows, 128), jnp.float32),
            pltpu.VMEM((rows, 128), jnp.float32),
            pltpu.VMEM((8, width), jnp.float32),
            pltpu.VMEM((1, width), jnp.float32),
            pltpu.VMEM((nd, 2, rows_dev), jnp.float32),
            pltpu.VMEM((nd, 2, rows_dev), jnp.float32),
            dma((3,)),
            dma((2, hops, PIECES)),
            dma((n, PIECES)),
            dma((n, 2, PIECES)),
            dma((nd,)), dma((nd,)), dma((nd,)), dma((nd,)), dma((nd,)), dma((nd,)),
        ],
        compiler_params=pltpu.CompilerParams(collective_id=0, has_side_effects=True),
        name="ring_distances",
    )(docs, cents, assigned.reshape(1, rows_dev))
    return 1.0 - near.reshape(rows_dev), 1.0 - chosen.reshape(rows_dev)


def solution(mesh):
    placed = (P(("clu", "doc"), None), P("doc", "clu"), P(("clu", "doc")))
    return jax.shard_map(
        on_device,
        mesh=mesh,
        in_specs=placed,
        out_specs=(P(("clu", "doc")), P(("clu", "doc"))),
        check_vma=False,
    )
```

```python
import functools

import jax
import jax.numpy as jnp
from jax import lax
from jax.experimental import pallas as pl
from jax.experimental.pallas import tpu as pltpu
from jax.sharding import PartitionSpec as P

epsilon = 1e-06
PIECES = 4
ROWS = 64
GROUP = 32
MESH = pl.DeviceIdType.MESH


def chip_at(pos, n):
    half = n // 2
    return jnp.where(pos < half, 2 * pos, 2 * (n - 1 - pos) + 1)


def cut(width):
    tiles = (width + 127) // 128
    ends = [min(-(-tiles * (c + 1) // PIECES) * 128, width) for c in range(PIECES)]
    return tuple((a, b - a) for a, b in zip([0] + ends[:-1], ends))


def kernel(n, nd, feat, docs_in, cents_in, ids_in, near_out, chosen_out,
           buf, docs_all, ids_all, dp_a, dp_b, dp_c, acc, idb, mx, ch, csq, scale, res, got,
           local_sem, ring_send, pair_send, recv, docs_send, docs_recv, ids_send, ids_recv,
           res_send, res_recv):
    hops = n // 2
    fp = cents_in.shape[0]
    width = cents_in.shape[1]
    rows_dev = docs_in.shape[0]
    chunks = cut(width)
    half = len(chunks) // 2

    clu, doc = lax.axis_index("clu"), lax.axis_index("doc")
    core, chip = lax.rem(clu, 2), lax.div(clu, 2)
    z, x = lax.div(chip, 2), lax.rem(chip, 2)
    pos = jnp.where(x == 0, z, n - 1 - z)
    right = chip_at(lax.rem(pos + 1, n), n) * 2 + core
    left = chip_at(lax.rem(pos + n - 1, n), n) * 2 + core
    partner = chip * 2 + (1 - core)

    own_c = pltpu.make_async_copy(cents_in, buf.at[pl.ds(0, fp), :], local_sem.at[0])
    own_d = pltpu.make_async_copy(docs_in, docs_all.at[0], local_sem.at[1])
    own_i = pltpu.make_async_copy(ids_in, ids_all.at[0], local_sem.at[2])
    own_c.start()
    own_d.start()
    own_i.start()

    barrier = pltpu.get_barrier_semaphore()
    for peer in (left, right, partner):
        pl.semaphore_signal(barrier, inc=1, device_id={"clu": peer}, device_id_type=MESH)
    for k in range(1, nd):
        pl.semaphore_signal(barrier, inc=1, device_id={"doc": lax.rem(doc + k, nd)}, device_id_type=MESH)
    pl.semaphore_wait(barrier, 3 + nd - 1)

    def slot(way, h):
        if h == 0:
            return 0
        if h == hops:
            return n - 1
        return 2 * h - 1 if way == 0 else 2 * h

    def piece(s, m, c):
        return buf.at[pl.ds((2 * s + m) * fp, fp), pl.ds(*chunks[c])]

    def reach(way, c):
        return hops if way == c // half else hops - 1

    sent = []

    def ring(way, h, c):
        s, t = slot(way, h), slot(way, h + 1)
        copy = pltpu.make_async_remote_copy(
            src_ref=piece(s, 0, c), dst_ref=piece(t, 0, c),
            send_sem=ring_send.at[way, h, c], recv_sem=recv.at[t, 0, c],
            device_id={"clu": right if way == 0 else left}, device_id_type=MESH)
        copy.start()
        sent.append(copy)

    def share(s, c):
        copy = pltpu.make_async_remote_copy(
            src_ref=piece(s, 0, c), dst_ref=piece(s, 1, c),
            send_sem=pair_send.at[s, c], recv_sem=recv.at[s, 1, c],
            device_id={"clu": partner}, device_id_type=MESH)
        copy.start()
        sent.append(copy)

    def landed(s, m, c):
        pltpu.make_async_remote_copy(
            src_ref=piece(s, m, c), dst_ref=piece(s, m, c),
            send_sem=pair_send.at[s, c], recv_sem=recv.at[s, m, c],
            device_id={"clu": partner}, device_id_type=MESH).wait_recv()

    own_c.wait()
    for i in range(PIECES):
        ring(0, 0, i)
        ring(1, 0, (i + half) % PIECES)
    for c in range(PIECES):
        share(0, c)
    own_d.wait()
    own_i.wait()
    doc_copies = []
    for k in range(1, nd):
        mate = lax.rem(doc + k, nd)
        for ref, ss, rs in ((ids_all, ids_send, ids_recv), (docs_all, docs_send, docs_recv)):
            copy = pltpu.make_async_remote_copy(
                src_ref=ref.at[0], dst_ref=ref.at[k], send_sem=ss.at[k], recv_sem=rs.at[k],
                device_id={"doc": mate}, device_id_type=MESH)
            copy.start()
            doc_copies.append(copy)

    def owner(s):
        if s == 0:
            p = pos
        elif s == n - 1:
            p = pos + hops
        elif s % 2:
            p = pos + n - (s + 1) // 2
        else:
            p = pos + s // 2
        return chip_at(lax.rem(p, n), n)

    ranges = ((0, n - 3), (n - 3, n - 1), (n - 1, n))
    spread = (dp_a, dp_b, dp_c)

    def permute(k):
        rows = docs_all[k]
        for (first, last), out in zip(ranges, spread):
            wide = out.shape[1]
            lane = lax.broadcasted_iota(jnp.int32, (1, wide), 1)
            target = jnp.full((1, wide), -1, jnp.int32)
            for s in range(first, last):
                chip_s = owner(s)
                for m in (0, 1):
                    part = chip_s * 2 + (core if m == 0 else 1 - core)
                    start = (2 * (s - first) + m) * fp
                    inside = (lane >= start) & (lane < start + feat)
                    target = jnp.where(inside, lane - start + part * feat, target)
            source = lax.broadcasted_iota(jnp.int32, (rows.shape[1], wide), 0)
            mover = jnp.where(source == target, 1.0, 0.0).astype(jnp.bfloat16)
            out[pl.ds(k * rows_dev, rows_dev), :] = jnp.dot(
                rows, mover, preferred_element_type=jnp.float32).astype(jnp.bfloat16)

    def prepare_ids(k):
        base = doc * width
        ids = ids_all[k] - base
        ids = jnp.where((ids >= 0) & (ids < width), ids, -1)
        full = jnp.broadcast_to(ids, (128, rows_dev)).T
        lanes = lax.broadcasted_iota(jnp.int32, (rows_dev, 128), 1)
        idb[pl.ds(k * rows_dev, rows_dev), :] = jnp.where(full >= 0, full - lanes, -(2**20))

    def phase(index, c):
        first, last = ranges[index]
        start, depth = 2 * first * fp, 2 * (last - first) * fp
        cols = pl.ds(*chunks[c])
        block = buf[pl.ds(start, depth), cols]
        prod = jnp.dot(spread[index][...], block, preferred_element_type=jnp.float32)
        w32 = block.astype(jnp.float32)
        sq = jnp.sum((w32 * w32).reshape(depth // 8, 8, chunks[c][1]), 0)
        if index == 0:
            acc[:, cols] = prod
            csq[:, cols] = sq
        else:
            acc[:, cols] += prod
            csq[:, cols] += sq

    tail = pl.ds(2 * (n - 1) * fp, 2 * fp)

    def finish_scale(c):
        cols = pl.ds(*chunks[c])
        w32 = buf[tail, cols].astype(jnp.float32)
        sq = jnp.sum((w32 * w32).reshape(2 * fp // 8, 8, chunks[c][1]), 0) + csq[:, cols]
        scale[:, cols] = lax.rsqrt(jnp.sum(sq, 0, keepdims=True) + epsilon)

    def final(k, c):
        start, wide = chunks[c]
        prod = jnp.dot(dp_c[pl.ds(k * rows_dev, rows_dev), :], buf[tail, pl.ds(start, wide)],
                       preferred_element_type=jnp.float32)
        for r in range(0, rows_dev, ROWS):
            rs = pl.ds(k * rows_dev + r, ROWS)
            top, hit = mx[rs, :], ch[rs, :]
            ids = idb[rs, :]
            for a in range(0, wide, 128):
                w = min(128, wide - a)
                cols = pl.ds(start + a, w)
                v = (acc[rs, cols] + prod[r:r + ROWS, a:a + w]) * scale[:, cols]
                if w == 128:
                    top = jnp.maximum(top, v)
                    hit = jnp.where(ids == start + a, v, hit)
                else:
                    mx[rs, :] = top
                    ch[rs, :] = hit
                    mx[rs, pl.ds(0, w)] = jnp.maximum(mx[rs, pl.ds(0, w)], v)
                    ch[rs, pl.ds(0, w)] = jnp.where(idb[rs, pl.ds(0, w)] == start + a, v, ch[rs, pl.ds(0, w)])
            if wide % 128 == 0:
                mx[rs, :] = top
                ch[rs, :] = hit

    def reduced(k):
        rs = pl.ds(k * rows_dev, rows_dev)
        return (jnp.max(mx[rs, :].T, 0, keepdims=True), jnp.sum(ch[rs, :].T, 0, keepdims=True))

    mx[...] = jnp.full(mx.shape, -3.0e38, jnp.float32)
    ch[...] = jnp.zeros(ch.shape, jnp.float32)
    permute(0)
    prepare_ids(0)
    wide = docs_all[0].astype(jnp.float32)
    squares = wide * wide
    total = squares[:, 0:128]
    for a in range(128, wide.shape[1], 128):
        total = total + squares[:, a:a + 128]
    scale_x = lax.rsqrt(jnp.sum(total.T, 0, keepdims=True) + epsilon)

    def step(way, h, c):
        s = slot(way, h)
        landed(s, 0, c)
        if h < reach(way, c):
            ring(way, h, c)
        share(s, c)

    def pair(h, i):
        step(0, h, i)
        step(1, h, (i + half) % PIECES)

    def partners(slots, c):
        for s in slots:
            landed(s, 1, c)

    early, late = range(n - 3), (n - 3, n - 2)
    order = [j // 2 + half * (j % 2) for j in range(PIECES)]
    for h in range(1, hops):
        for i in range(PIECES):
            pair(h, i)
            if h == hops - 2 and i == half:
                for copy in doc_copies:
                    copy.wait()
                for k in range(1, nd):
                    permute(k)
                    prepare_ids(k)
            if h == hops - 1:
                c = order[i]
                partners(early, c)
                phase(0, c)
    for c in order[:half]:
        partners(late, c)
        phase(1, c)
    for i in range(half):
        for way in (0, 1):
            c = i + half * way
            landed(n - 1, 0, c)
            share(n - 1, c)
    for c in order[half:]:
        partners(late, c)
        phase(1, c)
    for c in order[:-2]:
        landed(n - 1, 1, c)
        finish_scale(c)
        for k in range(nd):
            final(k, c)
    for c in order[-2:]:
        landed(n - 1, 1, c)
        finish_scale(c)

    returns = []
    for k in range(1, nd):
        for c in order[-2:]:
            final(k, c)
        best, chosen = reduced(k)
        res[k, 0:1, :] = best
        res[k, 1:2, :] = chosen
        copy = pltpu.make_async_remote_copy(
            src_ref=res.at[k], dst_ref=got.at[k], send_sem=res_send.at[k], recv_sem=res_recv.at[k],
            device_id={"doc": lax.rem(doc + nd - k, nd)}, device_id_type=MESH)
        copy.start()
        returns.append(copy)
    for c in order[-2:]:
        final(0, c)
    best, chosen = reduced(0)
    for k in range(1, nd):
        returns[k - 1].wait()
        best = jnp.maximum(best, got[k, 0:1, :])
        chosen = chosen + got[k, 1:2, :]
    near_out[...] = best * scale_x
    chosen_out[...] = chosen * scale_x
    for copy in sent:
        copy.wait_send()


def layer_kernel(nz, feat, docs_in, cents_in, ids_in, near_out, chosen_out,
                 own, raw, buf, docs, ids, turned, acc, idb, mx, ch, csq, scale, res, got,
                 local_sem, send_sem, c_recv, last_recv, d_recv, i_recv, r_recv):
    width = cents_in.shape[1]
    rows_dev, depth = docs_in.shape
    tiles = own.shape[1] // 128
    per = tiles // 2
    small = per // 2
    big = per - small
    wide = big * 128
    full = width // 128 * 128
    late = -(-4 * feat // 256) * 256
    k1 = 8 * feat // 256 * 256
    k2 = depth - late - k1
    a = rows_dev * 5 // 16 // 16 * 16
    b = (rows_dev - a) // 32 * 16
    spans = ((0, a), (a, b), (a + b, rows_dev - a - b))
    chunks = tuple((c, min(256, wide - c)) for c in range(0, wide, 256))

    clu, doc = lax.axis_index("clu"), lax.axis_index("doc")
    core, chip = lax.rem(clu, 2), lax.div(clu, 2)
    z, x = lax.div(chip, 2), lax.rem(chip, 2)
    upper = z >= nz // 2
    out = jnp.where(upper, 1, -1)
    end = (z == 0) | (z == nz - 1)
    inner = jnp.logical_not(end)

    def device(r, dz=0):
        dx, dy, dc = r // 4, r // 2 % 2, r % 2
        there = ((z + dz) * 2 + (1 - x if dx else x)) * 2 + (1 - core if dc else core)
        return {"clu": there, "doc": 1 - doc if dy else doc}

    def when(cond, body):
        if cond is None:
            body()
        else:
            pl.when(cond)(body)

    def both(p, q):
        return q if p is None else p if q is None else p & q

    sizes = ((None, big),) if big == small else ((1, big), (0, small))

    def sized(c, cond, body):
        for value, count in sizes:
            when(both(cond, None if value is None else c == value), functools.partial(body, count * 128))

    own_copy = pltpu.make_async_copy(cents_in.at[:, pl.ds(0, full)], own.at[:, pl.ds(0, full)], local_sem.at[0])
    docs_copy = pltpu.make_async_copy(docs_in, docs.at[0], local_sem.at[1])
    ids_copy = pltpu.make_async_copy(ids_in, ids.at[0], local_sem.at[2])
    own_copy.start()
    if full < width:
        raw_copy = pltpu.make_async_copy(cents_in.at[:, pl.ds(full, width - full)], raw, local_sem.at[3])
        raw_copy.start()
    docs_copy.start()
    ids_copy.start()

    barrier = pltpu.get_barrier_semaphore()

    def greet(to):
        pl.semaphore_signal(barrier, inc=1, device_id=to, device_id_type=MESH)

    pl.when(inner)(lambda: greet(device(0, out)))
    greet(device(0, -out))
    for r in (4, 5, 2, 1):
        greet(device(r))
    if small < big:
        @pl.when(core == 0)
        def _():
            buf[:, pl.ds(small * 128, 128)] = jnp.zeros((buf.shape[0], 128), buf.dtype)
    if full < width:
        raw_copy.wait()
        own[:, pl.ds(full, 128)] = jnp.concatenate(
            [raw[...], jnp.zeros((feat, full + 128 - width), raw.dtype)], axis=1)
    own_copy.wait()
    docs_copy.wait()
    ids_copy.wait()
    pl.semaphore_wait(barrier, 5 + inner.astype(jnp.int32))

    outward, inward, traded, doc_sent, id_sent, result_sent = (send_sem.at[i] for i in range(6))

    def start(make, cond=None):
        when(cond, lambda: make().start())

    def start_sized(make, c, cond=None):
        sized(c, cond, lambda w: make(w).start())

    def remote(src, dst, ss, rs, to):
        return pltpu.make_async_remote_copy(
            src_ref=src, dst_ref=dst, send_sem=ss, recv_sem=rs, device_id=to, device_id_type=MESH)

    near = (0, 1, 4, 5)

    def source(layer, j):
        r = near[j]
        there = (layer * 2 + (1 - x if r // 4 else x)) * 2 + (1 - core if r % 2 else core)
        return pl.ds(pl.multiple_of(there * feat, 16), feat)

    def columns(r, w):
        xd = 1 - x if r // 4 else x
        cd = 1 - core if r % 2 else core
        return pl.ds(pl.multiple_of((xd * per + cd * small) * 128, 128), w)

    mine = source(z, 0)

    def exchange(j):
        r = near[j]
        start_sized(lambda w: remote(own.at[:, columns(r, w)], buf.at[mine, pl.ds(0, w)],
                                     traded, c_recv.at[z, j], device(r)),
                    1 - core if r % 2 else core)

    def landed(layer, j, cond=None):
        rows = source(layer, j)
        sized(core, cond, lambda w: remote(
            buf.at[rows, pl.ds(0, w)], buf.at[rows, pl.ds(0, w)], traded, c_recv.at[layer, j],
            device(1)).wait_recv())

    def carry(layer, j, way, s, cond=None):
        rows = source(layer, j)
        src = (lambda w: own.at[:, columns(0, w)]) if s == 0 and j == 0 else (lambda w: buf.at[rows, pl.ds(0, w)])
        start_sized(lambda w: remote(src(w), buf.at[rows, pl.ds(0, w)], inward if way else outward,
                                     c_recv.at[layer, j], device(0, -out if way else out)), core, cond)

    def spread(j):
        if j:
            landed(z, j)
        carry(z, j, 0, 0, inner)
        carry(z, j, 1, 0)

    def relay(j):
        landed(z - out, j)
        carry(z - out, j, 0, 1, inner)
        landed(z + out, j, inner)
        carry(z + out, j, 1, 1, inner)

    def pair(layer, k, w):
        rows = pl.ds(pl.multiple_of((layer * 2 + 1 - x) * 2 * feat, 16), 2 * feat)
        c = chunks[k][0]
        return buf.at[rows, pl.ds(c, min(w, c + chunks[k][1]) - c)]

    def relay_far(j):
        landed(z - 2 * out, j)
        if j < 2:
            carry(z - 2 * out, j, 0, 2, inner)
        elif j == 3:
            for k in range(len(chunks)):
                start_sized(lambda w, k=k: remote(
                    pair(z - 2 * out, k, w), pair(z - 2 * out, k, w), outward, last_recv.at[k],
                    device(0, out)), core, inner)

    def last_landed(k):
        sized(core, end, lambda w: remote(
            pair(z - 3 * out, k, w), pair(z - 3 * out, k, w), outward, last_recv.at[k],
            device(1)).wait_recv())

    ahead = {(1, 0): 0, (1, 1): 0, (1, 2): 0, (3, 0): 1, (3, 1): 1, (3, 2): 1, (5, 0): 2, (5, 1): 2, (5, 2): 2,
             (7, 0): 3, (7, 1): 3, (7, 2): 3, (2, 0): 4, (2, 1): 5, (2, 2): 5, (4, 0): 6, (4, 1): 7, (4, 2): 8,
             (6, 0): 9, (6, 1): 10, (6, 2): 11}
    id_at = {1: 0, 3: 0, 5: 0, 7: 0, 2: 1, 4: 2, 6: 3}

    def part(slot, *parts):
        first, last = spans[parts[0]], spans[parts[-1]]
        return docs.at[slot, pl.ds(first[0], last[0] + last[1] - first[0]), :]

    def send_docs(src_slot, dst_slot, r, *parts):
        start(lambda: remote(part(src_slot, *parts), part(dst_slot, *parts), doc_sent,
                             d_recv.at[ahead[dst_slot, parts[0]]], device(r)))

    def send_ids(src_slot, dst_slot, r):
        start(lambda: remote(ids.at[src_slot], ids.at[dst_slot], id_sent, i_recv.at[id_at[dst_slot]], device(r)))

    def have_docs(slot, *parts):
        remote(part(slot, *parts), part(slot, *parts), doc_sent, d_recv.at[ahead[slot, parts[0]]],
               device(1)).wait_recv()

    def have_ids(slot):
        some = ids.at[pl.ds(0, 4)] if slot % 2 else ids.at[slot]
        remote(some, some, id_sent, i_recv.at[id_at[slot]], device(1)).wait_recv()

    def share(slot, *parts):
        send_docs(slot, slot + 1, 1, *parts)

    spread(0)
    for j in (1, 2, 3):
        exchange(j)
    send_ids(0, 2, 2)
    send_docs(0, 2, 2, 0)
    send_docs(0, 2, 2, 1, 2)
    send_ids(0, 4, 4)
    for p in (1, 2, 0):
        send_docs(0, 4, 4, p)
    send_ids(0, 1, 1)
    send_docs(0, 1, 1, 0, 1, 2)

    part_cols = jnp.where(core == 1, big, small) * 128
    first = (x * per + core * small) * 128
    base = doc * width + first
    reach = jnp.minimum(part_cols, width - first)
    down = lax.broadcasted_iota(jnp.int32, (GROUP, 128), 0)

    def prepare_ids(slot):
        rel = ids[slot] - base
        rel = jnp.where((rel >= 0) & (rel < reach), rel, -(2**20))
        tall = jnp.broadcast_to(rel, (GROUP, rows_dev))
        idb[:, pl.ds(slot * rows_dev, rows_dev)] = tall - lax.broadcasted_iota(jnp.int32, (GROUP, rows_dev), 0)

    buf[mine, pl.ds(0, small * 128)] = own[:, columns(0, small * 128)]
    if small < big:
        @pl.when(core == 1)
        def _():
            start_col = pl.multiple_of((x * per + 2 * small) * 128, 128)
            buf[mine, pl.ds(small * 128, 128)] = own[:, pl.ds(start_col, 128)]

    k1_at = pl.multiple_of(jnp.where(upper, depth - k1, 0), 256)
    k2_at = pl.multiple_of(jnp.where(upper, late, k1), 256)
    late_at = pl.multiple_of(jnp.where(upper, 0, depth - late), 256)
    starts = (k1_at, k2_at, late_at)

    def squares(i, c, w):
        w32 = buf[pl.ds(starts[i], 256), pl.ds(c, w)].astype(jnp.float32)
        return jnp.sum((w32 * w32).reshape(32, 8, w), 0)

    def turn(i, c, w):
        turned[i, pl.ds(c, w), :] = buf[pl.ds(starts[i], 256), pl.ds(c, w)].T

    def gather(i):
        for c, w in chunks:
            turn(i, c, w)
        csq[...] = squares(i, 0, wide) + (csq[...] if i else 0.0)

    def times(i, c, w, slot, count):
        rows = docs[pl.ds(slot, count), :, pl.ds(starts[i], 256)].reshape(count * rows_dev, 256)
        return lax.dot_general(turned[i, pl.ds(c, w), :], rows, (((1,), (1,)), ((), ())),
                               preferred_element_type=jnp.float32)

    def begin(slot, count, *phases):
        where_docs = pl.ds(slot * rows_dev, count * rows_dev)
        prod = times(phases[0], 0, wide, slot, count)
        for i in phases[1:]:
            prod = prod + times(i, 0, wide, slot, count)
        if phases[0]:
            acc[:, where_docs] += prod
        else:
            acc[:, where_docs] = prod

    spread(1)
    prepare_ids(0)
    spread(2)
    relay(0)
    spread(3)
    relay(1)
    have_docs(2, 0)
    send_docs(2, 6, 4, 0)
    have_ids(4)
    send_ids(4, 6, 2)
    send_ids(4, 5, 1)
    have_ids(2)
    send_ids(2, 3, 1)
    relay(2)
    have_docs(4, 1)
    send_docs(4, 6, 2, 1)
    have_docs(2, 1, 2)
    share(2, 0, 1, 2)
    relay(3)
    relay_far(0)
    have_docs(4, 2)
    send_docs(4, 6, 2, 2)
    have_ids(6)
    send_ids(6, 7, 1)
    have_docs(1, 0, 1, 2)
    gather(0)
    begin(0, 2, 0)
    relay_far(1)
    have_ids(1)
    for slot in (1, 2, 3, 4, 5, 6, 7):
        prepare_ids(slot)
    have_docs(4, 0)
    share(4, 0, 1, 2)
    relay_far(2)
    have_docs(3, 0, 1, 2)
    begin(2, 2, 0)
    relay_far(3)
    gather(1)
    begin(0, 2, 1)
    begin(2, 2, 1)
    have_docs(5, 0, 1, 2)
    begin(4, 2, 0, 1)
    for p in (1, 2, 0):
        have_docs(6, p)
    share(6, 0, 1, 2)
    begin(6, 1, 0, 1)

    def scales(k):
        c, w = chunks[k]
        total = jnp.sum(csq[:, pl.ds(c, w)] + squares(2, c, w), 0, keepdims=True)
        scale[pl.ds(c, w), :] = jnp.broadcast_to(lax.rsqrt(total + epsilon), (128, w)).T

    def stage(k, slot, count):
        c0, w = chunks[k]
        prod = times(2, c0, w, slot, count)
        for d in range(0, count * rows_dev, 128):
            at = pl.ds(slot * rows_dev + d, 128)
            if k:
                top, hit = mx[:, at], ch[:, at]
            else:
                top = jnp.full((GROUP, 128), -3.0e38, jnp.float32)
                hit = jnp.zeros((GROUP, 128), jnp.float32)
            where_id = idb[:, at]
            for c in range(0, w, GROUP):
                rows = pl.ds(c0 + c, GROUP)
                v = (acc[rows, at] + prod[c:c + GROUP, d:d + 128]) * scale[rows, :]
                hit = jnp.where(where_id == c0 + c, v, hit)
                if c0 + c + 128 > small * 128:
                    v = jnp.where(down < reach - (c0 + c), v, -3.0e38)
                top = jnp.maximum(top, v)
            mx[:, at] = top
            ch[:, at] = hit

    def reduced(slot):
        at = pl.ds(slot * rows_dev, rows_dev)
        return jnp.max(mx[:, at], 0, keepdims=True), jnp.sum(ch[:, at], 0, keepdims=True)

    def give(slot):
        best, chosen = reduced(slot)
        res[slot, 0:1, :] = best
        res[slot, 1:2, :] = chosen
        remote(res.at[slot], got.at[slot], result_sent, r_recv, device(slot)).start()

    x32 = docs[0].astype(jnp.float32)
    sq = x32 * x32
    total = sq[:, 0:128]
    for c in range(128, depth, 128):
        total = total + sq[:, c:c + 128]
    scale_x = lax.rsqrt(jnp.sum(total.T, 0, keepdims=True) + epsilon)

    landed(z - 3 * out, 0, end)
    landed(z - 3 * out, 1, end)
    final = len(chunks) - 1
    for k in range(final):
        last_landed(k)
        turn(2, *chunks[k])
        scales(k)
        for slot in (0, 2, 4):
            stage(k, slot, 2)
        if k == 0:
            have_docs(7, 0, 1, 2)
            begin(7, 1, 0, 1)
        stage(k, 6, 2)
    last_landed(final)
    turn(2, *chunks[final])
    scales(final)
    stage(final, 6, 2)
    stage(final, 2, 2)
    give(7)
    give(6)
    stage(final, 4, 2)
    give(3)
    give(2)
    stage(final, 0, 2)
    give(5)
    give(4)
    give(1)
    best, chosen = reduced(0)
    everyone = pl.ds(1, 7)
    remote(got.at[everyone], got.at[everyone], result_sent, r_recv, device(1)).wait_recv()
    for slot in range(1, 8):
        best = jnp.maximum(best, got[slot, 0:1, :])
        chosen = chosen + got[slot, 1:2, :]
    near_out[...] = best * scale_x
    chosen_out[...] = chosen * scale_x

    def sent(ref, sem):
        remote(ref, ref, sem, r_recv, device(1)).wait_send()

    sent(res.at[everyone], result_sent)
    sent(docs.at[everyone], doc_sent)
    sent(ids.at[everyone], id_sent)
    layer = 4 * feat
    sized(core, inner, lambda w: sent(buf.at[pl.ds(0, 3 * layer), pl.ds(0, w)], outward))
    sized(core, inner, lambda w: sent(buf.at[pl.ds(0, 2 * layer), pl.ds(0, w)], inward))
    sized(core, end, lambda w: sent(buf.at[pl.ds(0, layer), pl.ds(0, w)], inward))
    sized(core, None, lambda w: sent(own.at[:, pl.ds(0, 2 * per * 128 - w)], traded))


def by_layers(docs, centroids, assigned):
    nz = lax.axis_size("clu") // 4
    rows_dev, depth = docs.shape
    width, feat = centroids.shape
    tiles = -(-width // 128)
    wide = (tiles // 2 - tiles // 4) * 128
    any_space = pl.BlockSpec(memory_space=pl.ANY)
    vmem = pl.BlockSpec(memory_space=pltpu.VMEM)
    dma = pltpu.SemaphoreType.DMA
    line = pltpu.VMEM((1, rows_dev), jnp.float32)
    near, chosen = pl.pallas_call(
        functools.partial(layer_kernel, nz, feat),
        out_shape=(line, line),
        in_specs=[any_space] * 3,
        out_specs=(vmem, vmem),
        scratch_shapes=[
            pltpu.VMEM((feat, tiles * 128), jnp.bfloat16),
            pltpu.VMEM((feat, width % 128 or 128), jnp.bfloat16),
            pltpu.VMEM((depth, wide), jnp.bfloat16),
            pltpu.VMEM((8, rows_dev, depth), jnp.bfloat16),
            pltpu.VMEM((8, 1, rows_dev), jnp.int32),
            pltpu.VMEM((3, wide, 256), jnp.bfloat16),
            pltpu.VMEM((wide, 8 * rows_dev), jnp.float32),
            pltpu.VMEM((GROUP, 8 * rows_dev), jnp.int32),
            pltpu.VMEM((GROUP, 8 * rows_dev), jnp.float32),
            pltpu.VMEM((GROUP, 8 * rows_dev), jnp.float32),
            pltpu.VMEM((8, wide), jnp.float32),
            pltpu.VMEM((wide, 128), jnp.float32),
            pltpu.VMEM((8, 2, rows_dev), jnp.float32),
            pltpu.VMEM((8, 2, rows_dev), jnp.float32),
            dma((4,)), dma((6,)), dma((nz, 4)), dma((-(-wide // 256),)), dma((12,)), dma((4,)), dma,
        ],
        compiler_params=pltpu.CompilerParams(collective_id=0, has_side_effects=True),
        name="layer_distances",
    )(docs, centroids.T, assigned.reshape(1, rows_dev))
    return 1.0 - near.reshape(rows_dev), 1.0 - chosen.reshape(rows_dev)


def fits_layers(docs, centroids):
    tiles = -(-centroids.shape[0] // 128)
    n_clu, feat = lax.axis_size("clu"), centroids.shape[1]
    return (lax.axis_size("doc") == 2 and n_clu == 16 and tiles % 2 == 0 and tiles >= 4
            and feat % 16 == 0 and docs.shape[0] % 128 == 0 and docs.shape[1] % 256 == 0
            and docs.shape[1] == n_clu * feat == 3 * 256)


def on_device(docs, centroids, assigned):
    if fits_layers(docs, centroids):
        return by_layers(docs, centroids, assigned)
    n_clu, nd = lax.axis_size("clu"), lax.axis_size("doc")
    n = n_clu // 2
    rows_dev, depth = docs.shape
    width, feat = centroids.shape
    fp = (feat + 15) // 16 * 16
    cents = centroids.T
    if fp != feat:
        cents = jnp.pad(cents, ((0, fp - feat), (0, 0)))
    rows = nd * rows_dev
    any_space = pl.BlockSpec(memory_space=pl.ANY)
    vmem = pl.BlockSpec(memory_space=pltpu.VMEM)
    dma = pltpu.SemaphoreType.DMA
    hops = n // 2
    line = jax.ShapeDtypeStruct((1, rows_dev), jnp.float32)
    near, chosen = pl.pallas_call(
        functools.partial(kernel, n, nd, feat),
        out_shape=(line, line),
        in_specs=[any_space] * 3,
        out_specs=(vmem, vmem),
        scratch_shapes=[
            pltpu.VMEM((n_clu * fp, width), jnp.bfloat16),
            pltpu.VMEM((nd, rows_dev, depth), jnp.bfloat16),
            pltpu.VMEM((nd, 1, rows_dev), jnp.int32),
            pltpu.VMEM((rows, (n - 3) * 2 * fp), jnp.bfloat16),
            pltpu.VMEM((rows, 4 * fp), jnp.bfloat16),
            pltpu.VMEM((rows, 2 * fp), jnp.bfloat16),
            pltpu.VMEM((rows, width), jnp.float32),
            pltpu.VMEM((rows, 128), jnp.int32),
            pltpu.VMEM((rows, 128), jnp.float32),
            pltpu.VMEM((rows, 128), jnp.float32),
            pltpu.VMEM((8, width), jnp.float32),
            pltpu.VMEM((1, width), jnp.float32),
            pltpu.VMEM((nd, 2, rows_dev), jnp.float32),
            pltpu.VMEM((nd, 2, rows_dev), jnp.float32),
            dma((3,)),
            dma((2, hops, PIECES)),
            dma((n, PIECES)),
            dma((n, 2, PIECES)),
            dma((nd,)), dma((nd,)), dma((nd,)), dma((nd,)), dma((nd,)), dma((nd,)),
        ],
        compiler_params=pltpu.CompilerParams(collective_id=0, has_side_effects=True),
        name="ring_distances",
    )(docs, cents, assigned.reshape(1, rows_dev))
    return 1.0 - near.reshape(rows_dev), 1.0 - chosen.reshape(rows_dev)


def solution(mesh):
    placed = (P(("clu", "doc"), None), P("doc", "clu"), P(("clu", "doc")))
    return jax.shard_map(
        on_device,
        mesh=mesh,
        in_specs=placed,
        out_specs=(P(("clu", "doc")), P(("clu", "doc"))),
        check_vma=False,
    )
```

```python
import functools

import jax
import jax.numpy as jnp
from jax import lax
from jax.experimental import pallas as pl
from jax.experimental.pallas import tpu as pltpu
from jax.sharding import PartitionSpec as P

epsilon = 1e-06
PIECES = 4
ROWS = 64
GROUP = 16
MESH = pl.DeviceIdType.MESH


def chip_at(pos, n):
    half = n // 2
    return jnp.where(pos < half, 2 * pos, 2 * (n - 1 - pos) + 1)


def cut(width):
    tiles = (width + 127) // 128
    ends = [min(-(-tiles * (c + 1) // PIECES) * 128, width) for c in range(PIECES)]
    return tuple((a, b - a) for a, b in zip([0] + ends[:-1], ends))


def kernel(n, nd, feat, docs_in, cents_in, ids_in, near_out, chosen_out,
           buf, docs_all, ids_all, dp_a, dp_b, dp_c, acc, idb, mx, ch, csq, scale, res, got,
           local_sem, ring_send, pair_send, recv, docs_send, docs_recv, ids_send, ids_recv,
           res_send, res_recv):
    hops = n // 2
    fp = cents_in.shape[0]
    width = cents_in.shape[1]
    rows_dev = docs_in.shape[0]
    chunks = cut(width)
    half = len(chunks) // 2

    clu, doc = lax.axis_index("clu"), lax.axis_index("doc")
    core, chip = lax.rem(clu, 2), lax.div(clu, 2)
    z, x = lax.div(chip, 2), lax.rem(chip, 2)
    pos = jnp.where(x == 0, z, n - 1 - z)
    right = chip_at(lax.rem(pos + 1, n), n) * 2 + core
    left = chip_at(lax.rem(pos + n - 1, n), n) * 2 + core
    partner = chip * 2 + (1 - core)

    own_c = pltpu.make_async_copy(cents_in, buf.at[pl.ds(0, fp), :], local_sem.at[0])
    own_d = pltpu.make_async_copy(docs_in, docs_all.at[0], local_sem.at[1])
    own_i = pltpu.make_async_copy(ids_in, ids_all.at[0], local_sem.at[2])
    own_c.start()
    own_d.start()
    own_i.start()

    barrier = pltpu.get_barrier_semaphore()
    for peer in (left, right, partner):
        pl.semaphore_signal(barrier, inc=1, device_id={"clu": peer}, device_id_type=MESH)
    for k in range(1, nd):
        pl.semaphore_signal(barrier, inc=1, device_id={"doc": lax.rem(doc + k, nd)}, device_id_type=MESH)
    pl.semaphore_wait(barrier, 3 + nd - 1)

    def slot(way, h):
        if h == 0:
            return 0
        if h == hops:
            return n - 1
        return 2 * h - 1 if way == 0 else 2 * h

    def piece(s, m, c):
        return buf.at[pl.ds((2 * s + m) * fp, fp), pl.ds(*chunks[c])]

    def reach(way, c):
        return hops if way == c // half else hops - 1

    sent = []

    def ring(way, h, c):
        s, t = slot(way, h), slot(way, h + 1)
        copy = pltpu.make_async_remote_copy(
            src_ref=piece(s, 0, c), dst_ref=piece(t, 0, c),
            send_sem=ring_send.at[way, h, c], recv_sem=recv.at[t, 0, c],
            device_id={"clu": right if way == 0 else left}, device_id_type=MESH)
        copy.start()
        sent.append(copy)

    def share(s, c):
        copy = pltpu.make_async_remote_copy(
            src_ref=piece(s, 0, c), dst_ref=piece(s, 1, c),
            send_sem=pair_send.at[s, c], recv_sem=recv.at[s, 1, c],
            device_id={"clu": partner}, device_id_type=MESH)
        copy.start()
        sent.append(copy)

    def landed(s, m, c):
        pltpu.make_async_remote_copy(
            src_ref=piece(s, m, c), dst_ref=piece(s, m, c),
            send_sem=pair_send.at[s, c], recv_sem=recv.at[s, m, c],
            device_id={"clu": partner}, device_id_type=MESH).wait_recv()

    own_c.wait()
    for i in range(PIECES):
        ring(0, 0, i)
        ring(1, 0, (i + half) % PIECES)
    for c in range(PIECES):
        share(0, c)
    own_d.wait()
    own_i.wait()
    doc_copies = []
    for k in range(1, nd):
        mate = lax.rem(doc + k, nd)
        for ref, ss, rs in ((ids_all, ids_send, ids_recv), (docs_all, docs_send, docs_recv)):
            copy = pltpu.make_async_remote_copy(
                src_ref=ref.at[0], dst_ref=ref.at[k], send_sem=ss.at[k], recv_sem=rs.at[k],
                device_id={"doc": mate}, device_id_type=MESH)
            copy.start()
            doc_copies.append(copy)

    def owner(s):
        if s == 0:
            p = pos
        elif s == n - 1:
            p = pos + hops
        elif s % 2:
            p = pos + n - (s + 1) // 2
        else:
            p = pos + s // 2
        return chip_at(lax.rem(p, n), n)

    ranges = ((0, n - 3), (n - 3, n - 1), (n - 1, n))
    spread = (dp_a, dp_b, dp_c)

    def permute(k):
        rows = docs_all[k]
        for (first, last), out in zip(ranges, spread):
            wide = out.shape[1]
            lane = lax.broadcasted_iota(jnp.int32, (1, wide), 1)
            target = jnp.full((1, wide), -1, jnp.int32)
            for s in range(first, last):
                chip_s = owner(s)
                for m in (0, 1):
                    part = chip_s * 2 + (core if m == 0 else 1 - core)
                    start = (2 * (s - first) + m) * fp
                    inside = (lane >= start) & (lane < start + feat)
                    target = jnp.where(inside, lane - start + part * feat, target)
            source = lax.broadcasted_iota(jnp.int32, (rows.shape[1], wide), 0)
            mover = jnp.where(source == target, 1.0, 0.0).astype(jnp.bfloat16)
            out[pl.ds(k * rows_dev, rows_dev), :] = jnp.dot(
                rows, mover, preferred_element_type=jnp.float32).astype(jnp.bfloat16)

    def prepare_ids(k):
        base = doc * width
        ids = ids_all[k] - base
        ids = jnp.where((ids >= 0) & (ids < width), ids, -1)
        full = jnp.broadcast_to(ids, (128, rows_dev)).T
        lanes = lax.broadcasted_iota(jnp.int32, (rows_dev, 128), 1)
        idb[pl.ds(k * rows_dev, rows_dev), :] = jnp.where(full >= 0, full - lanes, -(2**20))

    def phase(index, c):
        first, last = ranges[index]
        start, depth = 2 * first * fp, 2 * (last - first) * fp
        cols = pl.ds(*chunks[c])
        block = buf[pl.ds(start, depth), cols]
        prod = jnp.dot(spread[index][...], block, preferred_element_type=jnp.float32)
        w32 = block.astype(jnp.float32)
        sq = jnp.sum((w32 * w32).reshape(depth // 8, 8, chunks[c][1]), 0)
        if index == 0:
            acc[:, cols] = prod
            csq[:, cols] = sq
        else:
            acc[:, cols] += prod
            csq[:, cols] += sq

    tail = pl.ds(2 * (n - 1) * fp, 2 * fp)

    def finish_scale(c):
        cols = pl.ds(*chunks[c])
        w32 = buf[tail, cols].astype(jnp.float32)
        sq = jnp.sum((w32 * w32).reshape(2 * fp // 8, 8, chunks[c][1]), 0) + csq[:, cols]
        scale[:, cols] = lax.rsqrt(jnp.sum(sq, 0, keepdims=True) + epsilon)

    def final(k, c):
        start, wide = chunks[c]
        prod = jnp.dot(dp_c[pl.ds(k * rows_dev, rows_dev), :], buf[tail, pl.ds(start, wide)],
                       preferred_element_type=jnp.float32)
        for r in range(0, rows_dev, ROWS):
            rs = pl.ds(k * rows_dev + r, ROWS)
            top, hit = mx[rs, :], ch[rs, :]
            ids = idb[rs, :]
            for a in range(0, wide, 128):
                w = min(128, wide - a)
                cols = pl.ds(start + a, w)
                v = (acc[rs, cols] + prod[r:r + ROWS, a:a + w]) * scale[:, cols]
                if w == 128:
                    top = jnp.maximum(top, v)
                    hit = jnp.where(ids == start + a, v, hit)
                else:
                    mx[rs, :] = top
                    ch[rs, :] = hit
                    mx[rs, pl.ds(0, w)] = jnp.maximum(mx[rs, pl.ds(0, w)], v)
                    ch[rs, pl.ds(0, w)] = jnp.where(idb[rs, pl.ds(0, w)] == start + a, v, ch[rs, pl.ds(0, w)])
            if wide % 128 == 0:
                mx[rs, :] = top
                ch[rs, :] = hit

    def reduced(k):
        rs = pl.ds(k * rows_dev, rows_dev)
        return (jnp.max(mx[rs, :].T, 0, keepdims=True), jnp.sum(ch[rs, :].T, 0, keepdims=True))

    mx[...] = jnp.full(mx.shape, -3.0e38, jnp.float32)
    ch[...] = jnp.zeros(ch.shape, jnp.float32)
    permute(0)
    prepare_ids(0)
    wide = docs_all[0].astype(jnp.float32)
    squares = wide * wide
    total = squares[:, 0:128]
    for a in range(128, wide.shape[1], 128):
        total = total + squares[:, a:a + 128]
    scale_x = lax.rsqrt(jnp.sum(total.T, 0, keepdims=True) + epsilon)

    def step(way, h, c):
        s = slot(way, h)
        landed(s, 0, c)
        if h < reach(way, c):
            ring(way, h, c)
        share(s, c)

    def pair(h, i):
        step(0, h, i)
        step(1, h, (i + half) % PIECES)

    def partners(slots, c):
        for s in slots:
            landed(s, 1, c)

    early, late = range(n - 3), (n - 3, n - 2)
    order = [j // 2 + half * (j % 2) for j in range(PIECES)]
    for h in range(1, hops):
        for i in range(PIECES):
            pair(h, i)
            if h == hops - 2 and i == half:
                for copy in doc_copies:
                    copy.wait()
                for k in range(1, nd):
                    permute(k)
                    prepare_ids(k)
            if h == hops - 1:
                c = order[i]
                partners(early, c)
                phase(0, c)
    for c in order[:half]:
        partners(late, c)
        phase(1, c)
    for i in range(half):
        for way in (0, 1):
            c = i + half * way
            landed(n - 1, 0, c)
            share(n - 1, c)
    for c in order[half:]:
        partners(late, c)
        phase(1, c)
    for c in order[:-2]:
        landed(n - 1, 1, c)
        finish_scale(c)
        for k in range(nd):
            final(k, c)
    for c in order[-2:]:
        landed(n - 1, 1, c)
        finish_scale(c)

    returns = []
    for k in range(1, nd):
        for c in order[-2:]:
            final(k, c)
        best, chosen = reduced(k)
        res[k, 0:1, :] = best
        res[k, 1:2, :] = chosen
        copy = pltpu.make_async_remote_copy(
            src_ref=res.at[k], dst_ref=got.at[k], send_sem=res_send.at[k], recv_sem=res_recv.at[k],
            device_id={"doc": lax.rem(doc + nd - k, nd)}, device_id_type=MESH)
        copy.start()
        returns.append(copy)
    for c in order[-2:]:
        final(0, c)
    best, chosen = reduced(0)
    for k in range(1, nd):
        returns[k - 1].wait()
        best = jnp.maximum(best, got[k, 0:1, :])
        chosen = chosen + got[k, 1:2, :]
    near_out[...] = best * scale_x
    chosen_out[...] = chosen * scale_x
    for copy in sent:
        copy.wait_send()


def layer_kernel(nz, feat, docs_in, cents_in, ids_in, near_out, chosen_out,
                 own, raw, buf, docs, flat, ids, turned, acc, idb, mx, ch, csq, scale, res, got,
                 local_sem, send_sem, c_recv, last_recv, d_recv, i_recv, r_recv):
    width = cents_in.shape[1]
    rows_dev, depth = docs_in.shape
    tiles = own.shape[1] // 128
    per = tiles // 2
    small = per // 2
    big = per - small
    wide = big * 128
    full = width // 128 * 128
    late = -(-4 * feat // 256) * 256
    k1 = 8 * feat // 256 * 256
    k2 = depth - late - k1
    a = rows_dev * 5 // 16 // 16 * 16
    b = (rows_dev - a) // 32 * 16
    spans = ((0, a), (a, b), (a + b, rows_dev - a - b))
    chunks = tuple((c, min(256, wide - c)) for c in range(0, wide, 256))

    clu, doc = lax.axis_index("clu"), lax.axis_index("doc")
    core, chip = lax.rem(clu, 2), lax.div(clu, 2)
    z, x = lax.div(chip, 2), lax.rem(chip, 2)
    upper = z >= nz // 2
    out = jnp.where(upper, 1, -1)
    end = (z == 0) | (z == nz - 1)
    inner = jnp.logical_not(end)

    def device(r, dz=0):
        dx, dy, dc = r // 4, r // 2 % 2, r % 2
        there = ((z + dz) * 2 + (1 - x if dx else x)) * 2 + (1 - core if dc else core)
        return {"clu": there, "doc": 1 - doc if dy else doc}

    def when(cond, body):
        if cond is None:
            body()
        else:
            pl.when(cond)(body)

    def both(p, q):
        return q if p is None else p if q is None else p & q

    sizes = ((None, big),) if big == small else ((1, big), (0, small))

    def sized(c, cond, body):
        for value, count in sizes:
            when(both(cond, None if value is None else c == value), functools.partial(body, count * 128))

    own_copy = pltpu.make_async_copy(cents_in.at[:, pl.ds(0, full)], own.at[:, pl.ds(0, full)], local_sem.at[0])
    docs_copy = pltpu.make_async_copy(docs_in, docs.at[0], local_sem.at[1])
    ids_copy = pltpu.make_async_copy(ids_in, ids.at[0], local_sem.at[2])
    own_copy.start()
    if full < width:
        raw_copy = pltpu.make_async_copy(cents_in.at[:, pl.ds(full, width - full)], raw, local_sem.at[3])
        raw_copy.start()
    docs_copy.start()
    ids_copy.start()

    barrier = pltpu.get_barrier_semaphore()

    def greet(to):
        pl.semaphore_signal(barrier, inc=1, device_id=to, device_id_type=MESH)

    pl.when(inner)(lambda: greet(device(0, out)))
    greet(device(0, -out))
    for r in (4, 5, 2, 1):
        greet(device(r))
    if small < big:
        @pl.when(core == 0)
        def _():
            buf[:, pl.ds(small * 128, 128)] = jnp.zeros((buf.shape[0], 128), buf.dtype)
    if full < width:
        raw_copy.wait()
        own[:, pl.ds(full, 128)] = jnp.concatenate(
            [raw[...], jnp.zeros((feat, full + 128 - width), raw.dtype)], axis=1)
    own_copy.wait()
    docs_copy.wait()
    ids_copy.wait()
    pl.semaphore_wait(barrier, 5 + inner.astype(jnp.int32))

    outward, inward, traded, doc_sent, id_sent, result_sent = (send_sem.at[i] for i in range(6))

    def start(make, cond=None):
        when(cond, lambda: make().start())

    def start_sized(make, c, cond=None):
        sized(c, cond, lambda w: make(w).start())

    def remote(src, dst, ss, rs, to):
        return pltpu.make_async_remote_copy(
            src_ref=src, dst_ref=dst, send_sem=ss, recv_sem=rs, device_id=to, device_id_type=MESH)

    near = (0, 1, 4, 5)

    def source(layer, j):
        r = near[j]
        there = (layer * 2 + (1 - x if r // 4 else x)) * 2 + (1 - core if r % 2 else core)
        return pl.ds(pl.multiple_of(there * feat, 16), feat)

    def columns(r, w):
        xd = 1 - x if r // 4 else x
        cd = 1 - core if r % 2 else core
        return pl.ds(pl.multiple_of((xd * per + cd * small) * 128, 128), w)

    mine = source(z, 0)

    def exchange(j):
        r = near[j]
        start_sized(lambda w: remote(own.at[:, columns(r, w)], buf.at[mine, pl.ds(0, w)],
                                     traded, c_recv.at[z, j], device(r)),
                    1 - core if r % 2 else core)

    def landed(layer, j, cond=None):
        rows = source(layer, j)
        sized(core, cond, lambda w: remote(
            buf.at[rows, pl.ds(0, w)], buf.at[rows, pl.ds(0, w)], traded, c_recv.at[layer, j],
            device(1)).wait_recv())

    def carry(layer, j, way, s, cond=None):
        rows = source(layer, j)
        src = (lambda w: own.at[:, columns(0, w)]) if s == 0 and j == 0 else (lambda w: buf.at[rows, pl.ds(0, w)])
        start_sized(lambda w: remote(src(w), buf.at[rows, pl.ds(0, w)], inward if way else outward,
                                     c_recv.at[layer, j], device(0, -out if way else out)), core, cond)

    def spread(j):
        if j:
            landed(z, j)
        carry(z, j, 0, 0, inner)
        carry(z, j, 1, 0)

    def relay(j):
        landed(z - out, j)
        carry(z - out, j, 0, 1, inner)
        landed(z + out, j, inner)
        carry(z + out, j, 1, 1, inner)

    def pair(layer, k, w):
        rows = pl.ds(pl.multiple_of((layer * 2 + 1 - x) * 2 * feat, 16), 2 * feat)
        c = chunks[k][0]
        return buf.at[rows, pl.ds(c, min(w, c + chunks[k][1]) - c)]

    def relay_far(j):
        landed(z - 2 * out, j)
        if j < 2:
            carry(z - 2 * out, j, 0, 2, inner)
        elif j == 3:
            for k in range(len(chunks)):
                start_sized(lambda w, k=k: remote(
                    pair(z - 2 * out, k, w), pair(z - 2 * out, k, w), outward, last_recv.at[k],
                    device(0, out)), core, inner)

    def last_landed(k):
        sized(core, end, lambda w: remote(
            pair(z - 3 * out, k, w), pair(z - 3 * out, k, w), outward, last_recv.at[k],
            device(1)).wait_recv())

    ahead = {(1, 0): 0, (1, 1): 0, (1, 2): 0, (3, 0): 1, (3, 1): 1, (3, 2): 1, (5, 0): 2, (5, 1): 2, (5, 2): 2,
             (7, 0): 3, (7, 1): 3, (7, 2): 3, (2, 0): 4, (2, 1): 5, (2, 2): 5, (4, 0): 6, (4, 1): 7, (4, 2): 8,
             (6, 0): 9, (6, 1): 10, (6, 2): 11}
    id_at = {1: 0, 3: 0, 5: 0, 7: 0, 2: 1, 4: 2, 6: 3}

    def part(slot, *parts):
        first, last = spans[parts[0]], spans[parts[-1]]
        return docs.at[slot, pl.ds(first[0], last[0] + last[1] - first[0]), :]

    def send_docs(src_slot, dst_slot, r, *parts):
        start(lambda: remote(part(src_slot, *parts), part(dst_slot, *parts), doc_sent,
                             d_recv.at[ahead[dst_slot, parts[0]]], device(r)))

    def send_ids(src_slot, dst_slot, r):
        start(lambda: remote(ids.at[src_slot], ids.at[dst_slot], id_sent, i_recv.at[id_at[dst_slot]], device(r)))

    def have_docs(slot, *parts):
        remote(part(slot, *parts), part(slot, *parts), doc_sent, d_recv.at[ahead[slot, parts[0]]],
               device(1)).wait_recv()

    def have_ids(slot):
        some = ids.at[pl.ds(0, 4)] if slot % 2 else ids.at[slot]
        remote(some, some, id_sent, i_recv.at[id_at[slot]], device(1)).wait_recv()

    def share(slot, *parts):
        send_docs(slot, slot + 1, 1, *parts)

    spread(0)
    for j in (1, 2, 3):
        exchange(j)
    send_ids(0, 2, 2)
    send_docs(0, 2, 2, 0)
    send_docs(0, 2, 2, 1, 2)
    send_ids(0, 4, 4)
    for p in (1, 2, 0):
        send_docs(0, 4, 4, p)
    send_ids(0, 1, 1)
    send_docs(0, 1, 1, 0, 1, 2)

    part_cols = jnp.where(core == 1, big, small) * 128
    first = (x * per + core * small) * 128
    base = doc * width + first
    reach = jnp.minimum(part_cols, width - first)
    down = lax.broadcasted_iota(jnp.int32, (GROUP, 128), 0)

    def prepare_ids(slot):
        rel = ids[slot] - base
        rel = jnp.where((rel >= 0) & (rel < reach), rel, -(2**20))
        tall = jnp.broadcast_to(rel, (GROUP, rows_dev))
        idb[:, pl.ds(slot * rows_dev, rows_dev)] = tall - lax.broadcasted_iota(jnp.int32, (GROUP, rows_dev), 0)

    buf[mine, pl.ds(0, small * 128)] = own[:, columns(0, small * 128)]
    if small < big:
        @pl.when(core == 1)
        def _():
            start_col = pl.multiple_of((x * per + 2 * small) * 128, 128)
            buf[mine, pl.ds(small * 128, 128)] = own[:, pl.ds(start_col, 128)]

    k1_at = pl.multiple_of(jnp.where(upper, depth - k1, 0), 256)
    k2_at = pl.multiple_of(jnp.where(upper, late, k1), 256)
    late_at = pl.multiple_of(jnp.where(upper, 0, depth - late), 256)
    starts = (k1_at, k2_at, late_at)

    def squares(i, c, w):
        w32 = buf[pl.ds(starts[i], 256), pl.ds(c, w)].astype(jnp.float32)
        return jnp.sum((w32 * w32).reshape(32, 8, w), 0)

    def turn(i, c, w):
        turned[i, pl.ds(c, w), :] = buf[pl.ds(starts[i], 256), pl.ds(c, w)].T

    def gather(i):
        for c, w in chunks:
            turn(i, c, w)
        csq[...] = squares(i, 0, wide) + (csq[...] if i else 0.0)

    def flatten(*slots):
        for slot in slots:
            flat[:, pl.ds(slot * rows_dev, rows_dev)] = docs[slot].T

    def times(i, c, w, slot, count):
        return jnp.dot(turned[i, pl.ds(c, w), :],
                       flat[pl.ds(starts[i], 256), pl.ds(slot * rows_dev, count * rows_dev)],
                       preferred_element_type=jnp.float32)

    def begin(slot, count, *phases):
        where_docs = pl.ds(slot * rows_dev, count * rows_dev)
        prod = times(phases[0], 0, wide, slot, count)
        for i in phases[1:]:
            prod = prod + times(i, 0, wide, slot, count)
        if phases[0]:
            acc[:, where_docs] += prod
        else:
            acc[:, where_docs] = prod

    spread(1)
    prepare_ids(0)
    flatten(0)
    spread(2)
    relay(0)
    spread(3)
    relay(1)
    have_docs(2, 0)
    send_docs(2, 6, 4, 0)
    have_ids(4)
    send_ids(4, 6, 2)
    send_ids(4, 5, 1)
    have_ids(2)
    send_ids(2, 3, 1)
    relay(2)
    have_docs(4, 1)
    send_docs(4, 6, 2, 1)
    have_docs(1, 0, 1, 2)
    flatten(1)
    relay(3)
    relay_far(0)
    have_docs(2, 1, 2)
    share(2, 0, 1, 2)
    have_docs(4, 2)
    send_docs(4, 6, 2, 2)
    have_ids(6)
    send_ids(6, 7, 1)
    relay_far(1)
    gather(0)
    begin(0, 2, 0)
    flatten(2)
    have_ids(1)
    for slot in (1, 2, 3, 4, 5, 6, 7):
        prepare_ids(slot)
    relay_far(2)
    have_docs(4, 0)
    share(4, 0, 1, 2)
    have_docs(3, 0, 1, 2)
    flatten(3)
    begin(2, 2, 0)
    relay_far(3)
    gather(1)
    flatten(4)
    begin(0, 2, 1)
    begin(2, 2, 1)
    have_docs(5, 0, 1, 2)
    flatten(5)
    begin(4, 2, 0, 1)
    for p in (1, 2, 0):
        have_docs(6, p)
    share(6, 0, 1, 2)
    flatten(6)

    def scales(c, w):
        total = jnp.sum(csq[:, pl.ds(c, w)] + squares(2, c, w), 0, keepdims=True)
        scale[pl.ds(c, w), :] = jnp.broadcast_to(lax.rsqrt(total + epsilon), (128, w)).T

    def stage(c0, w, slot, count):
        prod = times(2, c0, w, slot, count)
        spots = [pl.ds(slot * rows_dev + d, 128) for d in range(0, count * rows_dev, 128)]
        if c0:
            tops, hits = [mx[:, at] for at in spots], [ch[:, at] for at in spots]
        else:
            tops = [jnp.full((GROUP, 128), -3.0e38, jnp.float32)] * len(spots)
            hits = [jnp.zeros((GROUP, 128), jnp.float32)] * len(spots)
        for c in range(0, w, GROUP):
            rows = pl.ds(c0 + c, GROUP)
            by = scale[rows, :]
            for n, at in enumerate(spots):
                v = (acc[rows, at] + prod[c:c + GROUP, n * 128:n * 128 + 128]) * by
                hits[n] = jnp.where(idb[:, at] == c0 + c, v, hits[n])
                if c0 + c + 128 > small * 128:
                    v = jnp.where(down < reach - (c0 + c), v, -3.0e38)
                tops[n] = jnp.maximum(tops[n], v)
        for n, at in enumerate(spots):
            mx[:, at], ch[:, at] = tops[n], hits[n]

    def reduced(slot):
        at = pl.ds(slot * rows_dev, rows_dev)
        return jnp.max(mx[:, at], 0, keepdims=True), jnp.sum(ch[:, at], 0, keepdims=True)

    def give(slot):
        best, chosen = reduced(slot)
        res[slot, 0:1, :] = best
        res[slot, 1:2, :] = chosen
        remote(res.at[slot], got.at[slot], result_sent, r_recv, device(slot)).start()

    x32 = docs[0].astype(jnp.float32)
    sq = x32 * x32
    total = sq[:, 0:128]
    for c in range(128, depth, 128):
        total = total + sq[:, c:c + 128]
    scale_x = lax.rsqrt(jnp.sum(total.T, 0, keepdims=True) + epsilon)

    landed(z - 3 * out, 0, end)
    landed(z - 3 * out, 1, end)
    final = len(chunks) - 1
    for i in range(final):
        last_landed(i)
        c, w = chunks[i]
        turn(2, c, w)
        scales(c, w)
        for slot in (0, 2, 4):
            stage(c, w, slot, 2)
        if i == 0:
            have_docs(7, 0, 1, 2)
            flatten(7)
            begin(6, 2, 0, 1)
        stage(c, w, 6, 2)
    last_landed(final)

    def finish(have):
        c = chunks[final][0]
        w = have - c
        turn(2, c, w)
        scales(c, w)
        stage(c, w, 6, 2)
        stage(c, w, 2, 2)
        give(7)
        give(6)
        stage(c, w, 4, 2)
        give(3)
        give(2)
        stage(c, w, 0, 2)
        give(5)
        give(4)
        give(1)

    sized(core, None, finish)
    best, chosen = reduced(0)
    everyone = pl.ds(1, 7)
    remote(got.at[everyone], got.at[everyone], result_sent, r_recv, device(1)).wait_recv()
    for slot in range(1, 8):
        best = jnp.maximum(best, got[slot, 0:1, :])
        chosen = chosen + got[slot, 1:2, :]
    near_out[...] = best * scale_x
    chosen_out[...] = chosen * scale_x

    def sent(ref, sem):
        remote(ref, ref, sem, r_recv, device(1)).wait_send()

    sent(res.at[everyone], result_sent)
    sent(docs.at[everyone], doc_sent)
    sent(ids.at[everyone], id_sent)
    layer = 4 * feat
    sized(core, inner, lambda w: sent(buf.at[pl.ds(0, 3 * layer), pl.ds(0, w)], outward))
    sized(core, inner, lambda w: sent(buf.at[pl.ds(0, 2 * layer), pl.ds(0, w)], inward))
    sized(core, end, lambda w: sent(buf.at[pl.ds(0, layer), pl.ds(0, w)], inward))
    sized(core, None, lambda w: sent(own.at[:, pl.ds(0, 2 * per * 128 - w)], traded))


def by_layers(docs, centroids, assigned):
    nz = lax.axis_size("clu") // 4
    rows_dev, depth = docs.shape
    width, feat = centroids.shape
    tiles = -(-width // 128)
    wide = (tiles // 2 - tiles // 4) * 128
    any_space = pl.BlockSpec(memory_space=pl.ANY)
    vmem = pl.BlockSpec(memory_space=pltpu.VMEM)
    dma = pltpu.SemaphoreType.DMA
    line = pltpu.VMEM((1, rows_dev), jnp.float32)
    near, chosen = pl.pallas_call(
        functools.partial(layer_kernel, nz, feat),
        out_shape=(line, line),
        in_specs=[any_space] * 3,
        out_specs=(vmem, vmem),
        scratch_shapes=[
            pltpu.VMEM((feat, tiles * 128), jnp.bfloat16),
            pltpu.VMEM((feat, width % 128 or 128), jnp.bfloat16),
            pltpu.VMEM((depth, wide), jnp.bfloat16),
            pltpu.VMEM((8, rows_dev, depth), jnp.bfloat16),
            pltpu.VMEM((depth, 8 * rows_dev), jnp.bfloat16),
            pltpu.VMEM((8, 1, rows_dev), jnp.int32),
            pltpu.VMEM((3, wide, 256), jnp.bfloat16),
            pltpu.VMEM((wide, 8 * rows_dev), jnp.float32),
            pltpu.VMEM((GROUP, 8 * rows_dev), jnp.int32),
            pltpu.VMEM((GROUP, 8 * rows_dev), jnp.float32),
            pltpu.VMEM((GROUP, 8 * rows_dev), jnp.float32),
            pltpu.VMEM((8, wide), jnp.float32),
            pltpu.VMEM((wide, 128), jnp.float32),
            pltpu.VMEM((8, 2, rows_dev), jnp.float32),
            pltpu.VMEM((8, 2, rows_dev), jnp.float32),
            dma((4,)), dma((6,)), dma((nz, 4)), dma((-(-wide // 256),)), dma((12,)), dma((4,)), dma,
        ],
        compiler_params=pltpu.CompilerParams(collective_id=0, has_side_effects=True),
        name="layer_distances",
    )(docs, centroids.T, assigned.reshape(1, rows_dev))
    return 1.0 - near.reshape(rows_dev), 1.0 - chosen.reshape(rows_dev)


def fits_layers(docs, centroids):
    tiles = -(-centroids.shape[0] // 128)
    n_clu, feat = lax.axis_size("clu"), centroids.shape[1]
    return (lax.axis_size("doc") == 2 and n_clu == 16 and tiles % 2 == 0 and tiles >= 4
            and feat % 16 == 0 and docs.shape[0] % 128 == 0 and docs.shape[1] % 256 == 0
            and docs.shape[1] == n_clu * feat == 3 * 256)


def on_device(docs, centroids, assigned):
    if fits_layers(docs, centroids):
        return by_layers(docs, centroids, assigned)
    n_clu, nd = lax.axis_size("clu"), lax.axis_size("doc")
    n = n_clu // 2
    rows_dev, depth = docs.shape
    width, feat = centroids.shape
    fp = (feat + 15) // 16 * 16
    cents = centroids.T
    if fp != feat:
        cents = jnp.pad(cents, ((0, fp - feat), (0, 0)))
    rows = nd * rows_dev
    any_space = pl.BlockSpec(memory_space=pl.ANY)
    vmem = pl.BlockSpec(memory_space=pltpu.VMEM)
    dma = pltpu.SemaphoreType.DMA
    hops = n // 2
    line = jax.ShapeDtypeStruct((1, rows_dev), jnp.float32)
    near, chosen = pl.pallas_call(
        functools.partial(kernel, n, nd, feat),
        out_shape=(line, line),
        in_specs=[any_space] * 3,
        out_specs=(vmem, vmem),
        scratch_shapes=[
            pltpu.VMEM((n_clu * fp, width), jnp.bfloat16),
            pltpu.VMEM((nd, rows_dev, depth), jnp.bfloat16),
            pltpu.VMEM((nd, 1, rows_dev), jnp.int32),
            pltpu.VMEM((rows, (n - 3) * 2 * fp), jnp.bfloat16),
            pltpu.VMEM((rows, 4 * fp), jnp.bfloat16),
            pltpu.VMEM((rows, 2 * fp), jnp.bfloat16),
            pltpu.VMEM((rows, width), jnp.float32),
            pltpu.VMEM((rows, 128), jnp.int32),
            pltpu.VMEM((rows, 128), jnp.float32),
            pltpu.VMEM((rows, 128), jnp.float32),
            pltpu.VMEM((8, width), jnp.float32),
            pltpu.VMEM((1, width), jnp.float32),
            pltpu.VMEM((nd, 2, rows_dev), jnp.float32),
            pltpu.VMEM((nd, 2, rows_dev), jnp.float32),
            dma((3,)),
            dma((2, hops, PIECES)),
            dma((n, PIECES)),
            dma((n, 2, PIECES)),
            dma((nd,)), dma((nd,)), dma((nd,)), dma((nd,)), dma((nd,)), dma((nd,)),
        ],
        compiler_params=pltpu.CompilerParams(collective_id=0, has_side_effects=True),
        name="ring_distances",
    )(docs, cents, assigned.reshape(1, rows_dev))
    return 1.0 - near.reshape(rows_dev), 1.0 - chosen.reshape(rows_dev)


def solution(mesh):
    placed = (P(("clu", "doc"), None), P("doc", "clu"), P(("clu", "doc")))
    return jax.shard_map(
        on_device,
        mesh=mesh,
        in_specs=placed,
        out_specs=(P(("clu", "doc")), P(("clu", "doc"))),
        check_vma=False,
    )
```

```python
import functools

import jax
import jax.numpy as jnp
from jax import lax
from jax.experimental import pallas as pl
from jax.experimental.pallas import tpu as pltpu
from jax.sharding import PartitionSpec as P

epsilon = 1e-06
PIECES = 4
ROWS = 64
GROUP = 16
MESH = pl.DeviceIdType.MESH


def chip_at(pos, n):
    half = n // 2
    return jnp.where(pos < half, 2 * pos, 2 * (n - 1 - pos) + 1)


def cut(width):
    tiles = (width + 127) // 128
    ends = [min(-(-tiles * (c + 1) // PIECES) * 128, width) for c in range(PIECES)]
    return tuple((a, b - a) for a, b in zip([0] + ends[:-1], ends))


def kernel(n, nd, feat, docs_in, cents_in, ids_in, near_out, chosen_out,
           buf, docs_all, ids_all, dp_a, dp_b, dp_c, acc, idb, mx, ch, csq, scale, res, got,
           local_sem, ring_send, pair_send, recv, docs_send, docs_recv, ids_send, ids_recv,
           res_send, res_recv):
    hops = n // 2
    fp = cents_in.shape[0]
    width = cents_in.shape[1]
    rows_dev = docs_in.shape[0]
    chunks = cut(width)
    half = len(chunks) // 2

    clu, doc = lax.axis_index("clu"), lax.axis_index("doc")
    core, chip = lax.rem(clu, 2), lax.div(clu, 2)
    z, x = lax.div(chip, 2), lax.rem(chip, 2)
    pos = jnp.where(x == 0, z, n - 1 - z)
    right = chip_at(lax.rem(pos + 1, n), n) * 2 + core
    left = chip_at(lax.rem(pos + n - 1, n), n) * 2 + core
    partner = chip * 2 + (1 - core)

    own_c = pltpu.make_async_copy(cents_in, buf.at[pl.ds(0, fp), :], local_sem.at[0])
    own_d = pltpu.make_async_copy(docs_in, docs_all.at[0], local_sem.at[1])
    own_i = pltpu.make_async_copy(ids_in, ids_all.at[0], local_sem.at[2])
    own_c.start()
    own_d.start()
    own_i.start()

    barrier = pltpu.get_barrier_semaphore()
    for peer in (left, right, partner):
        pl.semaphore_signal(barrier, inc=1, device_id={"clu": peer}, device_id_type=MESH)
    for k in range(1, nd):
        pl.semaphore_signal(barrier, inc=1, device_id={"doc": lax.rem(doc + k, nd)}, device_id_type=MESH)
    pl.semaphore_wait(barrier, 3 + nd - 1)

    def slot(way, h):
        if h == 0:
            return 0
        if h == hops:
            return n - 1
        return 2 * h - 1 if way == 0 else 2 * h

    def piece(s, m, c):
        return buf.at[pl.ds((2 * s + m) * fp, fp), pl.ds(*chunks[c])]

    def reach(way, c):
        return hops if way == c // half else hops - 1

    sent = []

    def ring(way, h, c):
        s, t = slot(way, h), slot(way, h + 1)
        copy = pltpu.make_async_remote_copy(
            src_ref=piece(s, 0, c), dst_ref=piece(t, 0, c),
            send_sem=ring_send.at[way, h, c], recv_sem=recv.at[t, 0, c],
            device_id={"clu": right if way == 0 else left}, device_id_type=MESH)
        copy.start()
        sent.append(copy)

    def share(s, c):
        copy = pltpu.make_async_remote_copy(
            src_ref=piece(s, 0, c), dst_ref=piece(s, 1, c),
            send_sem=pair_send.at[s, c], recv_sem=recv.at[s, 1, c],
            device_id={"clu": partner}, device_id_type=MESH)
        copy.start()
        sent.append(copy)

    def landed(s, m, c):
        pltpu.make_async_remote_copy(
            src_ref=piece(s, m, c), dst_ref=piece(s, m, c),
            send_sem=pair_send.at[s, c], recv_sem=recv.at[s, m, c],
            device_id={"clu": partner}, device_id_type=MESH).wait_recv()

    own_c.wait()
    for i in range(PIECES):
        ring(0, 0, i)
        ring(1, 0, (i + half) % PIECES)
    for c in range(PIECES):
        share(0, c)
    own_d.wait()
    own_i.wait()
    doc_copies = []
    for k in range(1, nd):
        mate = lax.rem(doc + k, nd)
        for ref, ss, rs in ((ids_all, ids_send, ids_recv), (docs_all, docs_send, docs_recv)):
            copy = pltpu.make_async_remote_copy(
                src_ref=ref.at[0], dst_ref=ref.at[k], send_sem=ss.at[k], recv_sem=rs.at[k],
                device_id={"doc": mate}, device_id_type=MESH)
            copy.start()
            doc_copies.append(copy)

    def owner(s):
        if s == 0:
            p = pos
        elif s == n - 1:
            p = pos + hops
        elif s % 2:
            p = pos + n - (s + 1) // 2
        else:
            p = pos + s // 2
        return chip_at(lax.rem(p, n), n)

    ranges = ((0, n - 3), (n - 3, n - 1), (n - 1, n))
    spread = (dp_a, dp_b, dp_c)

    def permute(k):
        rows = docs_all[k]
        for (first, last), out in zip(ranges, spread):
            wide = out.shape[1]
            lane = lax.broadcasted_iota(jnp.int32, (1, wide), 1)
            target = jnp.full((1, wide), -1, jnp.int32)
            for s in range(first, last):
                chip_s = owner(s)
                for m in (0, 1):
                    part = chip_s * 2 + (core if m == 0 else 1 - core)
                    start = (2 * (s - first) + m) * fp
                    inside = (lane >= start) & (lane < start + feat)
                    target = jnp.where(inside, lane - start + part * feat, target)
            source = lax.broadcasted_iota(jnp.int32, (rows.shape[1], wide), 0)
            mover = jnp.where(source == target, 1.0, 0.0).astype(jnp.bfloat16)
            out[pl.ds(k * rows_dev, rows_dev), :] = jnp.dot(
                rows, mover, preferred_element_type=jnp.float32).astype(jnp.bfloat16)

    def prepare_ids(k):
        base = doc * width
        ids = ids_all[k] - base
        ids = jnp.where((ids >= 0) & (ids < width), ids, -1)
        full = jnp.broadcast_to(ids, (128, rows_dev)).T
        lanes = lax.broadcasted_iota(jnp.int32, (rows_dev, 128), 1)
        idb[pl.ds(k * rows_dev, rows_dev), :] = jnp.where(full >= 0, full - lanes, -(2**20))

    def phase(index, c):
        first, last = ranges[index]
        start, depth = 2 * first * fp, 2 * (last - first) * fp
        cols = pl.ds(*chunks[c])
        block = buf[pl.ds(start, depth), cols]
        prod = jnp.dot(spread[index][...], block, preferred_element_type=jnp.float32)
        w32 = block.astype(jnp.float32)
        sq = jnp.sum((w32 * w32).reshape(depth // 8, 8, chunks[c][1]), 0)
        if index == 0:
            acc[:, cols] = prod
            csq[:, cols] = sq
        else:
            acc[:, cols] += prod
            csq[:, cols] += sq

    tail = pl.ds(2 * (n - 1) * fp, 2 * fp)

    def finish_scale(c):
        cols = pl.ds(*chunks[c])
        w32 = buf[tail, cols].astype(jnp.float32)
        sq = jnp.sum((w32 * w32).reshape(2 * fp // 8, 8, chunks[c][1]), 0) + csq[:, cols]
        scale[:, cols] = lax.rsqrt(jnp.sum(sq, 0, keepdims=True) + epsilon)

    def final(k, c):
        start, wide = chunks[c]
        prod = jnp.dot(dp_c[pl.ds(k * rows_dev, rows_dev), :], buf[tail, pl.ds(start, wide)],
                       preferred_element_type=jnp.float32)
        for r in range(0, rows_dev, ROWS):
            rs = pl.ds(k * rows_dev + r, ROWS)
            top, hit = mx[rs, :], ch[rs, :]
            ids = idb[rs, :]
            for a in range(0, wide, 128):
                w = min(128, wide - a)
                cols = pl.ds(start + a, w)
                v = (acc[rs, cols] + prod[r:r + ROWS, a:a + w]) * scale[:, cols]
                if w == 128:
                    top = jnp.maximum(top, v)
                    hit = jnp.where(ids == start + a, v, hit)
                else:
                    mx[rs, :] = top
                    ch[rs, :] = hit
                    mx[rs, pl.ds(0, w)] = jnp.maximum(mx[rs, pl.ds(0, w)], v)
                    ch[rs, pl.ds(0, w)] = jnp.where(idb[rs, pl.ds(0, w)] == start + a, v, ch[rs, pl.ds(0, w)])
            if wide % 128 == 0:
                mx[rs, :] = top
                ch[rs, :] = hit

    def reduced(k):
        rs = pl.ds(k * rows_dev, rows_dev)
        return (jnp.max(mx[rs, :].T, 0, keepdims=True), jnp.sum(ch[rs, :].T, 0, keepdims=True))

    mx[...] = jnp.full(mx.shape, -3.0e38, jnp.float32)
    ch[...] = jnp.zeros(ch.shape, jnp.float32)
    permute(0)
    prepare_ids(0)
    wide = docs_all[0].astype(jnp.float32)
    squares = wide * wide
    total = squares[:, 0:128]
    for a in range(128, wide.shape[1], 128):
        total = total + squares[:, a:a + 128]
    scale_x = lax.rsqrt(jnp.sum(total.T, 0, keepdims=True) + epsilon)

    def step(way, h, c):
        s = slot(way, h)
        landed(s, 0, c)
        if h < reach(way, c):
            ring(way, h, c)
        share(s, c)

    def pair(h, i):
        step(0, h, i)
        step(1, h, (i + half) % PIECES)

    def partners(slots, c):
        for s in slots:
            landed(s, 1, c)

    early, late = range(n - 3), (n - 3, n - 2)
    order = [j // 2 + half * (j % 2) for j in range(PIECES)]
    for h in range(1, hops):
        for i in range(PIECES):
            pair(h, i)
            if h == hops - 2 and i == half:
                for copy in doc_copies:
                    copy.wait()
                for k in range(1, nd):
                    permute(k)
                    prepare_ids(k)
            if h == hops - 1:
                c = order[i]
                partners(early, c)
                phase(0, c)
    for c in order[:half]:
        partners(late, c)
        phase(1, c)
    for i in range(half):
        for way in (0, 1):
            c = i + half * way
            landed(n - 1, 0, c)
            share(n - 1, c)
    for c in order[half:]:
        partners(late, c)
        phase(1, c)
    for c in order[:-2]:
        landed(n - 1, 1, c)
        finish_scale(c)
        for k in range(nd):
            final(k, c)
    for c in order[-2:]:
        landed(n - 1, 1, c)
        finish_scale(c)

    returns = []
    for k in range(1, nd):
        for c in order[-2:]:
            final(k, c)
        best, chosen = reduced(k)
        res[k, 0:1, :] = best
        res[k, 1:2, :] = chosen
        copy = pltpu.make_async_remote_copy(
            src_ref=res.at[k], dst_ref=got.at[k], send_sem=res_send.at[k], recv_sem=res_recv.at[k],
            device_id={"doc": lax.rem(doc + nd - k, nd)}, device_id_type=MESH)
        copy.start()
        returns.append(copy)
    for c in order[-2:]:
        final(0, c)
    best, chosen = reduced(0)
    for k in range(1, nd):
        returns[k - 1].wait()
        best = jnp.maximum(best, got[k, 0:1, :])
        chosen = chosen + got[k, 1:2, :]
    near_out[...] = best * scale_x
    chosen_out[...] = chosen * scale_x
    for copy in sent:
        copy.wait_send()


def layer_kernel(nz, feat, docs_in, cents_in, ids_in, near_out, chosen_out,
                 own, raw, buf, docs, flat, ids, turned, acc, idb, mx, ch, csq, scale, res, got,
                 local_sem, send_sem, c_recv, last_recv, d_recv, i_recv, r_recv):
    width = cents_in.shape[1]
    rows_dev, depth = docs_in.shape
    tiles = own.shape[1] // 128
    per = tiles // 2
    small = per // 2
    big = per - small
    wide = big * 128
    full = width // 128 * 128
    late = -(-4 * feat // 256) * 256
    k1 = 8 * feat // 256 * 256
    k2 = depth - late - k1
    a = rows_dev * 5 // 16 // 16 * 16
    b = (rows_dev - a) // 32 * 16
    spans = ((0, a), (a, b), (a + b, rows_dev - a - b))
    chunks = tuple((c, min(256, wide - c)) for c in range(0, wide, 256))

    clu, doc = lax.axis_index("clu"), lax.axis_index("doc")
    core, chip = lax.rem(clu, 2), lax.div(clu, 2)
    z, x = lax.div(chip, 2), lax.rem(chip, 2)
    upper = z >= nz // 2
    out = jnp.where(upper, 1, -1)
    end = (z == 0) | (z == nz - 1)
    inner = jnp.logical_not(end)

    def device(r, dz=0):
        dx, dy, dc = r // 4, r // 2 % 2, r % 2
        there = ((z + dz) * 2 + (1 - x if dx else x)) * 2 + (1 - core if dc else core)
        return {"clu": there, "doc": 1 - doc if dy else doc}

    def when(cond, body):
        if cond is None:
            body()
        else:
            pl.when(cond)(body)

    def both(p, q):
        return q if p is None else p if q is None else p & q

    sizes = ((None, big),) if big == small else ((1, big), (0, small))

    def sized(c, cond, body):
        for value, count in sizes:
            when(both(cond, None if value is None else c == value), functools.partial(body, count * 128))

    own_copy = pltpu.make_async_copy(cents_in.at[:, pl.ds(0, full)], own.at[:, pl.ds(0, full)], local_sem.at[0])
    docs_copy = pltpu.make_async_copy(docs_in, docs.at[0], local_sem.at[1])
    ids_copy = pltpu.make_async_copy(ids_in, ids.at[0], local_sem.at[2])
    own_copy.start()
    if full < width:
        raw_copy = pltpu.make_async_copy(cents_in.at[:, pl.ds(full, width - full)], raw, local_sem.at[3])
        raw_copy.start()
    docs_copy.start()
    ids_copy.start()

    barrier = pltpu.get_barrier_semaphore()

    def greet(to):
        pl.semaphore_signal(barrier, inc=1, device_id=to, device_id_type=MESH)

    pl.when(inner)(lambda: greet(device(0, out)))
    greet(device(0, -out))
    for r in (4, 5, 2, 1):
        greet(device(r))
    if small < big:
        @pl.when(core == 0)
        def _():
            buf[:, pl.ds(small * 128, 128)] = jnp.zeros((buf.shape[0], 128), buf.dtype)
    if full < width:
        raw_copy.wait()
        own[:, pl.ds(full, 128)] = jnp.concatenate(
            [raw[...], jnp.zeros((feat, full + 128 - width), raw.dtype)], axis=1)
    own_copy.wait()
    docs_copy.wait()
    ids_copy.wait()
    pl.semaphore_wait(barrier, 5 + inner.astype(jnp.int32))

    outward, inward, traded, doc_sent, id_sent, result_sent = (send_sem.at[i] for i in range(6))

    def start(make, cond=None):
        when(cond, lambda: make().start())

    def start_sized(make, c, cond=None):
        sized(c, cond, lambda w: make(w).start())

    def remote(src, dst, ss, rs, to):
        return pltpu.make_async_remote_copy(
            src_ref=src, dst_ref=dst, send_sem=ss, recv_sem=rs, device_id=to, device_id_type=MESH)

    near = (0, 1, 4, 5)

    def source(layer, j):
        r = near[j]
        there = (layer * 2 + (1 - x if r // 4 else x)) * 2 + (1 - core if r % 2 else core)
        return pl.ds(pl.multiple_of(there * feat, 16), feat)

    def columns(r, w):
        xd = 1 - x if r // 4 else x
        cd = 1 - core if r % 2 else core
        return pl.ds(pl.multiple_of((xd * per + cd * small) * 128, 128), w)

    mine = source(z, 0)

    def exchange(j):
        r = near[j]
        start_sized(lambda w: remote(own.at[:, columns(r, w)], buf.at[mine, pl.ds(0, w)],
                                     traded, c_recv.at[z, j], device(r)),
                    1 - core if r % 2 else core)

    def landed(layer, j, cond=None):
        rows = source(layer, j)
        sized(core, cond, lambda w: remote(
            buf.at[rows, pl.ds(0, w)], buf.at[rows, pl.ds(0, w)], traded, c_recv.at[layer, j],
            device(1)).wait_recv())

    def carry(layer, j, way, s, cond=None):
        rows = source(layer, j)
        src = (lambda w: own.at[:, columns(0, w)]) if s == 0 and j == 0 else (lambda w: buf.at[rows, pl.ds(0, w)])
        start_sized(lambda w: remote(src(w), buf.at[rows, pl.ds(0, w)], inward if way else outward,
                                     c_recv.at[layer, j], device(0, -out if way else out)), core, cond)

    def spread(j):
        if j:
            landed(z, j)
        carry(z, j, 0, 0, inner)
        carry(z, j, 1, 0)

    def relay(j):
        landed(z - out, j)
        carry(z - out, j, 0, 1, inner)
        landed(z + out, j, inner)
        carry(z + out, j, 1, 1, inner)

    def pair(layer, k, w):
        rows = pl.ds(pl.multiple_of((layer * 2 + 1 - x) * 2 * feat, 16), 2 * feat)
        c = chunks[k][0]
        return buf.at[rows, pl.ds(c, min(w, c + chunks[k][1]) - c)]

    def relay_far(j):
        landed(z - 2 * out, j)
        if j < 2:
            carry(z - 2 * out, j, 0, 2, inner)
        elif j == 3:
            for k in range(len(chunks)):
                start_sized(lambda w, k=k: remote(
                    pair(z - 2 * out, k, w), pair(z - 2 * out, k, w), outward, last_recv.at[k],
                    device(0, out)), core, inner)

    def last_landed(k):
        sized(core, end, lambda w: remote(
            pair(z - 3 * out, k, w), pair(z - 3 * out, k, w), outward, last_recv.at[k],
            device(1)).wait_recv())

    ahead = {(1, 0): 0, (1, 1): 0, (1, 2): 0, (3, 0): 1, (3, 1): 1, (3, 2): 1, (5, 0): 2, (5, 1): 2, (5, 2): 2,
             (7, 0): 3, (7, 1): 3, (7, 2): 3, (2, 0): 4, (2, 1): 5, (2, 2): 5, (4, 0): 6, (4, 1): 7, (4, 2): 8,
             (6, 0): 9, (6, 1): 10, (6, 2): 11}
    id_at = {1: 0, 3: 0, 5: 0, 7: 0, 2: 1, 4: 2, 6: 3}

    def part(slot, *parts):
        first, last = spans[parts[0]], spans[parts[-1]]
        return docs.at[slot, pl.ds(first[0], last[0] + last[1] - first[0]), :]

    def send_docs(src_slot, dst_slot, r, *parts):
        start(lambda: remote(part(src_slot, *parts), part(dst_slot, *parts), doc_sent,
                             d_recv.at[ahead[dst_slot, parts[0]]], device(r)))

    def send_ids(src_slot, dst_slot, r):
        start(lambda: remote(ids.at[src_slot], ids.at[dst_slot], id_sent, i_recv.at[id_at[dst_slot]], device(r)))

    def have_docs(slot, *parts):
        remote(part(slot, *parts), part(slot, *parts), doc_sent, d_recv.at[ahead[slot, parts[0]]],
               device(1)).wait_recv()

    def have_ids(slot):
        some = ids.at[pl.ds(0, 4)] if slot % 2 else ids.at[slot]
        remote(some, some, id_sent, i_recv.at[id_at[slot]], device(1)).wait_recv()

    def share(slot, *parts):
        send_docs(slot, slot + 1, 1, *parts)

    spread(0)
    for j in (1, 2, 3):
        exchange(j)
    send_ids(0, 2, 2)
    send_docs(0, 2, 2, 0)
    send_docs(0, 2, 2, 1, 2)
    send_ids(0, 4, 4)
    for p in (1, 2, 0):
        send_docs(0, 4, 4, p)
    send_ids(0, 1, 1)
    send_docs(0, 1, 1, 0, 1, 2)

    part_cols = jnp.where(core == 1, big, small) * 128
    first = (x * per + core * small) * 128
    base = doc * width + first
    reach = jnp.minimum(part_cols, width - first)
    down = lax.broadcasted_iota(jnp.int32, (GROUP, 128), 0)

    def prepare_ids(slot):
        rel = ids[slot] - base
        rel = jnp.where((rel >= 0) & (rel < reach), rel, -(2**20))
        tall = jnp.broadcast_to(rel, (GROUP, rows_dev))
        idb[:, pl.ds(slot * rows_dev, rows_dev)] = tall - lax.broadcasted_iota(jnp.int32, (GROUP, rows_dev), 0)

    buf[mine, pl.ds(0, small * 128)] = own[:, columns(0, small * 128)]
    if small < big:
        @pl.when(core == 1)
        def _():
            start_col = pl.multiple_of((x * per + 2 * small) * 128, 128)
            buf[mine, pl.ds(small * 128, 128)] = own[:, pl.ds(start_col, 128)]

    k1_at = pl.multiple_of(jnp.where(upper, depth - k1, 0), 256)
    k2_at = pl.multiple_of(jnp.where(upper, late, k1), 256)
    late_at = pl.multiple_of(jnp.where(upper, 0, depth - late), 256)
    starts = (k1_at, k2_at, late_at)

    def squares(i, c, w):
        w32 = buf[pl.ds(starts[i], 256), pl.ds(c, w)].astype(jnp.float32)
        return jnp.sum((w32 * w32).reshape(32, 8, w), 0)

    def turn(i, c, w):
        turned[i, pl.ds(c, w), :] = buf[pl.ds(starts[i], 256), pl.ds(c, w)].T

    def gather(i):
        for c, w in chunks:
            turn(i, c, w)
        csq[...] = squares(i, 0, wide) + (csq[...] if i else 0.0)

    def flatten(*slots):
        for slot in slots:
            flat[:, pl.ds(slot * rows_dev, rows_dev)] = docs[slot].T

    def times(i, c, w, slot, count):
        return jnp.dot(turned[i, pl.ds(c, w), :],
                       flat[pl.ds(starts[i], 256), pl.ds(slot * rows_dev, count * rows_dev)],
                       preferred_element_type=jnp.float32)

    def begin(slot, count, *phases):
        where_docs = pl.ds(slot * rows_dev, count * rows_dev)
        prod = times(phases[0], 0, wide, slot, count)
        for i in phases[1:]:
            prod = prod + times(i, 0, wide, slot, count)
        if phases[0]:
            acc[:, where_docs] += prod
        else:
            acc[:, where_docs] = prod

    spread(1)
    prepare_ids(0)
    flatten(0)
    spread(2)
    relay(0)
    spread(3)
    relay(1)
    have_docs(2, 0)
    send_docs(2, 6, 4, 0)
    have_ids(4)
    send_ids(4, 6, 2)
    send_ids(4, 5, 1)
    have_ids(2)
    send_ids(2, 3, 1)
    relay(2)
    have_docs(4, 1)
    send_docs(4, 6, 2, 1)
    have_docs(1, 0, 1, 2)
    flatten(1)
    relay(3)
    relay_far(0)
    have_docs(2, 1, 2)
    share(2, 0, 1, 2)
    have_docs(4, 2)
    send_docs(4, 6, 2, 2)
    have_ids(6)
    send_ids(6, 7, 1)
    relay_far(1)
    gather(0)
    begin(0, 2, 0)
    flatten(2)
    have_ids(1)
    for slot in (1, 2, 3, 4, 5, 6, 7):
        prepare_ids(slot)
    relay_far(2)
    have_docs(4, 0)
    share(4, 0, 1, 2)
    have_docs(3, 0, 1, 2)
    flatten(3)
    begin(2, 2, 0)
    relay_far(3)
    gather(1)
    flatten(4)
    begin(0, 2, 1)
    begin(2, 2, 1)
    have_docs(5, 0, 1, 2)
    flatten(5)
    begin(4, 2, 0, 1)
    for p in (1, 2, 0):
        have_docs(6, p)
    share(6, 0, 1, 2)
    flatten(6)

    def scales(c, w):
        total = jnp.sum(csq[:, pl.ds(c, w)] + squares(2, c, w), 0, keepdims=True)
        scale[pl.ds(c, w), :] = jnp.broadcast_to(lax.rsqrt(total + epsilon), (128, w)).T

    def stage(c0, w, slot, count):
        prod = times(2, c0, w, slot, count)
        spots = [pl.ds(slot * rows_dev + d, 128) for d in range(0, count * rows_dev, 128)]
        if c0:
            tops, hits = [mx[:, at] for at in spots], [ch[:, at] for at in spots]
        else:
            tops = [jnp.full((GROUP, 128), -3.0e38, jnp.float32)] * len(spots)
            hits = [jnp.zeros((GROUP, 128), jnp.float32)] * len(spots)
        for c in range(0, w, GROUP):
            rows = pl.ds(c0 + c, GROUP)
            by = scale[rows, :]
            for n, at in enumerate(spots):
                v = (acc[rows, at] + prod[c:c + GROUP, n * 128:n * 128 + 128]) * by
                hits[n] = jnp.where(idb[:, at] == c0 + c, v, hits[n])
                if c0 + c + 128 > small * 128:
                    v = jnp.where(down < reach - (c0 + c), v, -3.0e38)
                tops[n] = jnp.maximum(tops[n], v)
        for n, at in enumerate(spots):
            mx[:, at], ch[:, at] = tops[n], hits[n]

    def reduced(slot):
        at = pl.ds(slot * rows_dev, rows_dev)
        return jnp.max(mx[:, at], 0, keepdims=True), jnp.sum(ch[:, at], 0, keepdims=True)

    def give(slot):
        best, chosen = reduced(slot)
        res[slot, 0:1, :] = best
        res[slot, 1:2, :] = chosen
        remote(res.at[slot], got.at[slot], result_sent, r_recv, device(slot)).start()

    x32 = docs[0].astype(jnp.float32)
    sq = x32 * x32
    total = sq[:, 0:128]
    for c in range(128, depth, 128):
        total = total + sq[:, c:c + 128]
    scale_x = lax.rsqrt(jnp.sum(total.T, 0, keepdims=True) + epsilon)

    landed(z - 3 * out, 0, end)
    landed(z - 3 * out, 1, end)
    have_docs(7, 0, 1, 2)
    flatten(7)
    begin(6, 2, 0, 1)
    final = len(chunks) - 1
    for i in range(final):
        last_landed(i)
        c, w = chunks[i]
        turn(2, c, w)
        scales(c, w)
        for slot in (0, 2, 4, 6):
            stage(c, w, slot, 2)
    last_landed(final)

    def finish(have):
        c = chunks[final][0]
        w = have - c
        turn(2, c, w)
        scales(c, w)
        stage(c, w, 6, 2)
        give(6)
        give(7)
        stage(c, w, 2, 2)
        give(2)
        give(3)
        stage(c, w, 4, 2)
        give(4)
        give(5)
        stage(c, w, 0, 2)
        give(1)

    sized(core, None, finish)
    best, chosen = reduced(0)
    everyone = pl.ds(1, 7)
    remote(got.at[everyone], got.at[everyone], result_sent, r_recv, device(1)).wait_recv()
    for slot in range(1, 8):
        best = jnp.maximum(best, got[slot, 0:1, :])
        chosen = chosen + got[slot, 1:2, :]
    near_out[...] = best * scale_x
    chosen_out[...] = chosen * scale_x

    def sent(ref, sem):
        remote(ref, ref, sem, r_recv, device(1)).wait_send()

    sent(res.at[everyone], result_sent)
    sent(docs.at[everyone], doc_sent)
    sent(ids.at[everyone], id_sent)
    layer = 4 * feat
    sized(core, inner, lambda w: sent(buf.at[pl.ds(0, 3 * layer), pl.ds(0, w)], outward))
    sized(core, inner, lambda w: sent(buf.at[pl.ds(0, 2 * layer), pl.ds(0, w)], inward))
    sized(core, end, lambda w: sent(buf.at[pl.ds(0, layer), pl.ds(0, w)], inward))
    sized(core, None, lambda w: sent(own.at[:, pl.ds(0, 2 * per * 128 - w)], traded))


def by_layers(docs, centroids, assigned):
    nz = lax.axis_size("clu") // 4
    rows_dev, depth = docs.shape
    width, feat = centroids.shape
    tiles = -(-width // 128)
    wide = (tiles // 2 - tiles // 4) * 128
    any_space = pl.BlockSpec(memory_space=pl.ANY)
    vmem = pl.BlockSpec(memory_space=pltpu.VMEM)
    dma = pltpu.SemaphoreType.DMA
    line = pltpu.VMEM((1, rows_dev), jnp.float32)
    near, chosen = pl.pallas_call(
        functools.partial(layer_kernel, nz, feat),
        out_shape=(line, line),
        in_specs=[any_space] * 3,
        out_specs=(vmem, vmem),
        scratch_shapes=[
            pltpu.VMEM((feat, tiles * 128), jnp.bfloat16),
            pltpu.VMEM((feat, width % 128 or 128), jnp.bfloat16),
            pltpu.VMEM((depth, wide), jnp.bfloat16),
            pltpu.VMEM((8, rows_dev, depth), jnp.bfloat16),
            pltpu.VMEM((depth, 8 * rows_dev), jnp.bfloat16),
            pltpu.VMEM((8, 1, rows_dev), jnp.int32),
            pltpu.VMEM((3, wide, 256), jnp.bfloat16),
            pltpu.VMEM((wide, 8 * rows_dev), jnp.float32),
            pltpu.VMEM((GROUP, 8 * rows_dev), jnp.int32),
            pltpu.VMEM((GROUP, 8 * rows_dev), jnp.float32),
            pltpu.VMEM((GROUP, 8 * rows_dev), jnp.float32),
            pltpu.VMEM((8, wide), jnp.float32),
            pltpu.VMEM((wide, 128), jnp.float32),
            pltpu.VMEM((8, 2, rows_dev), jnp.float32),
            pltpu.VMEM((8, 2, rows_dev), jnp.float32),
            dma((4,)), dma((6,)), dma((nz, 4)), dma((-(-wide // 256),)), dma((12,)), dma((4,)), dma,
        ],
        compiler_params=pltpu.CompilerParams(collective_id=0, has_side_effects=True),
        name="layer_distances",
    )(docs, centroids.T, assigned.reshape(1, rows_dev))
    return 1.0 - near.reshape(rows_dev), 1.0 - chosen.reshape(rows_dev)


def fits_layers(docs, centroids):
    tiles = -(-centroids.shape[0] // 128)
    n_clu, feat = lax.axis_size("clu"), centroids.shape[1]
    return (lax.axis_size("doc") == 2 and n_clu == 16 and tiles % 2 == 0 and tiles >= 4
            and feat % 16 == 0 and docs.shape[0] % 128 == 0 and docs.shape[1] % 256 == 0
            and docs.shape[1] == n_clu * feat == 3 * 256)


def on_device(docs, centroids, assigned):
    if fits_layers(docs, centroids):
        return by_layers(docs, centroids, assigned)
    n_clu, nd = lax.axis_size("clu"), lax.axis_size("doc")
    n = n_clu // 2
    rows_dev, depth = docs.shape
    width, feat = centroids.shape
    fp = (feat + 15) // 16 * 16
    cents = centroids.T
    if fp != feat:
        cents = jnp.pad(cents, ((0, fp - feat), (0, 0)))
    rows = nd * rows_dev
    any_space = pl.BlockSpec(memory_space=pl.ANY)
    vmem = pl.BlockSpec(memory_space=pltpu.VMEM)
    dma = pltpu.SemaphoreType.DMA
    hops = n // 2
    line = jax.ShapeDtypeStruct((1, rows_dev), jnp.float32)
    near, chosen = pl.pallas_call(
        functools.partial(kernel, n, nd, feat),
        out_shape=(line, line),
        in_specs=[any_space] * 3,
        out_specs=(vmem, vmem),
        scratch_shapes=[
            pltpu.VMEM((n_clu * fp, width), jnp.bfloat16),
            pltpu.VMEM((nd, rows_dev, depth), jnp.bfloat16),
            pltpu.VMEM((nd, 1, rows_dev), jnp.int32),
            pltpu.VMEM((rows, (n - 3) * 2 * fp), jnp.bfloat16),
            pltpu.VMEM((rows, 4 * fp), jnp.bfloat16),
            pltpu.VMEM((rows, 2 * fp), jnp.bfloat16),
            pltpu.VMEM((rows, width), jnp.float32),
            pltpu.VMEM((rows, 128), jnp.int32),
            pltpu.VMEM((rows, 128), jnp.float32),
            pltpu.VMEM((rows, 128), jnp.float32),
            pltpu.VMEM((8, width), jnp.float32),
            pltpu.VMEM((1, width), jnp.float32),
            pltpu.VMEM((nd, 2, rows_dev), jnp.float32),
            pltpu.VMEM((nd, 2, rows_dev), jnp.float32),
            dma((3,)),
            dma((2, hops, PIECES)),
            dma((n, PIECES)),
            dma((n, 2, PIECES)),
            dma((nd,)), dma((nd,)), dma((nd,)), dma((nd,)), dma((nd,)), dma((nd,)),
        ],
        compiler_params=pltpu.CompilerParams(collective_id=0, has_side_effects=True),
        name="ring_distances",
    )(docs, cents, assigned.reshape(1, rows_dev))
    return 1.0 - near.reshape(rows_dev), 1.0 - chosen.reshape(rows_dev)


def solution(mesh):
    placed = (P(("clu", "doc"), None), P("doc", "clu"), P(("clu", "doc")))
    return jax.shard_map(
        on_device,
        mesh=mesh,
        in_specs=placed,
        out_specs=(P(("clu", "doc")), P(("clu", "doc"))),
        check_vma=False,
    )
```

```python
import functools

import jax
import jax.numpy as jnp
from jax import lax
from jax.experimental import pallas as pl
from jax.experimental.pallas import tpu as pltpu
from jax.sharding import PartitionSpec as P

epsilon = 1e-06
PIECES = 4
ROWS = 64
GROUP = 16
MESH = pl.DeviceIdType.MESH


def chip_at(pos, n):
    half = n // 2
    return jnp.where(pos < half, 2 * pos, 2 * (n - 1 - pos) + 1)


def cut(width):
    tiles = (width + 127) // 128
    ends = [min(-(-tiles * (c + 1) // PIECES) * 128, width) for c in range(PIECES)]
    return tuple((a, b - a) for a, b in zip([0] + ends[:-1], ends))


def kernel(n, nd, feat, docs_in, cents_in, ids_in, near_out, chosen_out,
           buf, docs_all, ids_all, dp_a, dp_b, dp_c, acc, idb, mx, ch, csq, scale, res, got,
           local_sem, ring_send, pair_send, recv, docs_send, docs_recv, ids_send, ids_recv,
           res_send, res_recv):
    hops = n // 2
    fp = cents_in.shape[0]
    width = cents_in.shape[1]
    rows_dev = docs_in.shape[0]
    chunks = cut(width)
    half = len(chunks) // 2

    clu, doc = lax.axis_index("clu"), lax.axis_index("doc")
    core, chip = lax.rem(clu, 2), lax.div(clu, 2)
    z, x = lax.div(chip, 2), lax.rem(chip, 2)
    pos = jnp.where(x == 0, z, n - 1 - z)
    right = chip_at(lax.rem(pos + 1, n), n) * 2 + core
    left = chip_at(lax.rem(pos + n - 1, n), n) * 2 + core
    partner = chip * 2 + (1 - core)

    own_c = pltpu.make_async_copy(cents_in, buf.at[pl.ds(0, fp), :], local_sem.at[0])
    own_d = pltpu.make_async_copy(docs_in, docs_all.at[0], local_sem.at[1])
    own_i = pltpu.make_async_copy(ids_in, ids_all.at[0], local_sem.at[2])
    own_c.start()
    own_d.start()
    own_i.start()

    barrier = pltpu.get_barrier_semaphore()
    for peer in (left, right, partner):
        pl.semaphore_signal(barrier, inc=1, device_id={"clu": peer}, device_id_type=MESH)
    for k in range(1, nd):
        pl.semaphore_signal(barrier, inc=1, device_id={"doc": lax.rem(doc + k, nd)}, device_id_type=MESH)
    pl.semaphore_wait(barrier, 3 + nd - 1)

    def slot(way, h):
        if h == 0:
            return 0
        if h == hops:
            return n - 1
        return 2 * h - 1 if way == 0 else 2 * h

    def piece(s, m, c):
        return buf.at[pl.ds((2 * s + m) * fp, fp), pl.ds(*chunks[c])]

    def reach(way, c):
        return hops if way == c // half else hops - 1

    sent = []

    def ring(way, h, c):
        s, t = slot(way, h), slot(way, h + 1)
        copy = pltpu.make_async_remote_copy(
            src_ref=piece(s, 0, c), dst_ref=piece(t, 0, c),
            send_sem=ring_send.at[way, h, c], recv_sem=recv.at[t, 0, c],
            device_id={"clu": right if way == 0 else left}, device_id_type=MESH)
        copy.start()
        sent.append(copy)

    def share(s, c):
        copy = pltpu.make_async_remote_copy(
            src_ref=piece(s, 0, c), dst_ref=piece(s, 1, c),
            send_sem=pair_send.at[s, c], recv_sem=recv.at[s, 1, c],
            device_id={"clu": partner}, device_id_type=MESH)
        copy.start()
        sent.append(copy)

    def landed(s, m, c):
        pltpu.make_async_remote_copy(
            src_ref=piece(s, m, c), dst_ref=piece(s, m, c),
            send_sem=pair_send.at[s, c], recv_sem=recv.at[s, m, c],
            device_id={"clu": partner}, device_id_type=MESH).wait_recv()

    own_c.wait()
    for i in range(PIECES):
        ring(0, 0, i)
        ring(1, 0, (i + half) % PIECES)
    for c in range(PIECES):
        share(0, c)
    own_d.wait()
    own_i.wait()
    doc_copies = []
    for k in range(1, nd):
        mate = lax.rem(doc + k, nd)
        for ref, ss, rs in ((ids_all, ids_send, ids_recv), (docs_all, docs_send, docs_recv)):
            copy = pltpu.make_async_remote_copy(
                src_ref=ref.at[0], dst_ref=ref.at[k], send_sem=ss.at[k], recv_sem=rs.at[k],
                device_id={"doc": mate}, device_id_type=MESH)
            copy.start()
            doc_copies.append(copy)

    def owner(s):
        if s == 0:
            p = pos
        elif s == n - 1:
            p = pos + hops
        elif s % 2:
            p = pos + n - (s + 1) // 2
        else:
            p = pos + s // 2
        return chip_at(lax.rem(p, n), n)

    ranges = ((0, n - 3), (n - 3, n - 1), (n - 1, n))
    spread = (dp_a, dp_b, dp_c)

    def permute(k):
        rows = docs_all[k]
        for (first, last), out in zip(ranges, spread):
            wide = out.shape[1]
            lane = lax.broadcasted_iota(jnp.int32, (1, wide), 1)
            target = jnp.full((1, wide), -1, jnp.int32)
            for s in range(first, last):
                chip_s = owner(s)
                for m in (0, 1):
                    part = chip_s * 2 + (core if m == 0 else 1 - core)
                    start = (2 * (s - first) + m) * fp
                    inside = (lane >= start) & (lane < start + feat)
                    target = jnp.where(inside, lane - start + part * feat, target)
            source = lax.broadcasted_iota(jnp.int32, (rows.shape[1], wide), 0)
            mover = jnp.where(source == target, 1.0, 0.0).astype(jnp.bfloat16)
            out[pl.ds(k * rows_dev, rows_dev), :] = jnp.dot(
                rows, mover, preferred_element_type=jnp.float32).astype(jnp.bfloat16)

    def prepare_ids(k):
        base = doc * width
        ids = ids_all[k] - base
        ids = jnp.where((ids >= 0) & (ids < width), ids, -1)
        full = jnp.broadcast_to(ids, (128, rows_dev)).T
        lanes = lax.broadcasted_iota(jnp.int32, (rows_dev, 128), 1)
        idb[pl.ds(k * rows_dev, rows_dev), :] = jnp.where(full >= 0, full - lanes, -(2**20))

    def phase(index, c):
        first, last = ranges[index]
        start, depth = 2 * first * fp, 2 * (last - first) * fp
        cols = pl.ds(*chunks[c])
        block = buf[pl.ds(start, depth), cols]
        prod = jnp.dot(spread[index][...], block, preferred_element_type=jnp.float32)
        w32 = block.astype(jnp.float32)
        sq = jnp.sum((w32 * w32).reshape(depth // 8, 8, chunks[c][1]), 0)
        if index == 0:
            acc[:, cols] = prod
            csq[:, cols] = sq
        else:
            acc[:, cols] += prod
            csq[:, cols] += sq

    tail = pl.ds(2 * (n - 1) * fp, 2 * fp)

    def finish_scale(c):
        cols = pl.ds(*chunks[c])
        w32 = buf[tail, cols].astype(jnp.float32)
        sq = jnp.sum((w32 * w32).reshape(2 * fp // 8, 8, chunks[c][1]), 0) + csq[:, cols]
        scale[:, cols] = lax.rsqrt(jnp.sum(sq, 0, keepdims=True) + epsilon)

    def final(k, c):
        start, wide = chunks[c]
        prod = jnp.dot(dp_c[pl.ds(k * rows_dev, rows_dev), :], buf[tail, pl.ds(start, wide)],
                       preferred_element_type=jnp.float32)
        for r in range(0, rows_dev, ROWS):
            rs = pl.ds(k * rows_dev + r, ROWS)
            top, hit = mx[rs, :], ch[rs, :]
            ids = idb[rs, :]
            for a in range(0, wide, 128):
                w = min(128, wide - a)
                cols = pl.ds(start + a, w)
                v = (acc[rs, cols] + prod[r:r + ROWS, a:a + w]) * scale[:, cols]
                if w == 128:
                    top = jnp.maximum(top, v)
                    hit = jnp.where(ids == start + a, v, hit)
                else:
                    mx[rs, :] = top
                    ch[rs, :] = hit
                    mx[rs, pl.ds(0, w)] = jnp.maximum(mx[rs, pl.ds(0, w)], v)
                    ch[rs, pl.ds(0, w)] = jnp.where(idb[rs, pl.ds(0, w)] == start + a, v, ch[rs, pl.ds(0, w)])
            if wide % 128 == 0:
                mx[rs, :] = top
                ch[rs, :] = hit

    def reduced(k):
        rs = pl.ds(k * rows_dev, rows_dev)
        return (jnp.max(mx[rs, :].T, 0, keepdims=True), jnp.sum(ch[rs, :].T, 0, keepdims=True))

    mx[...] = jnp.full(mx.shape, -3.0e38, jnp.float32)
    ch[...] = jnp.zeros(ch.shape, jnp.float32)
    permute(0)
    prepare_ids(0)
    wide = docs_all[0].astype(jnp.float32)
    squares = wide * wide
    total = squares[:, 0:128]
    for a in range(128, wide.shape[1], 128):
        total = total + squares[:, a:a + 128]
    scale_x = lax.rsqrt(jnp.sum(total.T, 0, keepdims=True) + epsilon)

    def step(way, h, c):
        s = slot(way, h)
        landed(s, 0, c)
        if h < reach(way, c):
            ring(way, h, c)
        share(s, c)

    def pair(h, i):
        step(0, h, i)
        step(1, h, (i + half) % PIECES)

    def partners(slots, c):
        for s in slots:
            landed(s, 1, c)

    early, late = range(n - 3), (n - 3, n - 2)
    order = [j // 2 + half * (j % 2) for j in range(PIECES)]
    for h in range(1, hops):
        for i in range(PIECES):
            pair(h, i)
            if h == hops - 2 and i == half:
                for copy in doc_copies:
                    copy.wait()
                for k in range(1, nd):
                    permute(k)
                    prepare_ids(k)
            if h == hops - 1:
                c = order[i]
                partners(early, c)
                phase(0, c)
    for c in order[:half]:
        partners(late, c)
        phase(1, c)
    for i in range(half):
        for way in (0, 1):
            c = i + half * way
            landed(n - 1, 0, c)
            share(n - 1, c)
    for c in order[half:]:
        partners(late, c)
        phase(1, c)
    for c in order[:-2]:
        landed(n - 1, 1, c)
        finish_scale(c)
        for k in range(nd):
            final(k, c)
    for c in order[-2:]:
        landed(n - 1, 1, c)
        finish_scale(c)

    returns = []
    for k in range(1, nd):
        for c in order[-2:]:
            final(k, c)
        best, chosen = reduced(k)
        res[k, 0:1, :] = best
        res[k, 1:2, :] = chosen
        copy = pltpu.make_async_remote_copy(
            src_ref=res.at[k], dst_ref=got.at[k], send_sem=res_send.at[k], recv_sem=res_recv.at[k],
            device_id={"doc": lax.rem(doc + nd - k, nd)}, device_id_type=MESH)
        copy.start()
        returns.append(copy)
    for c in order[-2:]:
        final(0, c)
    best, chosen = reduced(0)
    for k in range(1, nd):
        returns[k - 1].wait()
        best = jnp.maximum(best, got[k, 0:1, :])
        chosen = chosen + got[k, 1:2, :]
    near_out[...] = best * scale_x
    chosen_out[...] = chosen * scale_x
    for copy in sent:
        copy.wait_send()


def layer_kernel(nz, feat, docs_in, cents_in, ids_in, near_out, chosen_out,
                 own, raw, buf, docs, flat, ids, turned, acc, idb, mx, ch, csq, scale, res, got,
                 local_sem, send_sem, c_recv, last_recv, d_recv, i_recv, r_recv):
    width = cents_in.shape[1]
    rows_dev, depth = docs_in.shape
    tiles = own.shape[1] // 128
    per = tiles // 2
    small = per // 2
    big = per - small
    wide = big * 128
    full = width // 128 * 128
    late = -(-4 * feat // 256) * 256
    k1 = 8 * feat // 256 * 256
    k2 = depth - late - k1
    a = rows_dev * 5 // 16 // 16 * 16
    b = (rows_dev - a) // 32 * 16
    spans = ((0, a), (a, b), (a + b, rows_dev - a - b))
    cuts = {w: (0, 256, (w - 1) // 256 * 256, w) for w in (small * 128, wide)}

    clu, doc = lax.axis_index("clu"), lax.axis_index("doc")
    core, chip = lax.rem(clu, 2), lax.div(clu, 2)
    z, x = lax.div(chip, 2), lax.rem(chip, 2)
    upper = z >= nz // 2
    out = jnp.where(upper, 1, -1)
    end = (z == 0) | (z == nz - 1)
    inner = jnp.logical_not(end)

    def device(r, dz=0):
        dx, dy, dc = r // 4, r // 2 % 2, r % 2
        there = ((z + dz) * 2 + (1 - x if dx else x)) * 2 + (1 - core if dc else core)
        return {"clu": there, "doc": 1 - doc if dy else doc}

    def when(cond, body):
        if cond is None:
            body()
        else:
            pl.when(cond)(body)

    def both(p, q):
        return q if p is None else p if q is None else p & q

    sizes = ((None, big),) if big == small else ((1, big), (0, small))

    def sized(c, cond, body):
        for value, count in sizes:
            when(both(cond, None if value is None else c == value), functools.partial(body, count * 128))

    own_copy = pltpu.make_async_copy(cents_in.at[:, pl.ds(0, full)], own.at[:, pl.ds(0, full)], local_sem.at[0])
    docs_copy = pltpu.make_async_copy(docs_in, docs.at[0], local_sem.at[1])
    ids_copy = pltpu.make_async_copy(ids_in, ids.at[0], local_sem.at[2])
    own_copy.start()
    if full < width:
        raw_copy = pltpu.make_async_copy(cents_in.at[:, pl.ds(full, width - full)], raw, local_sem.at[3])
        raw_copy.start()
    docs_copy.start()
    ids_copy.start()

    barrier = pltpu.get_barrier_semaphore()

    def greet(to):
        pl.semaphore_signal(barrier, inc=1, device_id=to, device_id_type=MESH)

    pl.when(inner)(lambda: greet(device(0, out)))
    greet(device(0, -out))
    for r in (4, 5, 2, 1):
        greet(device(r))
    if small < big:
        @pl.when(core == 0)
        def _():
            buf[:, pl.ds(small * 128, 128)] = jnp.zeros((buf.shape[0], 128), buf.dtype)
    if full < width:
        raw_copy.wait()
        own[:, pl.ds(full, 128)] = jnp.concatenate(
            [raw[...], jnp.zeros((feat, full + 128 - width), raw.dtype)], axis=1)
    own_copy.wait()
    docs_copy.wait()
    ids_copy.wait()
    pl.semaphore_wait(barrier, 5 + inner.astype(jnp.int32))

    outward, inward, traded, doc_sent, id_sent, result_sent = (send_sem.at[i] for i in range(6))

    def start(make, cond=None):
        when(cond, lambda: make().start())

    def start_sized(make, c, cond=None):
        sized(c, cond, lambda w: make(w).start())

    def remote(src, dst, ss, rs, to):
        return pltpu.make_async_remote_copy(
            src_ref=src, dst_ref=dst, send_sem=ss, recv_sem=rs, device_id=to, device_id_type=MESH)

    near = (0, 1, 4, 5)

    def source(layer, j):
        r = near[j]
        there = (layer * 2 + (1 - x if r // 4 else x)) * 2 + (1 - core if r % 2 else core)
        return pl.ds(pl.multiple_of(there * feat, 16), feat)

    def columns(r, w):
        xd = 1 - x if r // 4 else x
        cd = 1 - core if r % 2 else core
        return pl.ds(pl.multiple_of((xd * per + cd * small) * 128, 128), w)

    mine = source(z, 0)

    def exchange(j):
        r = near[j]
        start_sized(lambda w: remote(own.at[:, columns(r, w)], buf.at[mine, pl.ds(0, w)],
                                     traded, c_recv.at[z, j], device(r)),
                    1 - core if r % 2 else core)

    def landed(layer, j, cond=None):
        rows = source(layer, j)
        sized(core, cond, lambda w: remote(
            buf.at[rows, pl.ds(0, w)], buf.at[rows, pl.ds(0, w)], traded, c_recv.at[layer, j],
            device(1)).wait_recv())

    def carry(layer, j, way, s, cond=None):
        rows = source(layer, j)
        src = (lambda w: own.at[:, columns(0, w)]) if s == 0 and j == 0 else (lambda w: buf.at[rows, pl.ds(0, w)])
        start_sized(lambda w: remote(src(w), buf.at[rows, pl.ds(0, w)], inward if way else outward,
                                     c_recv.at[layer, j], device(0, -out if way else out)), core, cond)

    def spread(j):
        if j:
            landed(z, j)
        carry(z, j, 0, 0, inner)
        carry(z, j, 1, 0)

    def relay(j):
        landed(z - out, j)
        carry(z - out, j, 0, 1, inner)
        landed(z + out, j, inner)
        carry(z + out, j, 1, 1, inner)

    def pair(layer, k, w):
        rows = pl.ds(pl.multiple_of((layer * 2 + 1 - x) * 2 * feat, 16), 2 * feat)
        return buf.at[rows, pl.ds(cuts[w][k], cuts[w][k + 1] - cuts[w][k])]

    def relay_far(j):
        landed(z - 2 * out, j)
        if j < 2:
            carry(z - 2 * out, j, 0, 2, inner)
        elif j == 3:
            for k in range(3):
                start_sized(lambda w, k=k: remote(
                    pair(z - 2 * out, k, w), pair(z - 2 * out, k, w), outward, last_recv.at[k],
                    device(0, out)), core, inner)

    def last_landed(k):
        sized(core, end, lambda w: remote(
            pair(z - 3 * out, k, w), pair(z - 3 * out, k, w), outward, last_recv.at[k],
            device(1)).wait_recv())

    ahead = {(1, 0): 0, (1, 1): 0, (1, 2): 0, (3, 0): 1, (3, 1): 1, (3, 2): 1, (5, 0): 2, (5, 1): 2, (5, 2): 2,
             (7, 0): 3, (7, 1): 3, (7, 2): 3, (2, 0): 4, (2, 1): 5, (2, 2): 5, (4, 0): 6, (4, 1): 7, (4, 2): 8,
             (6, 0): 9, (6, 1): 10, (6, 2): 11}
    id_at = {1: 0, 3: 0, 5: 0, 7: 0, 2: 1, 4: 2, 6: 3}

    def part(slot, *parts):
        first, last = spans[parts[0]], spans[parts[-1]]
        return docs.at[slot, pl.ds(first[0], last[0] + last[1] - first[0]), :]

    def send_docs(src_slot, dst_slot, r, *parts):
        start(lambda: remote(part(src_slot, *parts), part(dst_slot, *parts), doc_sent,
                             d_recv.at[ahead[dst_slot, parts[0]]], device(r)))

    def send_ids(src_slot, dst_slot, r):
        start(lambda: remote(ids.at[src_slot], ids.at[dst_slot], id_sent, i_recv.at[id_at[dst_slot]], device(r)))

    def have_docs(slot, *parts):
        remote(part(slot, *parts), part(slot, *parts), doc_sent, d_recv.at[ahead[slot, parts[0]]],
               device(1)).wait_recv()

    def have_ids(slot):
        some = ids.at[pl.ds(0, 4)] if slot % 2 else ids.at[slot]
        remote(some, some, id_sent, i_recv.at[id_at[slot]], device(1)).wait_recv()

    def share(slot, *parts):
        send_docs(slot, slot + 1, 1, *parts)

    spread(0)
    for j in (1, 2, 3):
        exchange(j)
    send_ids(0, 2, 2)
    send_docs(0, 2, 2, 0)
    send_docs(0, 2, 2, 1, 2)
    send_ids(0, 4, 4)
    for p in (1, 2, 0):
        send_docs(0, 4, 4, p)
    send_ids(0, 1, 1)
    send_docs(0, 1, 1, 0, 1, 2)

    part_cols = jnp.where(core == 1, big, small) * 128
    first = (x * per + core * small) * 128
    base = doc * width + first
    reach = jnp.minimum(part_cols, width - first)
    down = lax.broadcasted_iota(jnp.int32, (GROUP, 128), 0)

    def prepare_ids(slot):
        rel = ids[slot] - base
        rel = jnp.where((rel >= 0) & (rel < reach), rel, -(2**20))
        tall = jnp.broadcast_to(rel, (GROUP, rows_dev))
        idb[:, pl.ds(slot * rows_dev, rows_dev)] = tall - lax.broadcasted_iota(jnp.int32, (GROUP, rows_dev), 0)

    buf[mine, pl.ds(0, small * 128)] = own[:, columns(0, small * 128)]
    if small < big:
        @pl.when(core == 1)
        def _():
            start_col = pl.multiple_of((x * per + 2 * small) * 128, 128)
            buf[mine, pl.ds(small * 128, 128)] = own[:, pl.ds(start_col, 128)]

    k1_at = pl.multiple_of(jnp.where(upper, depth - k1, 0), 256)
    k2_at = pl.multiple_of(jnp.where(upper, late, k1), 256)
    late_at = pl.multiple_of(jnp.where(upper, 0, depth - late), 256)
    starts = (k1_at, k2_at, late_at)

    def squares(i, c, w):
        w32 = buf[pl.ds(starts[i], 256), pl.ds(c, w)].astype(jnp.float32)
        return jnp.sum((w32 * w32).reshape(32, 8, w), 0)

    def turn(i, c, w):
        turned[i, pl.ds(c, w), :] = buf[pl.ds(starts[i], 256), pl.ds(c, w)].T

    def gather(i):
        for c in range(0, wide, 256):
            turn(i, c, min(256, wide - c))
        csq[...] = squares(i, 0, wide) + (csq[...] if i else 0.0)

    def flatten(*slots):
        for slot in slots:
            flat[:, pl.ds(slot * rows_dev, rows_dev)] = docs[slot].T

    def times(i, c, w, slot, count):
        return jnp.dot(turned[i, pl.ds(c, w), :],
                       flat[pl.ds(starts[i], 256), pl.ds(slot * rows_dev, count * rows_dev)],
                       preferred_element_type=jnp.float32)

    def begin(slot, count, *phases):
        where_docs = pl.ds(slot * rows_dev, count * rows_dev)
        prod = times(phases[0], 0, wide, slot, count)
        for i in phases[1:]:
            prod = prod + times(i, 0, wide, slot, count)
        if phases[0]:
            acc[:, where_docs] += prod
        else:
            acc[:, where_docs] = prod

    spread(1)
    prepare_ids(0)
    flatten(0)
    spread(2)
    relay(0)
    spread(3)
    relay(1)
    have_docs(2, 0)
    send_docs(2, 6, 4, 0)
    have_ids(4)
    send_ids(4, 6, 2)
    send_ids(4, 5, 1)
    have_ids(2)
    send_ids(2, 3, 1)
    relay(2)
    have_docs(4, 1)
    send_docs(4, 6, 2, 1)
    have_docs(1, 0, 1, 2)
    flatten(1)
    relay(3)
    relay_far(0)
    have_docs(2, 1, 2)
    share(2, 0, 1, 2)
    have_docs(4, 2)
    send_docs(4, 6, 2, 2)
    have_ids(6)
    send_ids(6, 7, 1)
    relay_far(1)
    gather(0)
    begin(0, 2, 0)
    flatten(2)
    have_ids(1)
    for slot in (1, 2, 3, 4, 5, 6, 7):
        prepare_ids(slot)
    relay_far(2)
    have_docs(4, 0)
    share(4, 0, 1, 2)
    relay_far(3)
    have_docs(3, 0, 1, 2)
    flatten(3)
    begin(2, 2, 0)
    gather(1)
    flatten(4)
    begin(0, 2, 1)
    begin(2, 2, 1)
    have_docs(5, 0, 1, 2)
    flatten(5)
    begin(4, 2, 0, 1)
    for p in (1, 2, 0):
        have_docs(6, p)
    share(6, 0, 1, 2)
    flatten(6)

    def scales(c, w):
        total = jnp.sum(csq[:, pl.ds(c, w)] + squares(2, c, w), 0, keepdims=True)
        scale[pl.ds(c, w), :] = jnp.broadcast_to(lax.rsqrt(total + epsilon), (128, w)).T

    def stage(c0, w, slot, count):
        prod = times(2, c0, w, slot, count)
        spots = [pl.ds(slot * rows_dev + d, 128) for d in range(0, count * rows_dev, 128)]
        if c0:
            tops, hits = [mx[:, at] for at in spots], [ch[:, at] for at in spots]
        else:
            tops = [jnp.full((GROUP, 128), -3.0e38, jnp.float32)] * len(spots)
            hits = [jnp.zeros((GROUP, 128), jnp.float32)] * len(spots)
        for c in range(0, w, GROUP):
            rows = pl.ds(c0 + c, GROUP)
            by = scale[rows, :]
            for n, at in enumerate(spots):
                v = (acc[rows, at] + prod[c:c + GROUP, n * 128:n * 128 + 128]) * by
                hits[n] = jnp.where(idb[:, at] == c0 + c, v, hits[n])
                if c0 + c + 128 > small * 128:
                    v = jnp.where(down < reach - (c0 + c), v, -3.0e38)
                tops[n] = jnp.maximum(tops[n], v)
        for n, at in enumerate(spots):
            mx[:, at], ch[:, at] = tops[n], hits[n]

    def reduced(slot):
        at = pl.ds(slot * rows_dev, rows_dev)
        return jnp.max(mx[:, at], 0, keepdims=True), jnp.sum(ch[:, at], 0, keepdims=True)

    def give(slot):
        best, chosen = reduced(slot)
        res[slot, 0:1, :] = best
        res[slot, 1:2, :] = chosen
        remote(res.at[slot], got.at[slot], result_sent, r_recv, device(slot)).start()

    x32 = docs[0].astype(jnp.float32)
    sq = x32 * x32
    total = sq[:, 0:128]
    for c in range(128, depth, 128):
        total = total + sq[:, c:c + 128]
    scale_x = lax.rsqrt(jnp.sum(total.T, 0, keepdims=True) + epsilon)

    landed(z - 3 * out, 0, end)
    landed(z - 3 * out, 1, end)
    have_docs(7, 0, 1, 2)
    flatten(7)
    begin(6, 2, 0, 1)

    def advance(k, have):
        c, w = cuts[have][k], cuts[have][k + 1] - cuts[have][k]
        turn(2, c, w)
        scales(c, w)
        for slot in (6, 2, 4, 0):
            stage(c, w, slot, 2)
            if k == 2:
                give(slot + 1)
                if slot:
                    give(slot)

    for k in range(3):
        last_landed(k)
        sized(core, None, functools.partial(advance, k))
    best, chosen = reduced(0)
    everyone = pl.ds(1, 7)
    remote(got.at[everyone], got.at[everyone], result_sent, r_recv, device(1)).wait_recv()
    for slot in range(1, 8):
        best = jnp.maximum(best, got[slot, 0:1, :])
        chosen = chosen + got[slot, 1:2, :]
    near_out[...] = best * scale_x
    chosen_out[...] = chosen * scale_x

    def sent(ref, sem):
        remote(ref, ref, sem, r_recv, device(1)).wait_send()

    sent(res.at[everyone], result_sent)
    sent(docs.at[everyone], doc_sent)
    sent(ids.at[everyone], id_sent)
    layer = 4 * feat
    sized(core, inner, lambda w: sent(buf.at[pl.ds(0, 3 * layer), pl.ds(0, w)], outward))
    sized(core, inner, lambda w: sent(buf.at[pl.ds(0, 2 * layer), pl.ds(0, w)], inward))
    sized(core, end, lambda w: sent(buf.at[pl.ds(0, layer), pl.ds(0, w)], inward))
    sized(core, None, lambda w: sent(own.at[:, pl.ds(0, 2 * per * 128 - w)], traded))


def by_layers(docs, centroids, assigned):
    nz = lax.axis_size("clu") // 4
    rows_dev, depth = docs.shape
    width, feat = centroids.shape
    tiles = -(-width // 128)
    wide = (tiles // 2 - tiles // 4) * 128
    any_space = pl.BlockSpec(memory_space=pl.ANY)
    vmem = pl.BlockSpec(memory_space=pltpu.VMEM)
    dma = pltpu.SemaphoreType.DMA
    line = pltpu.VMEM((1, rows_dev), jnp.float32)
    near, chosen = pl.pallas_call(
        functools.partial(layer_kernel, nz, feat),
        out_shape=(line, line),
        in_specs=[any_space] * 3,
        out_specs=(vmem, vmem),
        scratch_shapes=[
            pltpu.VMEM((feat, tiles * 128), jnp.bfloat16),
            pltpu.VMEM((feat, width % 128 or 128), jnp.bfloat16),
            pltpu.VMEM((depth, wide), jnp.bfloat16),
            pltpu.VMEM((8, rows_dev, depth), jnp.bfloat16),
            pltpu.VMEM((depth, 8 * rows_dev), jnp.bfloat16),
            pltpu.VMEM((8, 1, rows_dev), jnp.int32),
            pltpu.VMEM((3, wide, 256), jnp.bfloat16),
            pltpu.VMEM((wide, 8 * rows_dev), jnp.float32),
            pltpu.VMEM((GROUP, 8 * rows_dev), jnp.int32),
            pltpu.VMEM((GROUP, 8 * rows_dev), jnp.float32),
            pltpu.VMEM((GROUP, 8 * rows_dev), jnp.float32),
            pltpu.VMEM((8, wide), jnp.float32),
            pltpu.VMEM((wide, 128), jnp.float32),
            pltpu.VMEM((8, 2, rows_dev), jnp.float32),
            pltpu.VMEM((8, 2, rows_dev), jnp.float32),
            dma((4,)), dma((6,)), dma((nz, 4)), dma((3,)), dma((12,)), dma((4,)), dma,
        ],
        compiler_params=pltpu.CompilerParams(collective_id=0, has_side_effects=True),
        name="layer_distances",
    )(docs, centroids.T, assigned.reshape(1, rows_dev))
    return 1.0 - near.reshape(rows_dev), 1.0 - chosen.reshape(rows_dev)


def fits_layers(docs, centroids):
    tiles = -(-centroids.shape[0] // 128)
    n_clu, feat = lax.axis_size("clu"), centroids.shape[1]
    return (lax.axis_size("doc") == 2 and n_clu == 16 and tiles % 2 == 0 and tiles >= 20
            and feat % 16 == 0 and docs.shape[0] % 128 == 0 and docs.shape[1] % 256 == 0
            and docs.shape[1] == n_clu * feat == 3 * 256)


def on_device(docs, centroids, assigned):
    if fits_layers(docs, centroids):
        return by_layers(docs, centroids, assigned)
    n_clu, nd = lax.axis_size("clu"), lax.axis_size("doc")
    n = n_clu // 2
    rows_dev, depth = docs.shape
    width, feat = centroids.shape
    fp = (feat + 15) // 16 * 16
    cents = centroids.T
    if fp != feat:
        cents = jnp.pad(cents, ((0, fp - feat), (0, 0)))
    rows = nd * rows_dev
    any_space = pl.BlockSpec(memory_space=pl.ANY)
    vmem = pl.BlockSpec(memory_space=pltpu.VMEM)
    dma = pltpu.SemaphoreType.DMA
    hops = n // 2
    line = jax.ShapeDtypeStruct((1, rows_dev), jnp.float32)
    near, chosen = pl.pallas_call(
        functools.partial(kernel, n, nd, feat),
        out_shape=(line, line),
        in_specs=[any_space] * 3,
        out_specs=(vmem, vmem),
        scratch_shapes=[
            pltpu.VMEM((n_clu * fp, width), jnp.bfloat16),
            pltpu.VMEM((nd, rows_dev, depth), jnp.bfloat16),
            pltpu.VMEM((nd, 1, rows_dev), jnp.int32),
            pltpu.VMEM((rows, (n - 3) * 2 * fp), jnp.bfloat16),
            pltpu.VMEM((rows, 4 * fp), jnp.bfloat16),
            pltpu.VMEM((rows, 2 * fp), jnp.bfloat16),
            pltpu.VMEM((rows, width), jnp.float32),
            pltpu.VMEM((rows, 128), jnp.int32),
            pltpu.VMEM((rows, 128), jnp.float32),
            pltpu.VMEM((rows, 128), jnp.float32),
            pltpu.VMEM((8, width), jnp.float32),
            pltpu.VMEM((1, width), jnp.float32),
            pltpu.VMEM((nd, 2, rows_dev), jnp.float32),
            pltpu.VMEM((nd, 2, rows_dev), jnp.float32),
            dma((3,)),
            dma((2, hops, PIECES)),
            dma((n, PIECES)),
            dma((n, 2, PIECES)),
            dma((nd,)), dma((nd,)), dma((nd,)), dma((nd,)), dma((nd,)), dma((nd,)),
        ],
        compiler_params=pltpu.CompilerParams(collective_id=0, has_side_effects=True),
        name="ring_distances",
    )(docs, cents, assigned.reshape(1, rows_dev))
    return 1.0 - near.reshape(rows_dev), 1.0 - chosen.reshape(rows_dev)


def solution(mesh):
    placed = (P(("clu", "doc"), None), P("doc", "clu"), P(("clu", "doc")))
    return jax.shard_map(
        on_device,
        mesh=mesh,
        in_specs=placed,
        out_specs=(P(("clu", "doc")), P(("clu", "doc"))),
        check_vma=False,
    )
```

```python
import functools

import jax
import jax.numpy as jnp
from jax import lax
from jax.experimental import pallas as pl
from jax.experimental.pallas import tpu as pltpu
from jax.sharding import PartitionSpec as P

epsilon = 1e-06
PIECES = 4
ROWS = 64
GROUP = 16
MESH = pl.DeviceIdType.MESH


def chip_at(pos, n):
    half = n // 2
    return jnp.where(pos < half, 2 * pos, 2 * (n - 1 - pos) + 1)


def cut(width):
    tiles = (width + 127) // 128
    ends = [min(-(-tiles * (c + 1) // PIECES) * 128, width) for c in range(PIECES)]
    return tuple((a, b - a) for a, b in zip([0] + ends[:-1], ends))


def kernel(n, nd, feat, docs_in, cents_in, ids_in, near_out, chosen_out,
           buf, docs_all, ids_all, dp_a, dp_b, dp_c, acc, idb, mx, ch, csq, scale, res, got,
           local_sem, ring_send, pair_send, recv, docs_send, docs_recv, ids_send, ids_recv,
           res_send, res_recv):
    hops = n // 2
    fp = cents_in.shape[0]
    width = cents_in.shape[1]
    rows_dev = docs_in.shape[0]
    chunks = cut(width)
    half = len(chunks) // 2

    clu, doc = lax.axis_index("clu"), lax.axis_index("doc")
    core, chip = lax.rem(clu, 2), lax.div(clu, 2)
    z, x = lax.div(chip, 2), lax.rem(chip, 2)
    pos = jnp.where(x == 0, z, n - 1 - z)
    right = chip_at(lax.rem(pos + 1, n), n) * 2 + core
    left = chip_at(lax.rem(pos + n - 1, n), n) * 2 + core
    partner = chip * 2 + (1 - core)

    own_c = pltpu.make_async_copy(cents_in, buf.at[pl.ds(0, fp), :], local_sem.at[0])
    own_d = pltpu.make_async_copy(docs_in, docs_all.at[0], local_sem.at[1])
    own_i = pltpu.make_async_copy(ids_in, ids_all.at[0], local_sem.at[2])
    own_c.start()
    own_d.start()
    own_i.start()

    barrier = pltpu.get_barrier_semaphore()
    for peer in (left, right, partner):
        pl.semaphore_signal(barrier, inc=1, device_id={"clu": peer}, device_id_type=MESH)
    for k in range(1, nd):
        pl.semaphore_signal(barrier, inc=1, device_id={"doc": lax.rem(doc + k, nd)}, device_id_type=MESH)
    pl.semaphore_wait(barrier, 3 + nd - 1)

    def slot(way, h):
        if h == 0:
            return 0
        if h == hops:
            return n - 1
        return 2 * h - 1 if way == 0 else 2 * h

    def piece(s, m, c):
        return buf.at[pl.ds((2 * s + m) * fp, fp), pl.ds(*chunks[c])]

    def reach(way, c):
        return hops if way == c // half else hops - 1

    sent = []

    def ring(way, h, c):
        s, t = slot(way, h), slot(way, h + 1)
        copy = pltpu.make_async_remote_copy(
            src_ref=piece(s, 0, c), dst_ref=piece(t, 0, c),
            send_sem=ring_send.at[way, h, c], recv_sem=recv.at[t, 0, c],
            device_id={"clu": right if way == 0 else left}, device_id_type=MESH)
        copy.start()
        sent.append(copy)

    def share(s, c):
        copy = pltpu.make_async_remote_copy(
            src_ref=piece(s, 0, c), dst_ref=piece(s, 1, c),
            send_sem=pair_send.at[s, c], recv_sem=recv.at[s, 1, c],
            device_id={"clu": partner}, device_id_type=MESH)
        copy.start()
        sent.append(copy)

    def landed(s, m, c):
        pltpu.make_async_remote_copy(
            src_ref=piece(s, m, c), dst_ref=piece(s, m, c),
            send_sem=pair_send.at[s, c], recv_sem=recv.at[s, m, c],
            device_id={"clu": partner}, device_id_type=MESH).wait_recv()

    own_c.wait()
    for i in range(PIECES):
        ring(0, 0, i)
        ring(1, 0, (i + half) % PIECES)
    for c in range(PIECES):
        share(0, c)
    own_d.wait()
    own_i.wait()
    doc_copies = []
    for k in range(1, nd):
        mate = lax.rem(doc + k, nd)
        for ref, ss, rs in ((ids_all, ids_send, ids_recv), (docs_all, docs_send, docs_recv)):
            copy = pltpu.make_async_remote_copy(
                src_ref=ref.at[0], dst_ref=ref.at[k], send_sem=ss.at[k], recv_sem=rs.at[k],
                device_id={"doc": mate}, device_id_type=MESH)
            copy.start()
            doc_copies.append(copy)

    def owner(s):
        if s == 0:
            p = pos
        elif s == n - 1:
            p = pos + hops
        elif s % 2:
            p = pos + n - (s + 1) // 2
        else:
            p = pos + s // 2
        return chip_at(lax.rem(p, n), n)

    ranges = ((0, n - 3), (n - 3, n - 1), (n - 1, n))
    spread = (dp_a, dp_b, dp_c)

    def permute(k):
        rows = docs_all[k]
        for (first, last), out in zip(ranges, spread):
            wide = out.shape[1]
            lane = lax.broadcasted_iota(jnp.int32, (1, wide), 1)
            target = jnp.full((1, wide), -1, jnp.int32)
            for s in range(first, last):
                chip_s = owner(s)
                for m in (0, 1):
                    part = chip_s * 2 + (core if m == 0 else 1 - core)
                    start = (2 * (s - first) + m) * fp
                    inside = (lane >= start) & (lane < start + feat)
                    target = jnp.where(inside, lane - start + part * feat, target)
            source = lax.broadcasted_iota(jnp.int32, (rows.shape[1], wide), 0)
            mover = jnp.where(source == target, 1.0, 0.0).astype(jnp.bfloat16)
            out[pl.ds(k * rows_dev, rows_dev), :] = jnp.dot(
                rows, mover, preferred_element_type=jnp.float32).astype(jnp.bfloat16)

    def prepare_ids(k):
        base = doc * width
        ids = ids_all[k] - base
        ids = jnp.where((ids >= 0) & (ids < width), ids, -1)
        full = jnp.broadcast_to(ids, (128, rows_dev)).T
        lanes = lax.broadcasted_iota(jnp.int32, (rows_dev, 128), 1)
        idb[pl.ds(k * rows_dev, rows_dev), :] = jnp.where(full >= 0, full - lanes, -(2**20))

    def phase(index, c):
        first, last = ranges[index]
        start, depth = 2 * first * fp, 2 * (last - first) * fp
        cols = pl.ds(*chunks[c])
        block = buf[pl.ds(start, depth), cols]
        prod = jnp.dot(spread[index][...], block, preferred_element_type=jnp.float32)
        w32 = block.astype(jnp.float32)
        sq = jnp.sum((w32 * w32).reshape(depth // 8, 8, chunks[c][1]), 0)
        if index == 0:
            acc[:, cols] = prod
            csq[:, cols] = sq
        else:
            acc[:, cols] += prod
            csq[:, cols] += sq

    tail = pl.ds(2 * (n - 1) * fp, 2 * fp)

    def finish_scale(c):
        cols = pl.ds(*chunks[c])
        w32 = buf[tail, cols].astype(jnp.float32)
        sq = jnp.sum((w32 * w32).reshape(2 * fp // 8, 8, chunks[c][1]), 0) + csq[:, cols]
        scale[:, cols] = lax.rsqrt(jnp.sum(sq, 0, keepdims=True) + epsilon)

    def final(k, c):
        start, wide = chunks[c]
        prod = jnp.dot(dp_c[pl.ds(k * rows_dev, rows_dev), :], buf[tail, pl.ds(start, wide)],
                       preferred_element_type=jnp.float32)
        for r in range(0, rows_dev, ROWS):
            rs = pl.ds(k * rows_dev + r, ROWS)
            top, hit = mx[rs, :], ch[rs, :]
            ids = idb[rs, :]
            for a in range(0, wide, 128):
                w = min(128, wide - a)
                cols = pl.ds(start + a, w)
                v = (acc[rs, cols] + prod[r:r + ROWS, a:a + w]) * scale[:, cols]
                if w == 128:
                    top = jnp.maximum(top, v)
                    hit = jnp.where(ids == start + a, v, hit)
                else:
                    mx[rs, :] = top
                    ch[rs, :] = hit
                    mx[rs, pl.ds(0, w)] = jnp.maximum(mx[rs, pl.ds(0, w)], v)
                    ch[rs, pl.ds(0, w)] = jnp.where(idb[rs, pl.ds(0, w)] == start + a, v, ch[rs, pl.ds(0, w)])
            if wide % 128 == 0:
                mx[rs, :] = top
                ch[rs, :] = hit

    def reduced(k):
        rs = pl.ds(k * rows_dev, rows_dev)
        return (jnp.max(mx[rs, :].T, 0, keepdims=True), jnp.sum(ch[rs, :].T, 0, keepdims=True))

    mx[...] = jnp.full(mx.shape, -3.0e38, jnp.float32)
    ch[...] = jnp.zeros(ch.shape, jnp.float32)
    permute(0)
    prepare_ids(0)
    wide = docs_all[0].astype(jnp.float32)
    squares = wide * wide
    total = squares[:, 0:128]
    for a in range(128, wide.shape[1], 128):
        total = total + squares[:, a:a + 128]
    scale_x = lax.rsqrt(jnp.sum(total.T, 0, keepdims=True) + epsilon)

    def step(way, h, c):
        s = slot(way, h)
        landed(s, 0, c)
        if h < reach(way, c):
            ring(way, h, c)
        share(s, c)

    def pair(h, i):
        step(0, h, i)
        step(1, h, (i + half) % PIECES)

    def partners(slots, c):
        for s in slots:
            landed(s, 1, c)

    early, late = range(n - 3), (n - 3, n - 2)
    order = [j // 2 + half * (j % 2) for j in range(PIECES)]
    for h in range(1, hops):
        for i in range(PIECES):
            pair(h, i)
            if h == hops - 2 and i == half:
                for copy in doc_copies:
                    copy.wait()
                for k in range(1, nd):
                    permute(k)
                    prepare_ids(k)
            if h == hops - 1:
                c = order[i]
                partners(early, c)
                phase(0, c)
    for c in order[:half]:
        partners(late, c)
        phase(1, c)
    for i in range(half):
        for way in (0, 1):
            c = i + half * way
            landed(n - 1, 0, c)
            share(n - 1, c)
    for c in order[half:]:
        partners(late, c)
        phase(1, c)
    for c in order[:-2]:
        landed(n - 1, 1, c)
        finish_scale(c)
        for k in range(nd):
            final(k, c)
    for c in order[-2:]:
        landed(n - 1, 1, c)
        finish_scale(c)

    returns = []
    for k in range(1, nd):
        for c in order[-2:]:
            final(k, c)
        best, chosen = reduced(k)
        res[k, 0:1, :] = best
        res[k, 1:2, :] = chosen
        copy = pltpu.make_async_remote_copy(
            src_ref=res.at[k], dst_ref=got.at[k], send_sem=res_send.at[k], recv_sem=res_recv.at[k],
            device_id={"doc": lax.rem(doc + nd - k, nd)}, device_id_type=MESH)
        copy.start()
        returns.append(copy)
    for c in order[-2:]:
        final(0, c)
    best, chosen = reduced(0)
    for k in range(1, nd):
        returns[k - 1].wait()
        best = jnp.maximum(best, got[k, 0:1, :])
        chosen = chosen + got[k, 1:2, :]
    near_out[...] = best * scale_x
    chosen_out[...] = chosen * scale_x
    for copy in sent:
        copy.wait_send()


def layer_kernel(nz, feat, docs_in, cents_in, ids_in, near_out, chosen_out,
                 own, raw, buf, docs, flat, ids, turned, acc, idb, mx, ch, csq, scale, res, got,
                 local_sem, send_sem, c_recv, last_recv, d_recv, i_recv, r_recv):
    width = cents_in.shape[1]
    rows_dev, depth = docs_in.shape
    tiles = own.shape[1] // 128
    per = tiles // 2
    small = per // 2
    big = per - small
    wide = big * 128
    full = width // 128 * 128
    late = -(-4 * feat // 256) * 256
    k1 = 8 * feat // 256 * 256
    k2 = depth - late - k1
    a = rows_dev * 5 // 16 // 16 * 16
    b = (rows_dev - a) // 32 * 16
    spans = ((0, a), (a, b), (a + b, rows_dev - a - b))
    cuts = {w: (0, 256, (w - 1) // 256 * 256, w) for w in (small * 128, wide)}

    clu, doc = lax.axis_index("clu"), lax.axis_index("doc")
    core, chip = lax.rem(clu, 2), lax.div(clu, 2)
    z, x = lax.div(chip, 2), lax.rem(chip, 2)
    upper = z >= nz // 2
    out = jnp.where(upper, 1, -1)
    end = (z == 0) | (z == nz - 1)
    inner = jnp.logical_not(end)

    def device(r, dz=0):
        dx, dy, dc = r // 4, r // 2 % 2, r % 2
        there = ((z + dz) * 2 + (1 - x if dx else x)) * 2 + (1 - core if dc else core)
        return {"clu": there, "doc": 1 - doc if dy else doc}

    def when(cond, body):
        if cond is None:
            body()
        else:
            pl.when(cond)(body)

    def both(p, q):
        return q if p is None else p if q is None else p & q

    sizes = ((None, big),) if big == small else ((1, big), (0, small))

    def sized(c, cond, body):
        for value, count in sizes:
            when(both(cond, None if value is None else c == value), functools.partial(body, count * 128))

    own_copy = pltpu.make_async_copy(cents_in.at[:, pl.ds(0, full)], own.at[:, pl.ds(0, full)], local_sem.at[0])
    docs_copy = pltpu.make_async_copy(docs_in, docs.at[0], local_sem.at[1])
    ids_copy = pltpu.make_async_copy(ids_in, ids.at[0], local_sem.at[2])
    own_copy.start()
    if full < width:
        raw_copy = pltpu.make_async_copy(cents_in.at[:, pl.ds(full, width - full)], raw, local_sem.at[3])
        raw_copy.start()
    docs_copy.start()
    ids_copy.start()

    barrier = pltpu.get_barrier_semaphore()

    def greet(to):
        pl.semaphore_signal(barrier, inc=1, device_id=to, device_id_type=MESH)

    pl.when(inner)(lambda: greet(device(0, out)))
    greet(device(0, -out))
    for r in (4, 5, 2, 1):
        greet(device(r))
    if small < big:
        @pl.when(core == 0)
        def _():
            buf[:, pl.ds(small * 128, 128)] = jnp.zeros((buf.shape[0], 128), buf.dtype)
    if full < width:
        raw_copy.wait()
        own[:, pl.ds(full, 128)] = jnp.concatenate(
            [raw[...], jnp.zeros((feat, full + 128 - width), raw.dtype)], axis=1)
    own_copy.wait()
    docs_copy.wait()
    ids_copy.wait()
    pl.semaphore_wait(barrier, 5 + inner.astype(jnp.int32))

    outward, inward, traded, doc_sent, id_sent, result_sent = (send_sem.at[i] for i in range(6))

    def start(make, cond=None):
        when(cond, lambda: make().start())

    def start_sized(make, c, cond=None):
        sized(c, cond, lambda w: make(w).start())

    def remote(src, dst, ss, rs, to):
        return pltpu.make_async_remote_copy(
            src_ref=src, dst_ref=dst, send_sem=ss, recv_sem=rs, device_id=to, device_id_type=MESH)

    near = (0, 1, 4, 5)

    def source(layer, j):
        r = near[j]
        there = (layer * 2 + (1 - x if r // 4 else x)) * 2 + (1 - core if r % 2 else core)
        return pl.ds(pl.multiple_of(there * feat, 16), feat)

    def columns(r, w):
        xd = 1 - x if r // 4 else x
        cd = 1 - core if r % 2 else core
        return pl.ds(pl.multiple_of((xd * per + cd * small) * 128, 128), w)

    mine = source(z, 0)

    def exchange(j):
        r = near[j]
        start_sized(lambda w: remote(own.at[:, columns(r, w)], buf.at[mine, pl.ds(0, w)],
                                     traded, c_recv.at[z, j], device(r)),
                    1 - core if r % 2 else core)

    def landed(layer, j, cond=None):
        rows = source(layer, j)
        sized(core, cond, lambda w: remote(
            buf.at[rows, pl.ds(0, w)], buf.at[rows, pl.ds(0, w)], traded, c_recv.at[layer, j],
            device(1)).wait_recv())

    def carry(layer, j, way, s, cond=None):
        rows = source(layer, j)
        src = (lambda w: own.at[:, columns(0, w)]) if s == 0 and j == 0 else (lambda w: buf.at[rows, pl.ds(0, w)])
        start_sized(lambda w: remote(src(w), buf.at[rows, pl.ds(0, w)], inward if way else outward,
                                     c_recv.at[layer, j], device(0, -out if way else out)), core, cond)

    def spread(j):
        if j:
            landed(z, j)
        carry(z, j, 0, 0, inner)
        carry(z, j, 1, 0)

    def relay(j):
        landed(z - out, j)
        carry(z - out, j, 0, 1, inner)
        landed(z + out, j, inner)
        carry(z + out, j, 1, 1, inner)

    def pair(layer, k, w):
        rows = pl.ds(pl.multiple_of((layer * 2 + 1 - x) * 2 * feat, 16), 2 * feat)
        return buf.at[rows, pl.ds(cuts[w][k], cuts[w][k + 1] - cuts[w][k])]

    def relay_far(j):
        landed(z - 2 * out, j)
        if j < 2:
            carry(z - 2 * out, j, 0, 2, inner)

    def send_last(cond):
        for k in range(3):
            start_sized(lambda w, k=k: remote(
                pair(z - 2 * out, k, w), pair(z - 2 * out, k, w), outward, last_recv.at[k],
                device(0, out)), core, inner & cond)

    def last_landed(k):
        sized(core, end, lambda w: remote(
            pair(z - 3 * out, k, w), pair(z - 3 * out, k, w), outward, last_recv.at[k],
            device(1)).wait_recv())

    ahead = {(1, 0): 0, (1, 1): 0, (1, 2): 0, (3, 0): 1, (3, 1): 1, (3, 2): 1, (5, 0): 2, (5, 1): 2, (5, 2): 2,
             (7, 0): 3, (7, 1): 3, (7, 2): 3, (2, 0): 4, (2, 1): 5, (2, 2): 5, (4, 0): 6, (4, 1): 7, (4, 2): 8,
             (6, 0): 9, (6, 1): 10, (6, 2): 11}
    id_at = {1: 0, 3: 0, 5: 0, 7: 0, 2: 1, 4: 2, 6: 3}

    def part(slot, *parts):
        first, last = spans[parts[0]], spans[parts[-1]]
        return docs.at[slot, pl.ds(first[0], last[0] + last[1] - first[0]), :]

    def send_docs(src_slot, dst_slot, r, *parts):
        start(lambda: remote(part(src_slot, *parts), part(dst_slot, *parts), doc_sent,
                             d_recv.at[ahead[dst_slot, parts[0]]], device(r)))

    def send_ids(src_slot, dst_slot, r):
        start(lambda: remote(ids.at[src_slot], ids.at[dst_slot], id_sent, i_recv.at[id_at[dst_slot]], device(r)))

    def have_docs(slot, *parts):
        remote(part(slot, *parts), part(slot, *parts), doc_sent, d_recv.at[ahead[slot, parts[0]]],
               device(1)).wait_recv()

    def have_ids(slot):
        some = ids.at[pl.ds(0, 4)] if slot % 2 else ids.at[slot]
        remote(some, some, id_sent, i_recv.at[id_at[slot]], device(1)).wait_recv()

    def share(slot, *parts):
        send_docs(slot, slot + 1, 1, *parts)

    spread(0)
    for j in (1, 2, 3):
        exchange(j)
    send_ids(0, 2, 2)
    send_docs(0, 2, 2, 0)
    send_docs(0, 2, 2, 1, 2)
    send_ids(0, 4, 4)
    for p in (1, 2, 0):
        send_docs(0, 4, 4, p)
    send_ids(0, 1, 1)
    send_docs(0, 1, 1, 0, 1, 2)

    part_cols = jnp.where(core == 1, big, small) * 128
    first = (x * per + core * small) * 128
    base = doc * width + first
    reach = jnp.minimum(part_cols, width - first)
    down = lax.broadcasted_iota(jnp.int32, (GROUP, 128), 0)

    def prepare_ids(slot):
        rel = ids[slot] - base
        rel = jnp.where((rel >= 0) & (rel < reach), rel, -(2**20))
        tall = jnp.broadcast_to(rel, (GROUP, rows_dev))
        idb[:, pl.ds(slot * rows_dev, rows_dev)] = tall - lax.broadcasted_iota(jnp.int32, (GROUP, rows_dev), 0)

    buf[mine, pl.ds(0, small * 128)] = own[:, columns(0, small * 128)]
    if small < big:
        @pl.when(core == 1)
        def _():
            start_col = pl.multiple_of((x * per + 2 * small) * 128, 128)
            buf[mine, pl.ds(small * 128, 128)] = own[:, pl.ds(start_col, 128)]

    k1_at = pl.multiple_of(jnp.where(upper, depth - k1, 0), 256)
    k2_at = pl.multiple_of(jnp.where(upper, late, k1), 256)
    late_at = pl.multiple_of(jnp.where(upper, 0, depth - late), 256)
    starts = (k1_at, k2_at, late_at)

    def squares(i, c, w):
        w32 = buf[pl.ds(starts[i], 256), pl.ds(c, w)].astype(jnp.float32)
        return jnp.sum((w32 * w32).reshape(32, 8, w), 0)

    def turn(i, c, w):
        turned[i, pl.ds(c, w), :] = buf[pl.ds(starts[i], 256), pl.ds(c, w)].T

    def gather(i):
        for c in range(0, wide, 256):
            turn(i, c, min(256, wide - c))
        csq[...] = squares(i, 0, wide) + (csq[...] if i else 0.0)

    def flatten(*slots):
        for slot in slots:
            flat[:, pl.ds(slot * rows_dev, rows_dev)] = docs[slot].T

    def times(i, c, w, slot, count):
        return jnp.dot(turned[i, pl.ds(c, w), :],
                       flat[pl.ds(starts[i], 256), pl.ds(slot * rows_dev, count * rows_dev)],
                       preferred_element_type=jnp.float32)

    def begin(slot, count, *phases):
        where_docs = pl.ds(slot * rows_dev, count * rows_dev)

        def add(w):
            prod = times(phases[0], 0, w, slot, count)
            for i in phases[1:]:
                prod = prod + times(i, 0, w, slot, count)
            if phases[0]:
                acc[pl.ds(0, w), where_docs] += prod
            else:
                acc[pl.ds(0, w), where_docs] = prod

        sized(core, None, add)

    spread(1)
    prepare_ids(0)
    flatten(0)
    spread(2)
    relay(0)
    spread(3)
    relay(1)
    have_docs(2, 0)
    send_docs(2, 6, 4, 0)
    have_ids(4)
    send_ids(4, 6, 2)
    send_ids(4, 5, 1)
    have_ids(2)
    send_ids(2, 3, 1)
    relay(2)
    have_docs(4, 1)
    send_docs(4, 6, 2, 1)
    have_docs(1, 0, 1, 2)
    flatten(1)
    relay(3)
    relay_far(0)
    have_docs(2, 1, 2)
    share(2, 0, 1, 2)
    have_docs(4, 2)
    send_docs(4, 6, 2, 2)
    have_ids(6)
    send_ids(6, 7, 1)
    relay_far(1)
    gather(0)
    begin(0, 2, 0)
    flatten(2)
    have_ids(1)
    for slot in (1, 2, 3, 4, 5, 6, 7):
        prepare_ids(slot)
    relay_far(2)
    have_docs(4, 0)
    share(4, 0, 1, 2)
    relay_far(3)
    send_last(core == 0)
    have_docs(3, 0, 1, 2)
    flatten(3)
    begin(2, 2, 0)
    gather(1)
    send_last(core == 1)
    flatten(4)
    begin(0, 2, 1)
    begin(2, 2, 1)

    def share_far():
        for p in (1, 2, 0):
            have_docs(6, p)
        share(6, 0, 1, 2)

    pl.when(core == 1)(share_far)
    have_docs(5, 0, 1, 2)
    flatten(5)
    pl.when(core == 0)(share_far)
    begin(4, 2, 0, 1)
    flatten(6)

    def scales(c, w):
        total = jnp.sum(csq[:, pl.ds(c, w)] + squares(2, c, w), 0, keepdims=True)
        scale[pl.ds(c, w), :] = jnp.broadcast_to(lax.rsqrt(total + epsilon), (128, w)).T

    def stage(c0, w, slot, count):
        prod = times(2, c0, w, slot, count)
        spots = [pl.ds(slot * rows_dev + d, 128) for d in range(0, count * rows_dev, 128)]
        if c0:
            tops, hits = [mx[:, at] for at in spots], [ch[:, at] for at in spots]
        else:
            tops = [jnp.full((GROUP, 128), -3.0e38, jnp.float32)] * len(spots)
            hits = [jnp.zeros((GROUP, 128), jnp.float32)] * len(spots)
        for c in range(0, w, GROUP):
            rows = pl.ds(c0 + c, GROUP)
            by = scale[rows, :]
            for n, at in enumerate(spots):
                v = (acc[rows, at] + prod[c:c + GROUP, n * 128:n * 128 + 128]) * by
                hits[n] = jnp.where(idb[:, at] == c0 + c, v, hits[n])
                if c0 + c + 128 > small * 128:
                    v = jnp.where(down < reach - (c0 + c), v, -3.0e38)
                tops[n] = jnp.maximum(tops[n], v)
        for n, at in enumerate(spots):
            mx[:, at], ch[:, at] = tops[n], hits[n]

    def reduced(slot):
        at = pl.ds(slot * rows_dev, rows_dev)
        return jnp.max(mx[:, at], 0, keepdims=True), jnp.sum(ch[:, at], 0, keepdims=True)

    def give(slot):
        best, chosen = reduced(slot)
        res[slot, 0:1, :] = best
        res[slot, 1:2, :] = chosen
        remote(res.at[slot], got.at[slot], result_sent, r_recv, device(slot)).start()

    x32 = docs[0].astype(jnp.float32)
    sq = x32 * x32
    total = sq[:, 0:128]
    for c in range(128, depth, 128):
        total = total + sq[:, c:c + 128]
    scale_x = lax.rsqrt(jnp.sum(total.T, 0, keepdims=True) + epsilon)

    landed(z - 3 * out, 0, end)
    landed(z - 3 * out, 1, end)
    have_docs(7, 0, 1, 2)
    flatten(7)
    begin(6, 2, 0, 1)

    def advance(k, have):
        c, w = cuts[have][k], cuts[have][k + 1] - cuts[have][k]
        turn(2, c, w)
        scales(c, w)
        for slot in (6, 2, 4, 0):
            stage(c, w, slot, 2)
            if k == 2:
                give(slot + 1)
                if slot:
                    give(slot)

    for k in range(3):
        last_landed(k)
        sized(core, None, functools.partial(advance, k))
    best, chosen = reduced(0)
    everyone = pl.ds(1, 7)
    remote(got.at[everyone], got.at[everyone], result_sent, r_recv, device(1)).wait_recv()
    for slot in range(1, 8):
        best = jnp.maximum(best, got[slot, 0:1, :])
        chosen = chosen + got[slot, 1:2, :]
    near_out[...] = best * scale_x
    chosen_out[...] = chosen * scale_x

    def sent(ref, sem):
        remote(ref, ref, sem, r_recv, device(1)).wait_send()

    sent(res.at[everyone], result_sent)
    sent(docs.at[everyone], doc_sent)
    sent(ids.at[everyone], id_sent)
    layer = 4 * feat
    sized(core, inner, lambda w: sent(buf.at[pl.ds(0, 3 * layer), pl.ds(0, w)], outward))
    sized(core, inner, lambda w: sent(buf.at[pl.ds(0, 2 * layer), pl.ds(0, w)], inward))
    sized(core, end, lambda w: sent(buf.at[pl.ds(0, layer), pl.ds(0, w)], inward))
    sized(core, None, lambda w: sent(own.at[:, pl.ds(0, 2 * per * 128 - w)], traded))


def by_layers(docs, centroids, assigned):
    nz = lax.axis_size("clu") // 4
    rows_dev, depth = docs.shape
    width, feat = centroids.shape
    tiles = -(-width // 128)
    wide = (tiles // 2 - tiles // 4) * 128
    any_space = pl.BlockSpec(memory_space=pl.ANY)
    vmem = pl.BlockSpec(memory_space=pltpu.VMEM)
    dma = pltpu.SemaphoreType.DMA
    line = pltpu.VMEM((1, rows_dev), jnp.float32)
    near, chosen = pl.pallas_call(
        functools.partial(layer_kernel, nz, feat),
        out_shape=(line, line),
        in_specs=[any_space] * 3,
        out_specs=(vmem, vmem),
        scratch_shapes=[
            pltpu.VMEM((feat, tiles * 128), jnp.bfloat16),
            pltpu.VMEM((feat, width % 128 or 128), jnp.bfloat16),
            pltpu.VMEM((depth, wide), jnp.bfloat16),
            pltpu.VMEM((8, rows_dev, depth), jnp.bfloat16),
            pltpu.VMEM((depth, 8 * rows_dev), jnp.bfloat16),
            pltpu.VMEM((8, 1, rows_dev), jnp.int32),
            pltpu.VMEM((3, wide, 256), jnp.bfloat16),
            pltpu.VMEM((wide, 8 * rows_dev), jnp.float32),
            pltpu.VMEM((GROUP, 8 * rows_dev), jnp.int32),
            pltpu.VMEM((GROUP, 8 * rows_dev), jnp.float32),
            pltpu.VMEM((GROUP, 8 * rows_dev), jnp.float32),
            pltpu.VMEM((8, wide), jnp.float32),
            pltpu.VMEM((wide, 128), jnp.float32),
            pltpu.VMEM((8, 2, rows_dev), jnp.float32),
            pltpu.VMEM((8, 2, rows_dev), jnp.float32),
            dma((4,)), dma((6,)), dma((nz, 4)), dma((3,)), dma((12,)), dma((4,)), dma,
        ],
        compiler_params=pltpu.CompilerParams(collective_id=0, has_side_effects=True),
        name="layer_distances",
    )(docs, centroids.T, assigned.reshape(1, rows_dev))
    return 1.0 - near.reshape(rows_dev), 1.0 - chosen.reshape(rows_dev)


def fits_layers(docs, centroids):
    tiles = -(-centroids.shape[0] // 128)
    n_clu, feat = lax.axis_size("clu"), centroids.shape[1]
    return (lax.axis_size("doc") == 2 and n_clu == 16 and tiles % 2 == 0 and tiles >= 20
            and feat % 16 == 0 and docs.shape[0] % 128 == 0 and docs.shape[1] % 256 == 0
            and docs.shape[1] == n_clu * feat == 3 * 256)


def on_device(docs, centroids, assigned):
    if fits_layers(docs, centroids):
        return by_layers(docs, centroids, assigned)
    n_clu, nd = lax.axis_size("clu"), lax.axis_size("doc")
    n = n_clu // 2
    rows_dev, depth = docs.shape
    width, feat = centroids.shape
    fp = (feat + 15) // 16 * 16
    cents = centroids.T
    if fp != feat:
        cents = jnp.pad(cents, ((0, fp - feat), (0, 0)))
    rows = nd * rows_dev
    any_space = pl.BlockSpec(memory_space=pl.ANY)
    vmem = pl.BlockSpec(memory_space=pltpu.VMEM)
    dma = pltpu.SemaphoreType.DMA
    hops = n // 2
    line = jax.ShapeDtypeStruct((1, rows_dev), jnp.float32)
    near, chosen = pl.pallas_call(
        functools.partial(kernel, n, nd, feat),
        out_shape=(line, line),
        in_specs=[any_space] * 3,
        out_specs=(vmem, vmem),
        scratch_shapes=[
            pltpu.VMEM((n_clu * fp, width), jnp.bfloat16),
            pltpu.VMEM((nd, rows_dev, depth), jnp.bfloat16),
            pltpu.VMEM((nd, 1, rows_dev), jnp.int32),
            pltpu.VMEM((rows, (n - 3) * 2 * fp), jnp.bfloat16),
            pltpu.VMEM((rows, 4 * fp), jnp.bfloat16),
            pltpu.VMEM((rows, 2 * fp), jnp.bfloat16),
            pltpu.VMEM((rows, width), jnp.float32),
            pltpu.VMEM((rows, 128), jnp.int32),
            pltpu.VMEM((rows, 128), jnp.float32),
            pltpu.VMEM((rows, 128), jnp.float32),
            pltpu.VMEM((8, width), jnp.float32),
            pltpu.VMEM((1, width), jnp.float32),
            pltpu.VMEM((nd, 2, rows_dev), jnp.float32),
            pltpu.VMEM((nd, 2, rows_dev), jnp.float32),
            dma((3,)),
            dma((2, hops, PIECES)),
            dma((n, PIECES)),
            dma((n, 2, PIECES)),
            dma((nd,)), dma((nd,)), dma((nd,)), dma((nd,)), dma((nd,)), dma((nd,)),
        ],
        compiler_params=pltpu.CompilerParams(collective_id=0, has_side_effects=True),
        name="ring_distances",
    )(docs, cents, assigned.reshape(1, rows_dev))
    return 1.0 - near.reshape(rows_dev), 1.0 - chosen.reshape(rows_dev)


def solution(mesh):
    placed = (P(("clu", "doc"), None), P("doc", "clu"), P(("clu", "doc")))
    return jax.shard_map(
        on_device,
        mesh=mesh,
        in_specs=placed,
        out_specs=(P(("clu", "doc")), P(("clu", "doc"))),
        check_vma=False,
    )
```

```python
import functools

import jax
import jax.numpy as jnp
from jax import lax
from jax.experimental import pallas as pl
from jax.experimental.pallas import tpu as pltpu
from jax.sharding import PartitionSpec as P

epsilon = 1e-06
PIECES = 4
ROWS = 64
GROUP = 16
MESH = pl.DeviceIdType.MESH


def chip_at(pos, n):
    half = n // 2
    return jnp.where(pos < half, 2 * pos, 2 * (n - 1 - pos) + 1)


def cut(width):
    tiles = (width + 127) // 128
    ends = [min(-(-tiles * (c + 1) // PIECES) * 128, width) for c in range(PIECES)]
    return tuple((a, b - a) for a, b in zip([0] + ends[:-1], ends))


def kernel(n, nd, feat, docs_in, cents_in, ids_in, near_out, chosen_out,
           buf, docs_all, ids_all, dp_a, dp_b, dp_c, acc, idb, mx, ch, csq, scale, res, got,
           local_sem, ring_send, pair_send, recv, docs_send, docs_recv, ids_send, ids_recv,
           res_send, res_recv):
    hops = n // 2
    fp = cents_in.shape[0]
    width = cents_in.shape[1]
    rows_dev = docs_in.shape[0]
    chunks = cut(width)
    half = len(chunks) // 2

    clu, doc = lax.axis_index("clu"), lax.axis_index("doc")
    core, chip = lax.rem(clu, 2), lax.div(clu, 2)
    z, x = lax.div(chip, 2), lax.rem(chip, 2)
    pos = jnp.where(x == 0, z, n - 1 - z)
    right = chip_at(lax.rem(pos + 1, n), n) * 2 + core
    left = chip_at(lax.rem(pos + n - 1, n), n) * 2 + core
    partner = chip * 2 + (1 - core)

    own_c = pltpu.make_async_copy(cents_in, buf.at[pl.ds(0, fp), :], local_sem.at[0])
    own_d = pltpu.make_async_copy(docs_in, docs_all.at[0], local_sem.at[1])
    own_i = pltpu.make_async_copy(ids_in, ids_all.at[0], local_sem.at[2])
    own_c.start()
    own_d.start()
    own_i.start()

    barrier = pltpu.get_barrier_semaphore()
    for peer in (left, right, partner):
        pl.semaphore_signal(barrier, inc=1, device_id={"clu": peer}, device_id_type=MESH)
    for k in range(1, nd):
        pl.semaphore_signal(barrier, inc=1, device_id={"doc": lax.rem(doc + k, nd)}, device_id_type=MESH)
    pl.semaphore_wait(barrier, 3 + nd - 1)

    def slot(way, h):
        if h == 0:
            return 0
        if h == hops:
            return n - 1
        return 2 * h - 1 if way == 0 else 2 * h

    def piece(s, m, c):
        return buf.at[pl.ds((2 * s + m) * fp, fp), pl.ds(*chunks[c])]

    def reach(way, c):
        return hops if way == c // half else hops - 1

    sent = []

    def ring(way, h, c):
        s, t = slot(way, h), slot(way, h + 1)
        copy = pltpu.make_async_remote_copy(
            src_ref=piece(s, 0, c), dst_ref=piece(t, 0, c),
            send_sem=ring_send.at[way, h, c], recv_sem=recv.at[t, 0, c],
            device_id={"clu": right if way == 0 else left}, device_id_type=MESH)
        copy.start()
        sent.append(copy)

    def share(s, c):
        copy = pltpu.make_async_remote_copy(
            src_ref=piece(s, 0, c), dst_ref=piece(s, 1, c),
            send_sem=pair_send.at[s, c], recv_sem=recv.at[s, 1, c],
            device_id={"clu": partner}, device_id_type=MESH)
        copy.start()
        sent.append(copy)

    def landed(s, m, c):
        pltpu.make_async_remote_copy(
            src_ref=piece(s, m, c), dst_ref=piece(s, m, c),
            send_sem=pair_send.at[s, c], recv_sem=recv.at[s, m, c],
            device_id={"clu": partner}, device_id_type=MESH).wait_recv()

    own_c.wait()
    for i in range(PIECES):
        ring(0, 0, i)
        ring(1, 0, (i + half) % PIECES)
    for c in range(PIECES):
        share(0, c)
    own_d.wait()
    own_i.wait()
    doc_copies = []
    for k in range(1, nd):
        mate = lax.rem(doc + k, nd)
        for ref, ss, rs in ((ids_all, ids_send, ids_recv), (docs_all, docs_send, docs_recv)):
            copy = pltpu.make_async_remote_copy(
                src_ref=ref.at[0], dst_ref=ref.at[k], send_sem=ss.at[k], recv_sem=rs.at[k],
                device_id={"doc": mate}, device_id_type=MESH)
            copy.start()
            doc_copies.append(copy)

    def owner(s):
        if s == 0:
            p = pos
        elif s == n - 1:
            p = pos + hops
        elif s % 2:
            p = pos + n - (s + 1) // 2
        else:
            p = pos + s // 2
        return chip_at(lax.rem(p, n), n)

    ranges = ((0, n - 3), (n - 3, n - 1), (n - 1, n))
    spread = (dp_a, dp_b, dp_c)

    def permute(k):
        rows = docs_all[k]
        for (first, last), out in zip(ranges, spread):
            wide = out.shape[1]
            lane = lax.broadcasted_iota(jnp.int32, (1, wide), 1)
            target = jnp.full((1, wide), -1, jnp.int32)
            for s in range(first, last):
                chip_s = owner(s)
                for m in (0, 1):
                    part = chip_s * 2 + (core if m == 0 else 1 - core)
                    start = (2 * (s - first) + m) * fp
                    inside = (lane >= start) & (lane < start + feat)
                    target = jnp.where(inside, lane - start + part * feat, target)
            source = lax.broadcasted_iota(jnp.int32, (rows.shape[1], wide), 0)
            mover = jnp.where(source == target, 1.0, 0.0).astype(jnp.bfloat16)
            out[pl.ds(k * rows_dev, rows_dev), :] = jnp.dot(
                rows, mover, preferred_element_type=jnp.float32).astype(jnp.bfloat16)

    def prepare_ids(k):
        base = doc * width
        ids = ids_all[k] - base
        ids = jnp.where((ids >= 0) & (ids < width), ids, -1)
        full = jnp.broadcast_to(ids, (128, rows_dev)).T
        lanes = lax.broadcasted_iota(jnp.int32, (rows_dev, 128), 1)
        idb[pl.ds(k * rows_dev, rows_dev), :] = jnp.where(full >= 0, full - lanes, -(2**20))

    def phase(index, c):
        first, last = ranges[index]
        start, depth = 2 * first * fp, 2 * (last - first) * fp
        cols = pl.ds(*chunks[c])
        block = buf[pl.ds(start, depth), cols]
        prod = jnp.dot(spread[index][...], block, preferred_element_type=jnp.float32)
        w32 = block.astype(jnp.float32)
        sq = jnp.sum((w32 * w32).reshape(depth // 8, 8, chunks[c][1]), 0)
        if index == 0:
            acc[:, cols] = prod
            csq[:, cols] = sq
        else:
            acc[:, cols] += prod
            csq[:, cols] += sq

    tail = pl.ds(2 * (n - 1) * fp, 2 * fp)

    def finish_scale(c):
        cols = pl.ds(*chunks[c])
        w32 = buf[tail, cols].astype(jnp.float32)
        sq = jnp.sum((w32 * w32).reshape(2 * fp // 8, 8, chunks[c][1]), 0) + csq[:, cols]
        scale[:, cols] = lax.rsqrt(jnp.sum(sq, 0, keepdims=True) + epsilon)

    def final(k, c):
        start, wide = chunks[c]
        prod = jnp.dot(dp_c[pl.ds(k * rows_dev, rows_dev), :], buf[tail, pl.ds(start, wide)],
                       preferred_element_type=jnp.float32)
        for r in range(0, rows_dev, ROWS):
            rs = pl.ds(k * rows_dev + r, ROWS)
            top, hit = mx[rs, :], ch[rs, :]
            ids = idb[rs, :]
            for a in range(0, wide, 128):
                w = min(128, wide - a)
                cols = pl.ds(start + a, w)
                v = (acc[rs, cols] + prod[r:r + ROWS, a:a + w]) * scale[:, cols]
                if w == 128:
                    top = jnp.maximum(top, v)
                    hit = jnp.where(ids == start + a, v, hit)
                else:
                    mx[rs, :] = top
                    ch[rs, :] = hit
                    mx[rs, pl.ds(0, w)] = jnp.maximum(mx[rs, pl.ds(0, w)], v)
                    ch[rs, pl.ds(0, w)] = jnp.where(idb[rs, pl.ds(0, w)] == start + a, v, ch[rs, pl.ds(0, w)])
            if wide % 128 == 0:
                mx[rs, :] = top
                ch[rs, :] = hit

    def reduced(k):
        rs = pl.ds(k * rows_dev, rows_dev)
        return (jnp.max(mx[rs, :].T, 0, keepdims=True), jnp.sum(ch[rs, :].T, 0, keepdims=True))

    mx[...] = jnp.full(mx.shape, -3.0e38, jnp.float32)
    ch[...] = jnp.zeros(ch.shape, jnp.float32)
    permute(0)
    prepare_ids(0)
    wide = docs_all[0].astype(jnp.float32)
    squares = wide * wide
    total = squares[:, 0:128]
    for a in range(128, wide.shape[1], 128):
        total = total + squares[:, a:a + 128]
    scale_x = lax.rsqrt(jnp.sum(total.T, 0, keepdims=True) + epsilon)

    def step(way, h, c):
        s = slot(way, h)
        landed(s, 0, c)
        if h < reach(way, c):
            ring(way, h, c)
        share(s, c)

    def pair(h, i):
        step(0, h, i)
        step(1, h, (i + half) % PIECES)

    def partners(slots, c):
        for s in slots:
            landed(s, 1, c)

    early, late = range(n - 3), (n - 3, n - 2)
    order = [j // 2 + half * (j % 2) for j in range(PIECES)]
    for h in range(1, hops):
        for i in range(PIECES):
            pair(h, i)
            if h == hops - 2 and i == half:
                for copy in doc_copies:
                    copy.wait()
                for k in range(1, nd):
                    permute(k)
                    prepare_ids(k)
            if h == hops - 1:
                c = order[i]
                partners(early, c)
                phase(0, c)
    for c in order[:half]:
        partners(late, c)
        phase(1, c)
    for i in range(half):
        for way in (0, 1):
            c = i + half * way
            landed(n - 1, 0, c)
            share(n - 1, c)
    for c in order[half:]:
        partners(late, c)
        phase(1, c)
    for c in order[:-2]:
        landed(n - 1, 1, c)
        finish_scale(c)
        for k in range(nd):
            final(k, c)
    for c in order[-2:]:
        landed(n - 1, 1, c)
        finish_scale(c)

    returns = []
    for k in range(1, nd):
        for c in order[-2:]:
            final(k, c)
        best, chosen = reduced(k)
        res[k, 0:1, :] = best
        res[k, 1:2, :] = chosen
        copy = pltpu.make_async_remote_copy(
            src_ref=res.at[k], dst_ref=got.at[k], send_sem=res_send.at[k], recv_sem=res_recv.at[k],
            device_id={"doc": lax.rem(doc + nd - k, nd)}, device_id_type=MESH)
        copy.start()
        returns.append(copy)
    for c in order[-2:]:
        final(0, c)
    best, chosen = reduced(0)
    for k in range(1, nd):
        returns[k - 1].wait()
        best = jnp.maximum(best, got[k, 0:1, :])
        chosen = chosen + got[k, 1:2, :]
    near_out[...] = best * scale_x
    chosen_out[...] = chosen * scale_x
    for copy in sent:
        copy.wait_send()


def layer_kernel(nz, feat, docs_in, cents_in, ids_in, near_out, chosen_out,
                 own, raw, ends, buf, docs, flat, ids, turned, acc, idb, mx, ch, csq, scale, res, got,
                 local_sem, send_sem, c_recv, last_recv, d_recv, i_recv, r_recv):
    width = cents_in.shape[1]
    rows_dev, depth = docs_in.shape
    half = width // 2
    count, extra = half // 128, half % 128
    small = count // 2 * 128
    wide = small + extra
    turn_at = (count + 1) * 128
    full = width // 128 * 128
    rest = width - full
    late = -(-4 * feat // 256) * 256
    k1 = 8 * feat // 256 * 256
    k2 = depth - late - k1
    a = rows_dev * 5 // 16 // 16 * 16
    b = (rows_dev - a) // 32 * 16
    spans = ((0, a), (a, b), (a + b, rows_dev - a - b))
    cuts = {w: (0, 256, (w - 1) // 256 * 256, w) for w in (small, wide)}

    clu, doc = lax.axis_index("clu"), lax.axis_index("doc")
    core, chip = lax.rem(clu, 2), lax.div(clu, 2)
    z, x = lax.div(chip, 2), lax.rem(chip, 2)
    upper = z >= nz // 2
    out = jnp.where(upper, 1, -1)
    end = (z == 0) | (z == nz - 1)
    inner = jnp.logical_not(end)

    def device(r, dz=0):
        dx, dy, dc = r // 4, r // 2 % 2, r % 2
        there = ((z + dz) * 2 + (1 - x if dx else x)) * 2 + (1 - core if dc else core)
        return {"clu": there, "doc": 1 - doc if dy else doc}

    def when(cond, body):
        if cond is None:
            body()
        else:
            pl.when(cond)(body)

    def both(p, q):
        return q if p is None else p if q is None else p & q

    def sized(c, cond, body):
        for value, w in ((1, wide), (0, small)):
            when(both(cond, c == value), functools.partial(body, w))

    own_copy = pltpu.make_async_copy(cents_in.at[:, pl.ds(0, full)], own.at[:, pl.ds(0, full)], local_sem.at[0])
    docs_copy = pltpu.make_async_copy(docs_in, docs.at[0], local_sem.at[1])
    ids_copy = pltpu.make_async_copy(ids_in, ids.at[0], local_sem.at[2])
    own_copy.start()
    raw_copy = pltpu.make_async_copy(cents_in.at[:, pl.ds(full, rest)], raw, local_sem.at[3])
    raw_copy.start()
    end_copies = [pltpu.make_async_copy(cents_in.at[:, pl.ds(k * turn_at + small, small)],
                                        ends.at[k, :, pl.ds(0, small)], local_sem.at[4 + k]) for k in (0, 1)]
    for copy in end_copies:
        copy.start()
    docs_copy.start()
    ids_copy.start()

    barrier = pltpu.get_barrier_semaphore()

    def greet(to):
        pl.semaphore_signal(barrier, inc=1, device_id=to, device_id_type=MESH)

    pl.when(inner)(lambda: greet(device(0, out)))
    greet(device(0, -out))
    for r in (4, 5, 2, 1):
        greet(device(r))

    @pl.when(core == 0)
    def _():
        buf[:, pl.ds(small, extra)] = jnp.zeros((buf.shape[0], extra), buf.dtype)

    own_copy.wait()
    raw_copy.wait()
    middle = own[:, pl.ds(turn_at - 128, 128)]
    ends[0, :, pl.ds(small, extra)] = middle[:, 0:extra]
    ends[1, :, pl.ds(small, extra)] = jnp.concatenate([raw[...], middle[:, extra:128]], axis=1)
    for copy in end_copies:
        copy.wait()
    docs_copy.wait()
    ids_copy.wait()
    pl.semaphore_wait(barrier, 5 + inner.astype(jnp.int32))

    outward, inward, doc_sent, id_sent, result_sent, traded, traded_wide = (send_sem.at[i] for i in range(7))

    def start(make, cond=None):
        when(cond, lambda: make().start())

    def start_sized(make, c, cond=None):
        sized(c, cond, lambda w: make(w).start())

    def remote(src, dst, ss, rs, to):
        return pltpu.make_async_remote_copy(
            src_ref=src, dst_ref=dst, send_sem=ss, recv_sem=rs, device_id=to, device_id_type=MESH)

    near = (0, 1, 4, 5)

    def source(layer, j):
        r = near[j]
        there = (layer * 2 + (1 - x if r // 4 else x)) * 2 + (1 - core if r % 2 else core)
        return pl.ds(pl.multiple_of(there * feat, 16), feat)

    def piece(r, w):
        xd = 1 - x if r // 4 else x
        if w == wide:
            return ends.at[xd]
        return own.at[:, pl.ds(pl.multiple_of(xd * turn_at, 128), w)]

    mine = source(z, 0)

    def exchange(j):
        r = near[j]
        start_sized(lambda w: remote(piece(r, w), buf.at[mine, pl.ds(0, w)],
                                     traded_wide if w == wide else traded, c_recv.at[z, j], device(r)),
                    1 - core if r % 2 else core)

    def landed(layer, j, cond=None):
        rows = source(layer, j)
        sized(core, cond, lambda w: remote(
            buf.at[rows, pl.ds(0, w)], buf.at[rows, pl.ds(0, w)], traded, c_recv.at[layer, j],
            device(1)).wait_recv())

    def carry(layer, j, way, s, cond=None):
        rows = source(layer, j)
        src = (lambda w: piece(0, w)) if s == 0 and j == 0 else (lambda w: buf.at[rows, pl.ds(0, w)])
        start_sized(lambda w: remote(src(w), buf.at[rows, pl.ds(0, w)], inward if way else outward,
                                     c_recv.at[layer, j], device(0, -out if way else out)), core, cond)

    def spread(j):
        if j:
            landed(z, j)
        carry(z, j, 0, 0, inner)
        carry(z, j, 1, 0)

    def relay(j):
        landed(z - out, j)
        carry(z - out, j, 0, 1, inner)
        landed(z + out, j, inner)
        carry(z + out, j, 1, 1, inner)

    def pair(layer, k, w):
        rows = pl.ds(pl.multiple_of((layer * 2 + 1 - x) * 2 * feat, 16), 2 * feat)
        return buf.at[rows, pl.ds(cuts[w][k], cuts[w][k + 1] - cuts[w][k])]

    def relay_far(j):
        landed(z - 2 * out, j)
        if j < 2:
            carry(z - 2 * out, j, 0, 2, inner)

    def send_last(cond):
        for k in range(3):
            start_sized(lambda w, k=k: remote(
                pair(z - 2 * out, k, w), pair(z - 2 * out, k, w), outward, last_recv.at[k],
                device(0, out)), core, inner & cond)

    def last_landed(k):
        sized(core, end, lambda w: remote(
            pair(z - 3 * out, k, w), pair(z - 3 * out, k, w), outward, last_recv.at[k],
            device(1)).wait_recv())

    ahead = {(1, 0): 0, (1, 1): 0, (1, 2): 0, (3, 0): 1, (3, 1): 1, (3, 2): 1, (5, 0): 2, (5, 1): 2, (5, 2): 2,
             (7, 0): 3, (7, 1): 3, (7, 2): 3, (2, 0): 4, (2, 1): 5, (2, 2): 5, (4, 0): 6, (4, 1): 7, (4, 2): 8,
             (6, 0): 9, (6, 1): 10, (6, 2): 11}
    id_at = {1: 0, 3: 0, 5: 0, 7: 0, 2: 1, 4: 2, 6: 3}

    def part(slot, *parts):
        first, last = spans[parts[0]], spans[parts[-1]]
        return docs.at[slot, pl.ds(first[0], last[0] + last[1] - first[0]), :]

    def send_docs(src_slot, dst_slot, r, *parts):
        start(lambda: remote(part(src_slot, *parts), part(dst_slot, *parts), doc_sent,
                             d_recv.at[ahead[dst_slot, parts[0]]], device(r)))

    def send_ids(src_slot, dst_slot, r):
        start(lambda: remote(ids.at[src_slot], ids.at[dst_slot], id_sent, i_recv.at[id_at[dst_slot]], device(r)))

    def have_docs(slot, *parts):
        remote(part(slot, *parts), part(slot, *parts), doc_sent, d_recv.at[ahead[slot, parts[0]]],
               device(1)).wait_recv()

    def have_ids(slot):
        some = ids.at[pl.ds(0, 4)] if slot % 2 else ids.at[slot]
        remote(some, some, id_sent, i_recv.at[id_at[slot]], device(1)).wait_recv()

    def share(slot, *parts):
        send_docs(slot, slot + 1, 1, *parts)

    spread(0)
    for j in (1, 2, 3):
        exchange(j)
    send_ids(0, 2, 2)
    send_docs(0, 2, 2, 0)
    send_docs(0, 2, 2, 1, 2)
    send_ids(0, 4, 4)
    for p in (1, 2, 0):
        send_docs(0, 4, 4, p)
    send_ids(0, 1, 1)
    send_docs(0, 1, 1, 0, 1, 2)

    first = x * turn_at + core * small
    reach = small + jnp.where(core == 0, 0, jnp.where(x == 0, extra, rest))
    tail = (core == 1) & (x == 1)
    lines = lax.broadcasted_iota(jnp.int32, (GROUP, rows_dev), 0)

    def prepare_ids(slot):
        local = ids[slot] - doc * width
        rel = jnp.where((local >= first) & (local < first + reach), local - first, -(2**20))
        rel = jnp.where((local >= half) & (local < turn_at) & tail, local - half + small + rest, rel)
        idb[:, pl.ds(slot * rows_dev, rows_dev)] = jnp.broadcast_to(rel, (GROUP, rows_dev)) - lines

    def place(w):
        buf[mine, pl.ds(0, w)] = ends[x] if w == wide else piece(0, w)[...]

    sized(core, None, place)

    k1_at = pl.multiple_of(jnp.where(upper, depth - k1, 0), 256)
    k2_at = pl.multiple_of(jnp.where(upper, late, k1), 256)
    late_at = pl.multiple_of(jnp.where(upper, 0, depth - late), 256)
    starts = (k1_at, k2_at, late_at)

    def squares(i, c, w):
        w32 = buf[pl.ds(starts[i], 256), pl.ds(c, w)].astype(jnp.float32)
        return jnp.sum((w32 * w32).reshape(32, 8, w), 0)

    def turn(i, c, w):
        turned[i, pl.ds(c, w), :] = buf[pl.ds(starts[i], 256), pl.ds(c, w)].T

    def gather(i):
        for c in range(0, wide, 256):
            turn(i, c, min(256, wide - c))
        csq[...] = squares(i, 0, wide) + (csq[...] if i else 0.0)

    def flatten(*slots):
        for slot in slots:
            flat[:, pl.ds(slot * rows_dev, rows_dev)] = docs[slot].T

    def times(i, c, w, slot, count):
        return jnp.dot(turned[i, pl.ds(c, w), :],
                       flat[pl.ds(starts[i], 256), pl.ds(slot * rows_dev, count * rows_dev)],
                       preferred_element_type=jnp.float32)

    def begin(slot, count, *phases):
        where_docs = pl.ds(slot * rows_dev, count * rows_dev)

        def add(w):
            prod = times(phases[0], 0, w, slot, count)
            for i in phases[1:]:
                prod = prod + times(i, 0, w, slot, count)
            if phases[0]:
                acc[pl.ds(0, w), where_docs] += prod
            else:
                acc[pl.ds(0, w), where_docs] = prod

        sized(core, None, add)

    spread(1)
    prepare_ids(0)
    flatten(0)
    spread(2)
    relay(0)
    spread(3)
    relay(1)
    have_docs(2, 0)
    send_docs(2, 6, 4, 0)
    have_ids(4)
    send_ids(4, 6, 2)
    send_ids(4, 5, 1)
    have_ids(2)
    send_ids(2, 3, 1)
    relay(2)
    have_docs(4, 1)
    send_docs(4, 6, 2, 1)
    have_docs(1, 0, 1, 2)
    flatten(1)
    relay(3)
    relay_far(0)
    have_docs(2, 1, 2)
    share(2, 0, 1, 2)
    have_docs(4, 2)
    send_docs(4, 6, 2, 2)
    have_ids(6)
    send_ids(6, 7, 1)
    relay_far(1)
    gather(0)
    begin(0, 2, 0)
    flatten(2)
    have_ids(1)
    for slot in (1, 2, 3, 4, 5, 6, 7):
        prepare_ids(slot)
    relay_far(2)
    have_docs(4, 0)
    share(4, 0, 1, 2)
    relay_far(3)
    send_last(core == 0)
    have_docs(3, 0, 1, 2)
    flatten(3)
    begin(2, 2, 0)
    gather(1)
    send_last(core == 1)
    flatten(4)
    begin(0, 2, 1)
    begin(2, 2, 1)

    def share_far():
        for p in (1, 2, 0):
            have_docs(6, p)
        share(6, 0, 1, 2)

    pl.when(core == 1)(share_far)
    have_docs(5, 0, 1, 2)
    flatten(5)
    pl.when(core == 0)(share_far)
    begin(4, 2, 0, 1)
    flatten(6)

    def scales(c, w):
        total = jnp.sum(csq[:, pl.ds(c, w)] + squares(2, c, w), 0, keepdims=True)
        scale[pl.ds(c, w), :] = jnp.broadcast_to(lax.rsqrt(total + epsilon), (128, w)).T

    def stage(c0, w, slot, count):
        prod = times(2, c0, w, slot, count)
        spots = [pl.ds(slot * rows_dev + d, 128) for d in range(0, count * rows_dev, 128)]
        if c0:
            tops, hits = [mx[:, at] for at in spots], [ch[:, at] for at in spots]
        else:
            tops = [jnp.full((GROUP, 128), -3.0e38, jnp.float32)] * len(spots)
            hits = [jnp.zeros((GROUP, 128), jnp.float32)] * len(spots)
        for c in range(0, w, GROUP):
            rows = pl.ds(c0 + c, GROUP)
            by = scale[rows, :]
            for n, at in enumerate(spots):
                v = (acc[rows, at] + prod[c:c + GROUP, n * 128:n * 128 + 128]) * by
                hits[n] = jnp.where(idb[:, at] == c0 + c, v, hits[n])
                tops[n] = jnp.maximum(tops[n], v)
        for n, at in enumerate(spots):
            mx[:, at], ch[:, at] = tops[n], hits[n]

    def reduced(slot):
        at = pl.ds(slot * rows_dev, rows_dev)
        return jnp.max(mx[:, at], 0, keepdims=True), jnp.sum(ch[:, at], 0, keepdims=True)

    def give(slot):
        best, chosen = reduced(slot)
        res[slot, 0:1, :] = best
        res[slot, 1:2, :] = chosen
        remote(res.at[slot], got.at[slot], result_sent, r_recv, device(slot)).start()

    x32 = docs[0].astype(jnp.float32)
    sq = x32 * x32
    total = sq[:, 0:128]
    for c in range(128, depth, 128):
        total = total + sq[:, c:c + 128]
    scale_x = lax.rsqrt(jnp.sum(total.T, 0, keepdims=True) + epsilon)

    landed(z - 3 * out, 0, end)
    landed(z - 3 * out, 1, end)
    have_docs(7, 0, 1, 2)
    flatten(7)
    begin(6, 2, 0, 1)

    def advance(k, have):
        c, w = cuts[have][k], cuts[have][k + 1] - cuts[have][k]
        turn(2, c, w)
        scales(c, w)
        for slot in (6, 2, 4, 0):
            stage(c, w, slot, 2)
            if k == 2:
                give(slot + 1)
                if slot:
                    give(slot)

    for k in range(3):
        last_landed(k)
        sized(core, None, functools.partial(advance, k))
    best, chosen = reduced(0)
    everyone = pl.ds(1, 7)
    remote(got.at[everyone], got.at[everyone], result_sent, r_recv, device(1)).wait_recv()
    for slot in range(1, 8):
        best = jnp.maximum(best, got[slot, 0:1, :])
        chosen = chosen + got[slot, 1:2, :]
    near_out[...] = best * scale_x
    chosen_out[...] = chosen * scale_x

    def sent(ref, sem):
        remote(ref, ref, sem, r_recv, device(1)).wait_send()

    sent(res.at[everyone], result_sent)
    sent(docs.at[everyone], doc_sent)
    sent(ids.at[everyone], id_sent)
    layer = 4 * feat
    sized(core, inner, lambda w: sent(buf.at[pl.ds(0, 3 * layer), pl.ds(0, w)], outward))
    sized(core, inner, lambda w: sent(buf.at[pl.ds(0, 2 * layer), pl.ds(0, w)], inward))
    sized(core, end, lambda w: sent(buf.at[pl.ds(0, layer), pl.ds(0, w)], inward))
    for w, sem, two in ((wide, traded_wide, 0), (small, traded, 1)):
        pl.when(core == two)(lambda: sent(buf.at[pl.ds(0, 2 * feat), pl.ds(0, w)], sem))
        pl.when(core != two)(lambda: sent(buf.at[pl.ds(0, feat), pl.ds(0, w)], sem))


def by_layers(docs, centroids, assigned):
    nz = lax.axis_size("clu") // 4
    rows_dev, depth = docs.shape
    width, feat = centroids.shape
    wide = width // 512 * 128 + width // 2 % 128
    any_space = pl.BlockSpec(memory_space=pl.ANY)
    vmem = pl.BlockSpec(memory_space=pltpu.VMEM)
    dma = pltpu.SemaphoreType.DMA
    line = pltpu.VMEM((1, rows_dev), jnp.float32)
    near, chosen = pl.pallas_call(
        functools.partial(layer_kernel, nz, feat),
        out_shape=(line, line),
        in_specs=[any_space] * 3,
        out_specs=(vmem, vmem),
        scratch_shapes=[
            pltpu.VMEM((feat, width // 128 * 128), jnp.bfloat16),
            pltpu.VMEM((feat, width % 128), jnp.bfloat16),
            pltpu.VMEM((2, feat, wide), jnp.bfloat16),
            pltpu.VMEM((depth, wide), jnp.bfloat16),
            pltpu.VMEM((8, rows_dev, depth), jnp.bfloat16),
            pltpu.VMEM((depth, 8 * rows_dev), jnp.bfloat16),
            pltpu.VMEM((8, 1, rows_dev), jnp.int32),
            pltpu.VMEM((3, wide, 256), jnp.bfloat16),
            pltpu.VMEM((wide, 8 * rows_dev), jnp.float32),
            pltpu.VMEM((GROUP, 8 * rows_dev), jnp.int32),
            pltpu.VMEM((GROUP, 8 * rows_dev), jnp.float32),
            pltpu.VMEM((GROUP, 8 * rows_dev), jnp.float32),
            pltpu.VMEM((8, wide), jnp.float32),
            pltpu.VMEM((wide, 128), jnp.float32),
            pltpu.VMEM((8, 2, rows_dev), jnp.float32),
            pltpu.VMEM((8, 2, rows_dev), jnp.float32),
            dma((6,)), dma((7,)), dma((nz, 4)), dma((3,)), dma((12,)), dma((4,)), dma,
        ],
        compiler_params=pltpu.CompilerParams(collective_id=0, has_side_effects=True),
        name="layer_distances",
    )(docs, centroids.T, assigned.reshape(1, rows_dev))
    return 1.0 - near.reshape(rows_dev), 1.0 - chosen.reshape(rows_dev)


def fits_layers(docs, centroids):
    n_clu, feat = lax.axis_size("clu"), centroids.shape[1]
    width = centroids.shape[0]
    count, extra = width // 2 // 128, width // 2 % 128
    return (lax.axis_size("doc") == 2 and n_clu == 16 and feat % 16 == 0
            and width % 2 == 0 and count % 2 == 0 and count >= 10 and extra > 64 and extra % GROUP == 0
            and docs.shape[0] % 128 == 0 and docs.shape[1] == n_clu * feat == 3 * 256)


def on_device(docs, centroids, assigned):
    if fits_layers(docs, centroids):
        return by_layers(docs, centroids, assigned)
    n_clu, nd = lax.axis_size("clu"), lax.axis_size("doc")
    n = n_clu // 2
    rows_dev, depth = docs.shape
    width, feat = centroids.shape
    fp = (feat + 15) // 16 * 16
    cents = centroids.T
    if fp != feat:
        cents = jnp.pad(cents, ((0, fp - feat), (0, 0)))
    rows = nd * rows_dev
    any_space = pl.BlockSpec(memory_space=pl.ANY)
    vmem = pl.BlockSpec(memory_space=pltpu.VMEM)
    dma = pltpu.SemaphoreType.DMA
    hops = n // 2
    line = jax.ShapeDtypeStruct((1, rows_dev), jnp.float32)
    near, chosen = pl.pallas_call(
        functools.partial(kernel, n, nd, feat),
        out_shape=(line, line),
        in_specs=[any_space] * 3,
        out_specs=(vmem, vmem),
        scratch_shapes=[
            pltpu.VMEM((n_clu * fp, width), jnp.bfloat16),
            pltpu.VMEM((nd, rows_dev, depth), jnp.bfloat16),
            pltpu.VMEM((nd, 1, rows_dev), jnp.int32),
            pltpu.VMEM((rows, (n - 3) * 2 * fp), jnp.bfloat16),
            pltpu.VMEM((rows, 4 * fp), jnp.bfloat16),
            pltpu.VMEM((rows, 2 * fp), jnp.bfloat16),
            pltpu.VMEM((rows, width), jnp.float32),
            pltpu.VMEM((rows, 128), jnp.int32),
            pltpu.VMEM((rows, 128), jnp.float32),
            pltpu.VMEM((rows, 128), jnp.float32),
            pltpu.VMEM((8, width), jnp.float32),
            pltpu.VMEM((1, width), jnp.float32),
            pltpu.VMEM((nd, 2, rows_dev), jnp.float32),
            pltpu.VMEM((nd, 2, rows_dev), jnp.float32),
            dma((3,)),
            dma((2, hops, PIECES)),
            dma((n, PIECES)),
            dma((n, 2, PIECES)),
            dma((nd,)), dma((nd,)), dma((nd,)), dma((nd,)), dma((nd,)), dma((nd,)),
        ],
        compiler_params=pltpu.CompilerParams(collective_id=0, has_side_effects=True),
        name="ring_distances",
    )(docs, cents, assigned.reshape(1, rows_dev))
    return 1.0 - near.reshape(rows_dev), 1.0 - chosen.reshape(rows_dev)


def solution(mesh):
    placed = (P(("clu", "doc"), None), P("doc", "clu"), P(("clu", "doc")))
    return jax.shard_map(
        on_device,
        mesh=mesh,
        in_specs=placed,
        out_specs=(P(("clu", "doc")), P(("clu", "doc"))),
        check_vma=False,
    )
```

```python
import functools

import jax
import jax.numpy as jnp
from jax import lax
from jax.experimental import pallas as pl
from jax.experimental.pallas import tpu as pltpu
from jax.sharding import PartitionSpec as P

epsilon = 1e-06
PIECES = 4
ROWS = 64
GROUP = 16
MESH = pl.DeviceIdType.MESH


def chip_at(pos, n):
    half = n // 2
    return jnp.where(pos < half, 2 * pos, 2 * (n - 1 - pos) + 1)


def cut(width):
    tiles = (width + 127) // 128
    ends = [min(-(-tiles * (c + 1) // PIECES) * 128, width) for c in range(PIECES)]
    return tuple((a, b - a) for a, b in zip([0] + ends[:-1], ends))


def kernel(n, nd, feat, docs_in, cents_in, ids_in, near_out, chosen_out,
           buf, docs_all, ids_all, dp_a, dp_b, dp_c, acc, idb, mx, ch, csq, scale, res, got,
           local_sem, ring_send, pair_send, recv, docs_send, docs_recv, ids_send, ids_recv,
           res_send, res_recv):
    hops = n // 2
    fp = cents_in.shape[0]
    width = cents_in.shape[1]
    rows_dev = docs_in.shape[0]
    chunks = cut(width)
    half = len(chunks) // 2

    clu, doc = lax.axis_index("clu"), lax.axis_index("doc")
    core, chip = lax.rem(clu, 2), lax.div(clu, 2)
    z, x = lax.div(chip, 2), lax.rem(chip, 2)
    pos = jnp.where(x == 0, z, n - 1 - z)
    right = chip_at(lax.rem(pos + 1, n), n) * 2 + core
    left = chip_at(lax.rem(pos + n - 1, n), n) * 2 + core
    partner = chip * 2 + (1 - core)

    own_c = pltpu.make_async_copy(cents_in, buf.at[pl.ds(0, fp), :], local_sem.at[0])
    own_d = pltpu.make_async_copy(docs_in, docs_all.at[0], local_sem.at[1])
    own_i = pltpu.make_async_copy(ids_in, ids_all.at[0], local_sem.at[2])
    own_c.start()
    own_d.start()
    own_i.start()

    barrier = pltpu.get_barrier_semaphore()
    for peer in (left, right, partner):
        pl.semaphore_signal(barrier, inc=1, device_id={"clu": peer}, device_id_type=MESH)
    for k in range(1, nd):
        pl.semaphore_signal(barrier, inc=1, device_id={"doc": lax.rem(doc + k, nd)}, device_id_type=MESH)
    pl.semaphore_wait(barrier, 3 + nd - 1)

    def slot(way, h):
        if h == 0:
            return 0
        if h == hops:
            return n - 1
        return 2 * h - 1 if way == 0 else 2 * h

    def piece(s, m, c):
        return buf.at[pl.ds((2 * s + m) * fp, fp), pl.ds(*chunks[c])]

    def reach(way, c):
        return hops if way == c // half else hops - 1

    sent = []

    def ring(way, h, c):
        s, t = slot(way, h), slot(way, h + 1)
        copy = pltpu.make_async_remote_copy(
            src_ref=piece(s, 0, c), dst_ref=piece(t, 0, c),
            send_sem=ring_send.at[way, h, c], recv_sem=recv.at[t, 0, c],
            device_id={"clu": right if way == 0 else left}, device_id_type=MESH)
        copy.start()
        sent.append(copy)

    def share(s, c):
        copy = pltpu.make_async_remote_copy(
            src_ref=piece(s, 0, c), dst_ref=piece(s, 1, c),
            send_sem=pair_send.at[s, c], recv_sem=recv.at[s, 1, c],
            device_id={"clu": partner}, device_id_type=MESH)
        copy.start()
        sent.append(copy)

    def landed(s, m, c):
        pltpu.make_async_remote_copy(
            src_ref=piece(s, m, c), dst_ref=piece(s, m, c),
            send_sem=pair_send.at[s, c], recv_sem=recv.at[s, m, c],
            device_id={"clu": partner}, device_id_type=MESH).wait_recv()

    own_c.wait()
    for i in range(PIECES):
        ring(0, 0, i)
        ring(1, 0, (i + half) % PIECES)
    for c in range(PIECES):
        share(0, c)
    own_d.wait()
    own_i.wait()
    doc_copies = []
    for k in range(1, nd):
        mate = lax.rem(doc + k, nd)
        for ref, ss, rs in ((ids_all, ids_send, ids_recv), (docs_all, docs_send, docs_recv)):
            copy = pltpu.make_async_remote_copy(
                src_ref=ref.at[0], dst_ref=ref.at[k], send_sem=ss.at[k], recv_sem=rs.at[k],
                device_id={"doc": mate}, device_id_type=MESH)
            copy.start()
            doc_copies.append(copy)

    def owner(s):
        if s == 0:
            p = pos
        elif s == n - 1:
            p = pos + hops
        elif s % 2:
            p = pos + n - (s + 1) // 2
        else:
            p = pos + s // 2
        return chip_at(lax.rem(p, n), n)

    ranges = ((0, n - 3), (n - 3, n - 1), (n - 1, n))
    spread = (dp_a, dp_b, dp_c)

    def permute(k):
        rows = docs_all[k]
        for (first, last), out in zip(ranges, spread):
            wide = out.shape[1]
            lane = lax.broadcasted_iota(jnp.int32, (1, wide), 1)
            target = jnp.full((1, wide), -1, jnp.int32)
            for s in range(first, last):
                chip_s = owner(s)
                for m in (0, 1):
                    part = chip_s * 2 + (core if m == 0 else 1 - core)
                    start = (2 * (s - first) + m) * fp
                    inside = (lane >= start) & (lane < start + feat)
                    target = jnp.where(inside, lane - start + part * feat, target)
            source = lax.broadcasted_iota(jnp.int32, (rows.shape[1], wide), 0)
            mover = jnp.where(source == target, 1.0, 0.0).astype(jnp.bfloat16)
            out[pl.ds(k * rows_dev, rows_dev), :] = jnp.dot(
                rows, mover, preferred_element_type=jnp.float32).astype(jnp.bfloat16)

    def prepare_ids(k):
        base = doc * width
        ids = ids_all[k] - base
        ids = jnp.where((ids >= 0) & (ids < width), ids, -1)
        full = jnp.broadcast_to(ids, (128, rows_dev)).T
        lanes = lax.broadcasted_iota(jnp.int32, (rows_dev, 128), 1)
        idb[pl.ds(k * rows_dev, rows_dev), :] = jnp.where(full >= 0, full - lanes, -(2**20))

    def phase(index, c):
        first, last = ranges[index]
        start, depth = 2 * first * fp, 2 * (last - first) * fp
        cols = pl.ds(*chunks[c])
        block = buf[pl.ds(start, depth), cols]
        prod = jnp.dot(spread[index][...], block, preferred_element_type=jnp.float32)
        w32 = block.astype(jnp.float32)
        sq = jnp.sum((w32 * w32).reshape(depth // 8, 8, chunks[c][1]), 0)
        if index == 0:
            acc[:, cols] = prod
            csq[:, cols] = sq
        else:
            acc[:, cols] += prod
            csq[:, cols] += sq

    tail = pl.ds(2 * (n - 1) * fp, 2 * fp)

    def finish_scale(c):
        cols = pl.ds(*chunks[c])
        w32 = buf[tail, cols].astype(jnp.float32)
        sq = jnp.sum((w32 * w32).reshape(2 * fp // 8, 8, chunks[c][1]), 0) + csq[:, cols]
        scale[:, cols] = lax.rsqrt(jnp.sum(sq, 0, keepdims=True) + epsilon)

    def final(k, c):
        start, wide = chunks[c]
        prod = jnp.dot(dp_c[pl.ds(k * rows_dev, rows_dev), :], buf[tail, pl.ds(start, wide)],
                       preferred_element_type=jnp.float32)
        for r in range(0, rows_dev, ROWS):
            rs = pl.ds(k * rows_dev + r, ROWS)
            top, hit = mx[rs, :], ch[rs, :]
            ids = idb[rs, :]
            for a in range(0, wide, 128):
                w = min(128, wide - a)
                cols = pl.ds(start + a, w)
                v = (acc[rs, cols] + prod[r:r + ROWS, a:a + w]) * scale[:, cols]
                if w == 128:
                    top = jnp.maximum(top, v)
                    hit = jnp.where(ids == start + a, v, hit)
                else:
                    mx[rs, :] = top
                    ch[rs, :] = hit
                    mx[rs, pl.ds(0, w)] = jnp.maximum(mx[rs, pl.ds(0, w)], v)
                    ch[rs, pl.ds(0, w)] = jnp.where(idb[rs, pl.ds(0, w)] == start + a, v, ch[rs, pl.ds(0, w)])
            if wide % 128 == 0:
                mx[rs, :] = top
                ch[rs, :] = hit

    def reduced(k):
        rs = pl.ds(k * rows_dev, rows_dev)
        return (jnp.max(mx[rs, :].T, 0, keepdims=True), jnp.sum(ch[rs, :].T, 0, keepdims=True))

    mx[...] = jnp.full(mx.shape, -3.0e38, jnp.float32)
    ch[...] = jnp.zeros(ch.shape, jnp.float32)
    permute(0)
    prepare_ids(0)
    wide = docs_all[0].astype(jnp.float32)
    squares = wide * wide
    total = squares[:, 0:128]
    for a in range(128, wide.shape[1], 128):
        total = total + squares[:, a:a + 128]
    scale_x = lax.rsqrt(jnp.sum(total.T, 0, keepdims=True) + epsilon)

    def step(way, h, c):
        s = slot(way, h)
        landed(s, 0, c)
        if h < reach(way, c):
            ring(way, h, c)
        share(s, c)

    def pair(h, i):
        step(0, h, i)
        step(1, h, (i + half) % PIECES)

    def partners(slots, c):
        for s in slots:
            landed(s, 1, c)

    early, late = range(n - 3), (n - 3, n - 2)
    order = [j // 2 + half * (j % 2) for j in range(PIECES)]
    for h in range(1, hops):
        for i in range(PIECES):
            pair(h, i)
            if h == hops - 2 and i == half:
                for copy in doc_copies:
                    copy.wait()
                for k in range(1, nd):
                    permute(k)
                    prepare_ids(k)
            if h == hops - 1:
                c = order[i]
                partners(early, c)
                phase(0, c)
    for c in order[:half]:
        partners(late, c)
        phase(1, c)
    for i in range(half):
        for way in (0, 1):
            c = i + half * way
            landed(n - 1, 0, c)
            share(n - 1, c)
    for c in order[half:]:
        partners(late, c)
        phase(1, c)
    for c in order[:-2]:
        landed(n - 1, 1, c)
        finish_scale(c)
        for k in range(nd):
            final(k, c)
    for c in order[-2:]:
        landed(n - 1, 1, c)
        finish_scale(c)

    returns = []
    for k in range(1, nd):
        for c in order[-2:]:
            final(k, c)
        best, chosen = reduced(k)
        res[k, 0:1, :] = best
        res[k, 1:2, :] = chosen
        copy = pltpu.make_async_remote_copy(
            src_ref=res.at[k], dst_ref=got.at[k], send_sem=res_send.at[k], recv_sem=res_recv.at[k],
            device_id={"doc": lax.rem(doc + nd - k, nd)}, device_id_type=MESH)
        copy.start()
        returns.append(copy)
    for c in order[-2:]:
        final(0, c)
    best, chosen = reduced(0)
    for k in range(1, nd):
        returns[k - 1].wait()
        best = jnp.maximum(best, got[k, 0:1, :])
        chosen = chosen + got[k, 1:2, :]
    near_out[...] = best * scale_x
    chosen_out[...] = chosen * scale_x
    for copy in sent:
        copy.wait_send()


def layer_kernel(nz, feat, docs_in, cents_in, ids_in, near_out, chosen_out,
                 own, raw, ends, buf, docs, flat, ids, turned, acc, idb, mx, ch, csq, scale, res, got,
                 local_sem, send_sem, c_recv, last_recv, d_recv, i_recv, r_recv):
    width = cents_in.shape[1]
    rows_dev, depth = docs_in.shape
    half = width // 2
    count, extra = half // 128, half % 128
    small = count // 2 * 128
    wide = small + extra
    turn_at = (count + 1) * 128
    full = width // 128 * 128
    rest = width - full
    late = -(-4 * feat // 256) * 256
    k1 = 8 * feat // 256 * 256
    k2 = depth - late - k1
    a = rows_dev * 5 // 16 // 16 * 16
    b = (rows_dev - a) // 32 * 16
    spans = ((0, a), (a, b), (a + b, rows_dev - a - b))
    cuts = {w: (0, 256, (w - 1) // 256 * 256, w) for w in (small, wide)}

    clu, doc = lax.axis_index("clu"), lax.axis_index("doc")
    core, chip = lax.rem(clu, 2), lax.div(clu, 2)
    z, x = lax.div(chip, 2), lax.rem(chip, 2)
    upper = z >= nz // 2
    out = jnp.where(upper, 1, -1)
    end = (z == 0) | (z == nz - 1)
    inner = jnp.logical_not(end)

    def device(r, dz=0):
        dx, dy, dc = r // 4, r // 2 % 2, r % 2
        there = ((z + dz) * 2 + (1 - x if dx else x)) * 2 + (1 - core if dc else core)
        return {"clu": there, "doc": 1 - doc if dy else doc}

    def when(cond, body):
        if cond is None:
            body()
        else:
            pl.when(cond)(body)

    def both(p, q):
        return q if p is None else p if q is None else p & q

    def sized(c, cond, body):
        for value, w in ((1, wide), (0, small)):
            when(both(cond, c == value), functools.partial(body, w))

    own_copy = pltpu.make_async_copy(cents_in.at[:, pl.ds(0, full)], own.at[:, pl.ds(0, full)], local_sem.at[0])
    docs_copy = pltpu.make_async_copy(docs_in, docs.at[0], local_sem.at[1])
    ids_copy = pltpu.make_async_copy(ids_in, ids.at[0], local_sem.at[2])
    own_copy.start()
    raw_copy = pltpu.make_async_copy(cents_in.at[:, pl.ds(full, rest)], raw, local_sem.at[3])
    raw_copy.start()
    end_copies = [pltpu.make_async_copy(cents_in.at[:, pl.ds(k * turn_at + small, small)],
                                        ends.at[k, :, pl.ds(0, small)], local_sem.at[4 + k]) for k in (0, 1)]
    for copy in end_copies:
        copy.start()
    docs_copy.start()
    ids_copy.start()

    barrier = pltpu.get_barrier_semaphore()

    def greet(to):
        pl.semaphore_signal(barrier, inc=1, device_id=to, device_id_type=MESH)

    pl.when(inner)(lambda: greet(device(0, out)))
    greet(device(0, -out))
    for r in (4, 5, 2, 1):
        greet(device(r))

    @pl.when(core == 0)
    def _():
        buf[:, pl.ds(small, extra)] = jnp.zeros((buf.shape[0], extra), buf.dtype)

    own_copy.wait()
    raw_copy.wait()
    middle = own[:, pl.ds(turn_at - 128, 128)]
    ends[0, :, pl.ds(small, extra)] = middle[:, 0:extra]
    ends[1, :, pl.ds(small, extra)] = jnp.concatenate([raw[...], middle[:, extra:128]], axis=1)
    for copy in end_copies:
        copy.wait()
    docs_copy.wait()
    ids_copy.wait()
    pl.semaphore_wait(barrier, 5 + inner.astype(jnp.int32))

    outward, inward, doc_sent, id_sent, result_sent, traded, traded_wide = (send_sem.at[i] for i in range(7))

    def start(make, cond=None):
        when(cond, lambda: make().start())

    def start_sized(make, c, cond=None):
        sized(c, cond, lambda w: make(w).start())

    def remote(src, dst, ss, rs, to):
        return pltpu.make_async_remote_copy(
            src_ref=src, dst_ref=dst, send_sem=ss, recv_sem=rs, device_id=to, device_id_type=MESH)

    near = (0, 1, 4, 5)

    def source(layer, j):
        r = near[j]
        there = (layer * 2 + (1 - x if r // 4 else x)) * 2 + (1 - core if r % 2 else core)
        return pl.ds(pl.multiple_of(there * feat, 16), feat)

    def piece(r, w):
        xd = 1 - x if r // 4 else x
        if w == wide:
            return ends.at[xd]
        return own.at[:, pl.ds(pl.multiple_of(xd * turn_at, 128), w)]

    mine = source(z, 0)

    def exchange(j):
        r = near[j]
        start_sized(lambda w: remote(piece(r, w), buf.at[mine, pl.ds(0, w)],
                                     traded_wide if w == wide else traded, c_recv.at[z, j], device(r)),
                    1 - core if r % 2 else core)

    def landed(layer, j, cond=None):
        rows = source(layer, j)
        sized(core, cond, lambda w: remote(
            buf.at[rows, pl.ds(0, w)], buf.at[rows, pl.ds(0, w)], traded, c_recv.at[layer, j],
            device(1)).wait_recv())

    def carry(layer, j, way, s, cond=None):
        rows = source(layer, j)
        src = (lambda w: piece(0, w)) if s == 0 and j == 0 else (lambda w: buf.at[rows, pl.ds(0, w)])
        start_sized(lambda w: remote(src(w), buf.at[rows, pl.ds(0, w)], inward if way else outward,
                                     c_recv.at[layer, j], device(0, -out if way else out)), core, cond)

    def spread(j):
        if j:
            landed(z, j)
        carry(z, j, 0, 0, inner)
        carry(z, j, 1, 0)

    def relay(j):
        landed(z - out, j)
        carry(z - out, j, 0, 1, inner)
        landed(z + out, j, inner)
        carry(z + out, j, 1, 1, inner)

    def pair(layer, k, w):
        rows = pl.ds(pl.multiple_of((layer * 2 + 1 - x) * 2 * feat, 16), 2 * feat)
        return buf.at[rows, pl.ds(cuts[w][k], cuts[w][k + 1] - cuts[w][k])]

    def relay_far(j):
        landed(z - 2 * out, j)
        if j < 2:
            carry(z - 2 * out, j, 0, 2, inner)

    def send_last(cond):
        for k in range(3):
            start_sized(lambda w, k=k: remote(
                pair(z - 2 * out, k, w), pair(z - 2 * out, k, w), outward, last_recv.at[k],
                device(0, out)), core, inner & cond)

    def last_landed(k):
        sized(core, end, lambda w: remote(
            pair(z - 3 * out, k, w), pair(z - 3 * out, k, w), outward, last_recv.at[k],
            device(1)).wait_recv())

    ahead = {(1, 0): 0, (1, 1): 0, (1, 2): 0, (3, 0): 1, (3, 1): 1, (3, 2): 1, (5, 0): 2, (5, 1): 2, (5, 2): 2,
             (7, 0): 3, (7, 1): 3, (7, 2): 3, (2, 0): 4, (2, 1): 5, (2, 2): 5, (4, 0): 6, (4, 1): 7, (4, 2): 8,
             (6, 0): 9, (6, 1): 10, (6, 2): 11}
    id_at = {1: 0, 3: 0, 5: 0, 7: 0, 2: 1, 4: 2, 6: 3}

    def part(slot, *parts):
        first, last = spans[parts[0]], spans[parts[-1]]
        return docs.at[slot, pl.ds(first[0], last[0] + last[1] - first[0]), :]

    def send_docs(src_slot, dst_slot, r, *parts):
        start(lambda: remote(part(src_slot, *parts), part(dst_slot, *parts), doc_sent,
                             d_recv.at[ahead[dst_slot, parts[0]]], device(r)))

    def send_ids(src_slot, dst_slot, r):
        start(lambda: remote(ids.at[src_slot], ids.at[dst_slot], id_sent, i_recv.at[id_at[dst_slot]], device(r)))

    def have_docs(slot, *parts):
        remote(part(slot, *parts), part(slot, *parts), doc_sent, d_recv.at[ahead[slot, parts[0]]],
               device(1)).wait_recv()

    def have_ids(slot):
        some = ids.at[pl.ds(0, 4)] if slot % 2 else ids.at[slot]
        remote(some, some, id_sent, i_recv.at[id_at[slot]], device(1)).wait_recv()

    def share(slot, *parts):
        send_docs(slot, slot + 1, 1, *parts)

    spread(0)
    for j in (1, 2, 3):
        exchange(j)
    send_ids(0, 2, 2)
    send_docs(0, 2, 2, 0)
    send_docs(0, 2, 2, 1, 2)
    send_ids(0, 4, 4)
    for p in (1, 2, 0):
        send_docs(0, 4, 4, p)
    send_ids(0, 1, 1)
    send_docs(0, 1, 1, 0, 1, 2)

    first = x * turn_at + core * small
    reach = small + jnp.where(core == 0, 0, jnp.where(x == 0, extra, rest))
    tail = (core == 1) & (x == 1)
    lines = lax.broadcasted_iota(jnp.int32, (GROUP, rows_dev), 0)

    def prepare_ids(slot):
        local = ids[slot] - doc * width
        rel = jnp.where((local >= first) & (local < first + reach), local - first, -(2**20))
        rel = jnp.where((local >= half) & (local < turn_at) & tail, local - half + small + rest, rel)
        idb[:, pl.ds(slot * rows_dev, rows_dev)] = jnp.broadcast_to(rel, (GROUP, rows_dev)) - lines

    def place(w):
        buf[mine, pl.ds(0, w)] = ends[x] if w == wide else piece(0, w)[...]

    sized(core, None, place)

    k1_at = pl.multiple_of(jnp.where(upper, depth - k1, 0), 256)
    k2_at = pl.multiple_of(jnp.where(upper, late, k1), 256)
    late_at = pl.multiple_of(jnp.where(upper, 0, depth - late), 256)
    starts = (k1_at, k2_at, late_at)

    def squares(i, c, w):
        w32 = buf[pl.ds(starts[i], 256), pl.ds(c, w)].astype(jnp.float32)
        return jnp.sum((w32 * w32).reshape(32, 8, w), 0)

    def turn(i, c, w):
        turned[i, pl.ds(c, w), :] = buf[pl.ds(starts[i], 256), pl.ds(c, w)].T

    def gather(i):
        for c in range(0, wide, 256):
            turn(i, c, min(256, wide - c))
        csq[...] = squares(i, 0, wide) + (csq[...] if i else 0.0)

    def flatten(*slots):
        for slot in slots:
            flat[:, pl.ds(slot * rows_dev, rows_dev)] = docs[slot].T

    def times(i, c, w, slot, count):
        return jnp.dot(turned[i, pl.ds(c, w), :],
                       flat[pl.ds(starts[i], 256), pl.ds(slot * rows_dev, count * rows_dev)],
                       preferred_element_type=jnp.float32)

    def begin(slot, count, *phases):
        where_docs = pl.ds(slot * rows_dev, count * rows_dev)

        def add(w):
            cut_at = w if count > 1 else w // 32 * 16
            for c, h in ((0, cut_at), (cut_at, w - cut_at)):
                if not h:
                    continue
                prod = times(phases[0], c, h, slot, count)
                for i in phases[1:]:
                    prod = prod + times(i, c, h, slot, count)
                if phases[0]:
                    acc[pl.ds(c, h), where_docs] += prod
                else:
                    acc[pl.ds(c, h), where_docs] = prod

        sized(core, None, add)

    spread(1)
    prepare_ids(0)
    flatten(0)
    spread(2)
    relay(0)
    spread(3)
    relay(1)
    have_docs(2, 0)
    send_docs(2, 6, 4, 0)
    share(2, 0)
    have_ids(4)
    send_ids(4, 6, 2)
    send_ids(4, 5, 1)
    have_ids(2)
    send_ids(2, 3, 1)
    relay(2)
    have_docs(4, 1)
    send_docs(4, 6, 2, 1)
    share(4, 1)
    have_docs(1, 0, 1, 2)
    flatten(1)
    relay(3)
    relay_far(0)
    have_docs(2, 1, 2)
    share(2, 1, 2)
    have_docs(4, 2)
    send_docs(4, 6, 2, 2)
    share(4, 2)
    have_ids(6)
    send_ids(6, 7, 1)
    relay_far(1)
    gather(0)
    begin(0, 2, 0)
    flatten(2)
    have_ids(1)
    for slot in (1, 2, 3, 4, 5, 6, 7):
        prepare_ids(slot)
    relay_far(2)
    have_docs(3, 0, 1, 2)
    flatten(3)
    begin(2, 2, 0)
    have_docs(4, 0)
    share(4, 0)
    flatten(4)
    relay_far(3)
    send_last(core == 0)
    gather(1)
    begin(0, 2, 1)
    begin(2, 2, 1)

    def share_far():
        for p in (1, 2, 0):
            have_docs(6, p)
            share(6, p)

    pl.when(core == 1)(share_far)
    have_docs(5, 0, 1, 2)
    flatten(5)
    begin(4, 2, 0, 1)
    send_last(core == 1)
    pl.when(core == 0)(share_far)
    flatten(6)
    begin(6, 1, 0, 1)

    def scales(c, w):
        total = jnp.sum(csq[:, pl.ds(c, w)] + squares(2, c, w), 0, keepdims=True)
        scale[pl.ds(c, w), :] = jnp.broadcast_to(lax.rsqrt(total + epsilon), (128, w)).T

    def stage(c0, w, slot, count):
        prod = times(2, c0, w, slot, count)
        spots = [pl.ds(slot * rows_dev + d, 128) for d in range(0, count * rows_dev, 128)]
        if c0:
            tops, hits = [mx[:, at] for at in spots], [ch[:, at] for at in spots]
        else:
            tops = [jnp.full((GROUP, 128), -3.0e38, jnp.float32)] * len(spots)
            hits = [jnp.zeros((GROUP, 128), jnp.float32)] * len(spots)
        for c in range(0, w, GROUP):
            rows = pl.ds(c0 + c, GROUP)
            by = scale[rows, :]
            for n, at in enumerate(spots):
                v = (acc[rows, at] + prod[c:c + GROUP, n * 128:n * 128 + 128]) * by
                hits[n] = jnp.where(idb[:, at] == c0 + c, v, hits[n])
                tops[n] = jnp.maximum(tops[n], v)
        for n, at in enumerate(spots):
            mx[:, at], ch[:, at] = tops[n], hits[n]

    def reduced(slot):
        at = pl.ds(slot * rows_dev, rows_dev)
        return jnp.max(mx[:, at], 0, keepdims=True), jnp.sum(ch[:, at], 0, keepdims=True)

    def give(slot):
        best, chosen = reduced(slot)
        res[slot, 0:1, :] = best
        res[slot, 1:2, :] = chosen
        remote(res.at[slot], got.at[slot], result_sent, r_recv, device(slot)).start()

    x32 = docs[0].astype(jnp.float32)
    sq = x32 * x32
    total = sq[:, 0:128]
    for c in range(128, depth, 128):
        total = total + sq[:, c:c + 128]
    scale_x = lax.rsqrt(jnp.sum(total.T, 0, keepdims=True) + epsilon)

    landed(z - 3 * out, 0, end)
    landed(z - 3 * out, 1, end)
    have_docs(7, 0, 1, 2)
    flatten(7)
    begin(7, 1, 0, 1)

    def advance(k, have):
        c, w = cuts[have][k], cuts[have][k + 1] - cuts[have][k]
        turn(2, c, w)
        scales(c, w)
        for slot in (6, 2, 4, 0):
            stage(c, w, slot, 2)
            if k == 2:
                give(slot + 1)
                if slot:
                    give(slot)

    for k in range(3):
        last_landed(k)
        sized(core, None, functools.partial(advance, k))
    best, chosen = reduced(0)
    everyone = pl.ds(1, 7)
    remote(got.at[everyone], got.at[everyone], result_sent, r_recv, device(1)).wait_recv()
    for slot in range(1, 8):
        best = jnp.maximum(best, got[slot, 0:1, :])
        chosen = chosen + got[slot, 1:2, :]
    near_out[...] = best * scale_x
    chosen_out[...] = chosen * scale_x

    def sent(ref, sem):
        remote(ref, ref, sem, r_recv, device(1)).wait_send()

    sent(res.at[everyone], result_sent)
    sent(docs.at[everyone], doc_sent)
    sent(ids.at[everyone], id_sent)
    layer = 4 * feat
    sized(core, inner, lambda w: sent(buf.at[pl.ds(0, 3 * layer), pl.ds(0, w)], outward))
    sized(core, inner, lambda w: sent(buf.at[pl.ds(0, 2 * layer), pl.ds(0, w)], inward))
    sized(core, end, lambda w: sent(buf.at[pl.ds(0, layer), pl.ds(0, w)], inward))
    for w, sem, two in ((wide, traded_wide, 0), (small, traded, 1)):
        pl.when(core == two)(lambda: sent(buf.at[pl.ds(0, 2 * feat), pl.ds(0, w)], sem))
        pl.when(core != two)(lambda: sent(buf.at[pl.ds(0, feat), pl.ds(0, w)], sem))


def by_layers(docs, centroids, assigned):
    nz = lax.axis_size("clu") // 4
    rows_dev, depth = docs.shape
    width, feat = centroids.shape
    wide = width // 512 * 128 + width // 2 % 128
    any_space = pl.BlockSpec(memory_space=pl.ANY)
    vmem = pl.BlockSpec(memory_space=pltpu.VMEM)
    dma = pltpu.SemaphoreType.DMA
    line = pltpu.VMEM((1, rows_dev), jnp.float32)
    near, chosen = pl.pallas_call(
        functools.partial(layer_kernel, nz, feat),
        out_shape=(line, line),
        in_specs=[any_space] * 3,
        out_specs=(vmem, vmem),
        scratch_shapes=[
            pltpu.VMEM((feat, width // 128 * 128), jnp.bfloat16),
            pltpu.VMEM((feat, width % 128), jnp.bfloat16),
            pltpu.VMEM((2, feat, wide), jnp.bfloat16),
            pltpu.VMEM((depth, wide), jnp.bfloat16),
            pltpu.VMEM((8, rows_dev, depth), jnp.bfloat16),
            pltpu.VMEM((depth, 8 * rows_dev), jnp.bfloat16),
            pltpu.VMEM((8, 1, rows_dev), jnp.int32),
            pltpu.VMEM((3, wide, 256), jnp.bfloat16),
            pltpu.VMEM((wide, 8 * rows_dev), jnp.float32),
            pltpu.VMEM((GROUP, 8 * rows_dev), jnp.int32),
            pltpu.VMEM((GROUP, 8 * rows_dev), jnp.float32),
            pltpu.VMEM((GROUP, 8 * rows_dev), jnp.float32),
            pltpu.VMEM((8, wide), jnp.float32),
            pltpu.VMEM((wide, 128), jnp.float32),
            pltpu.VMEM((8, 2, rows_dev), jnp.float32),
            pltpu.VMEM((8, 2, rows_dev), jnp.float32),
            dma((6,)), dma((7,)), dma((nz, 4)), dma((3,)), dma((12,)), dma((4,)), dma,
        ],
        compiler_params=pltpu.CompilerParams(collective_id=0, has_side_effects=True),
        name="layer_distances",
    )(docs, centroids.T, assigned.reshape(1, rows_dev))
    return 1.0 - near.reshape(rows_dev), 1.0 - chosen.reshape(rows_dev)


def fits_layers(docs, centroids):
    n_clu, feat = lax.axis_size("clu"), centroids.shape[1]
    width = centroids.shape[0]
    count, extra = width // 2 // 128, width // 2 % 128
    return (lax.axis_size("doc") == 2 and n_clu == 16 and feat % 16 == 0
            and width % 2 == 0 and count % 2 == 0 and count >= 10 and extra > 64 and extra % GROUP == 0
            and docs.shape[0] % 128 == 0 and docs.shape[1] == n_clu * feat == 3 * 256)


def on_device(docs, centroids, assigned):
    if fits_layers(docs, centroids):
        return by_layers(docs, centroids, assigned)
    n_clu, nd = lax.axis_size("clu"), lax.axis_size("doc")
    n = n_clu // 2
    rows_dev, depth = docs.shape
    width, feat = centroids.shape
    fp = (feat + 15) // 16 * 16
    cents = centroids.T
    if fp != feat:
        cents = jnp.pad(cents, ((0, fp - feat), (0, 0)))
    rows = nd * rows_dev
    any_space = pl.BlockSpec(memory_space=pl.ANY)
    vmem = pl.BlockSpec(memory_space=pltpu.VMEM)
    dma = pltpu.SemaphoreType.DMA
    hops = n // 2
    line = jax.ShapeDtypeStruct((1, rows_dev), jnp.float32)
    near, chosen = pl.pallas_call(
        functools.partial(kernel, n, nd, feat),
        out_shape=(line, line),
        in_specs=[any_space] * 3,
        out_specs=(vmem, vmem),
        scratch_shapes=[
            pltpu.VMEM((n_clu * fp, width), jnp.bfloat16),
            pltpu.VMEM((nd, rows_dev, depth), jnp.bfloat16),
            pltpu.VMEM((nd, 1, rows_dev), jnp.int32),
            pltpu.VMEM((rows, (n - 3) * 2 * fp), jnp.bfloat16),
            pltpu.VMEM((rows, 4 * fp), jnp.bfloat16),
            pltpu.VMEM((rows, 2 * fp), jnp.bfloat16),
            pltpu.VMEM((rows, width), jnp.float32),
            pltpu.VMEM((rows, 128), jnp.int32),
            pltpu.VMEM((rows, 128), jnp.float32),
            pltpu.VMEM((rows, 128), jnp.float32),
            pltpu.VMEM((8, width), jnp.float32),
            pltpu.VMEM((1, width), jnp.float32),
            pltpu.VMEM((nd, 2, rows_dev), jnp.float32),
            pltpu.VMEM((nd, 2, rows_dev), jnp.float32),
            dma((3,)),
            dma((2, hops, PIECES)),
            dma((n, PIECES)),
            dma((n, 2, PIECES)),
            dma((nd,)), dma((nd,)), dma((nd,)), dma((nd,)), dma((nd,)), dma((nd,)),
        ],
        compiler_params=pltpu.CompilerParams(collective_id=0, has_side_effects=True),
        name="ring_distances",
    )(docs, cents, assigned.reshape(1, rows_dev))
    return 1.0 - near.reshape(rows_dev), 1.0 - chosen.reshape(rows_dev)


def solution(mesh):
    placed = (P(("clu", "doc"), None), P("doc", "clu"), P(("clu", "doc")))
    return jax.shard_map(
        on_device,
        mesh=mesh,
        in_specs=placed,
        out_specs=(P(("clu", "doc")), P(("clu", "doc"))),
        check_vma=False,
    )
```

```python
import functools

import jax
import jax.numpy as jnp
from jax import lax
from jax.experimental import pallas as pl
from jax.experimental.pallas import tpu as pltpu
from jax.sharding import PartitionSpec as P

epsilon = 1e-06
PIECES = 4
ROWS = 64
GROUP = 16
MESH = pl.DeviceIdType.MESH


def chip_at(pos, n):
    half = n // 2
    return jnp.where(pos < half, 2 * pos, 2 * (n - 1 - pos) + 1)


def cut(width):
    tiles = (width + 127) // 128
    ends = [min(-(-tiles * (c + 1) // PIECES) * 128, width) for c in range(PIECES)]
    return tuple((a, b - a) for a, b in zip([0] + ends[:-1], ends))


def kernel(n, nd, feat, docs_in, cents_in, ids_in, near_out, chosen_out,
           buf, docs_all, ids_all, dp_a, dp_b, dp_c, acc, idb, mx, ch, csq, scale, res, got,
           local_sem, ring_send, pair_send, recv, docs_send, docs_recv, ids_send, ids_recv,
           res_send, res_recv):
    hops = n // 2
    fp = cents_in.shape[0]
    width = cents_in.shape[1]
    rows_dev = docs_in.shape[0]
    chunks = cut(width)
    half = len(chunks) // 2

    clu, doc = lax.axis_index("clu"), lax.axis_index("doc")
    core, chip = lax.rem(clu, 2), lax.div(clu, 2)
    z, x = lax.div(chip, 2), lax.rem(chip, 2)
    pos = jnp.where(x == 0, z, n - 1 - z)
    right = chip_at(lax.rem(pos + 1, n), n) * 2 + core
    left = chip_at(lax.rem(pos + n - 1, n), n) * 2 + core
    partner = chip * 2 + (1 - core)

    own_c = pltpu.make_async_copy(cents_in, buf.at[pl.ds(0, fp), :], local_sem.at[0])
    own_d = pltpu.make_async_copy(docs_in, docs_all.at[0], local_sem.at[1])
    own_i = pltpu.make_async_copy(ids_in, ids_all.at[0], local_sem.at[2])
    own_c.start()
    own_d.start()
    own_i.start()

    barrier = pltpu.get_barrier_semaphore()
    for peer in (left, right, partner):
        pl.semaphore_signal(barrier, inc=1, device_id={"clu": peer}, device_id_type=MESH)
    for k in range(1, nd):
        pl.semaphore_signal(barrier, inc=1, device_id={"doc": lax.rem(doc + k, nd)}, device_id_type=MESH)
    pl.semaphore_wait(barrier, 3 + nd - 1)

    def slot(way, h):
        if h == 0:
            return 0
        if h == hops:
            return n - 1
        return 2 * h - 1 if way == 0 else 2 * h

    def piece(s, m, c):
        return buf.at[pl.ds((2 * s + m) * fp, fp), pl.ds(*chunks[c])]

    def reach(way, c):
        return hops if way == c // half else hops - 1

    sent = []

    def ring(way, h, c):
        s, t = slot(way, h), slot(way, h + 1)
        copy = pltpu.make_async_remote_copy(
            src_ref=piece(s, 0, c), dst_ref=piece(t, 0, c),
            send_sem=ring_send.at[way, h, c], recv_sem=recv.at[t, 0, c],
            device_id={"clu": right if way == 0 else left}, device_id_type=MESH)
        copy.start()
        sent.append(copy)

    def share(s, c):
        copy = pltpu.make_async_remote_copy(
            src_ref=piece(s, 0, c), dst_ref=piece(s, 1, c),
            send_sem=pair_send.at[s, c], recv_sem=recv.at[s, 1, c],
            device_id={"clu": partner}, device_id_type=MESH)
        copy.start()
        sent.append(copy)

    def landed(s, m, c):
        pltpu.make_async_remote_copy(
            src_ref=piece(s, m, c), dst_ref=piece(s, m, c),
            send_sem=pair_send.at[s, c], recv_sem=recv.at[s, m, c],
            device_id={"clu": partner}, device_id_type=MESH).wait_recv()

    own_c.wait()
    for i in range(PIECES):
        ring(0, 0, i)
        ring(1, 0, (i + half) % PIECES)
    for c in range(PIECES):
        share(0, c)
    own_d.wait()
    own_i.wait()
    doc_copies = []
    for k in range(1, nd):
        mate = lax.rem(doc + k, nd)
        for ref, ss, rs in ((ids_all, ids_send, ids_recv), (docs_all, docs_send, docs_recv)):
            copy = pltpu.make_async_remote_copy(
                src_ref=ref.at[0], dst_ref=ref.at[k], send_sem=ss.at[k], recv_sem=rs.at[k],
                device_id={"doc": mate}, device_id_type=MESH)
            copy.start()
            doc_copies.append(copy)

    def owner(s):
        if s == 0:
            p = pos
        elif s == n - 1:
            p = pos + hops
        elif s % 2:
            p = pos + n - (s + 1) // 2
        else:
            p = pos + s // 2
        return chip_at(lax.rem(p, n), n)

    ranges = ((0, n - 3), (n - 3, n - 1), (n - 1, n))
    spread = (dp_a, dp_b, dp_c)

    def permute(k):
        rows = docs_all[k]
        for (first, last), out in zip(ranges, spread):
            wide = out.shape[1]
            lane = lax.broadcasted_iota(jnp.int32, (1, wide), 1)
            target = jnp.full((1, wide), -1, jnp.int32)
            for s in range(first, last):
                chip_s = owner(s)
                for m in (0, 1):
                    part = chip_s * 2 + (core if m == 0 else 1 - core)
                    start = (2 * (s - first) + m) * fp
                    inside = (lane >= start) & (lane < start + feat)
                    target = jnp.where(inside, lane - start + part * feat, target)
            source = lax.broadcasted_iota(jnp.int32, (rows.shape[1], wide), 0)
            mover = jnp.where(source == target, 1.0, 0.0).astype(jnp.bfloat16)
            out[pl.ds(k * rows_dev, rows_dev), :] = jnp.dot(
                rows, mover, preferred_element_type=jnp.float32).astype(jnp.bfloat16)

    def prepare_ids(k):
        base = doc * width
        ids = ids_all[k] - base
        ids = jnp.where((ids >= 0) & (ids < width), ids, -1)
        full = jnp.broadcast_to(ids, (128, rows_dev)).T
        lanes = lax.broadcasted_iota(jnp.int32, (rows_dev, 128), 1)
        idb[pl.ds(k * rows_dev, rows_dev), :] = jnp.where(full >= 0, full - lanes, -(2**20))

    def phase(index, c):
        first, last = ranges[index]
        start, depth = 2 * first * fp, 2 * (last - first) * fp
        cols = pl.ds(*chunks[c])
        block = buf[pl.ds(start, depth), cols]
        prod = jnp.dot(spread[index][...], block, preferred_element_type=jnp.float32)
        w32 = block.astype(jnp.float32)
        sq = jnp.sum((w32 * w32).reshape(depth // 8, 8, chunks[c][1]), 0)
        if index == 0:
            acc[:, cols] = prod
            csq[:, cols] = sq
        else:
            acc[:, cols] += prod
            csq[:, cols] += sq

    tail = pl.ds(2 * (n - 1) * fp, 2 * fp)

    def finish_scale(c):
        cols = pl.ds(*chunks[c])
        w32 = buf[tail, cols].astype(jnp.float32)
        sq = jnp.sum((w32 * w32).reshape(2 * fp // 8, 8, chunks[c][1]), 0) + csq[:, cols]
        scale[:, cols] = lax.rsqrt(jnp.sum(sq, 0, keepdims=True) + epsilon)

    def final(k, c):
        start, wide = chunks[c]
        prod = jnp.dot(dp_c[pl.ds(k * rows_dev, rows_dev), :], buf[tail, pl.ds(start, wide)],
                       preferred_element_type=jnp.float32)
        for r in range(0, rows_dev, ROWS):
            rs = pl.ds(k * rows_dev + r, ROWS)
            top, hit = mx[rs, :], ch[rs, :]
            ids = idb[rs, :]
            for a in range(0, wide, 128):
                w = min(128, wide - a)
                cols = pl.ds(start + a, w)
                v = (acc[rs, cols] + prod[r:r + ROWS, a:a + w]) * scale[:, cols]
                if w == 128:
                    top = jnp.maximum(top, v)
                    hit = jnp.where(ids == start + a, v, hit)
                else:
                    mx[rs, :] = top
                    ch[rs, :] = hit
                    mx[rs, pl.ds(0, w)] = jnp.maximum(mx[rs, pl.ds(0, w)], v)
                    ch[rs, pl.ds(0, w)] = jnp.where(idb[rs, pl.ds(0, w)] == start + a, v, ch[rs, pl.ds(0, w)])
            if wide % 128 == 0:
                mx[rs, :] = top
                ch[rs, :] = hit

    def reduced(k):
        rs = pl.ds(k * rows_dev, rows_dev)
        return (jnp.max(mx[rs, :].T, 0, keepdims=True), jnp.sum(ch[rs, :].T, 0, keepdims=True))

    mx[...] = jnp.full(mx.shape, -3.0e38, jnp.float32)
    ch[...] = jnp.zeros(ch.shape, jnp.float32)
    permute(0)
    prepare_ids(0)
    wide = docs_all[0].astype(jnp.float32)
    squares = wide * wide
    total = squares[:, 0:128]
    for a in range(128, wide.shape[1], 128):
        total = total + squares[:, a:a + 128]
    scale_x = lax.rsqrt(jnp.sum(total.T, 0, keepdims=True) + epsilon)

    def step(way, h, c):
        s = slot(way, h)
        landed(s, 0, c)
        if h < reach(way, c):
            ring(way, h, c)
        share(s, c)

    def pair(h, i):
        step(0, h, i)
        step(1, h, (i + half) % PIECES)

    def partners(slots, c):
        for s in slots:
            landed(s, 1, c)

    early, late = range(n - 3), (n - 3, n - 2)
    order = [j // 2 + half * (j % 2) for j in range(PIECES)]
    for h in range(1, hops):
        for i in range(PIECES):
            pair(h, i)
            if h == hops - 2 and i == half:
                for copy in doc_copies:
                    copy.wait()
                for k in range(1, nd):
                    permute(k)
                    prepare_ids(k)
            if h == hops - 1:
                c = order[i]
                partners(early, c)
                phase(0, c)
    for c in order[:half]:
        partners(late, c)
        phase(1, c)
    for i in range(half):
        for way in (0, 1):
            c = i + half * way
            landed(n - 1, 0, c)
            share(n - 1, c)
    for c in order[half:]:
        partners(late, c)
        phase(1, c)
    for c in order[:-2]:
        landed(n - 1, 1, c)
        finish_scale(c)
        for k in range(nd):
            final(k, c)
    for c in order[-2:]:
        landed(n - 1, 1, c)
        finish_scale(c)

    returns = []
    for k in range(1, nd):
        for c in order[-2:]:
            final(k, c)
        best, chosen = reduced(k)
        res[k, 0:1, :] = best
        res[k, 1:2, :] = chosen
        copy = pltpu.make_async_remote_copy(
            src_ref=res.at[k], dst_ref=got.at[k], send_sem=res_send.at[k], recv_sem=res_recv.at[k],
            device_id={"doc": lax.rem(doc + nd - k, nd)}, device_id_type=MESH)
        copy.start()
        returns.append(copy)
    for c in order[-2:]:
        final(0, c)
    best, chosen = reduced(0)
    for k in range(1, nd):
        returns[k - 1].wait()
        best = jnp.maximum(best, got[k, 0:1, :])
        chosen = chosen + got[k, 1:2, :]
    near_out[...] = best * scale_x
    chosen_out[...] = chosen * scale_x
    for copy in sent:
        copy.wait_send()


def layer_kernel(nz, feat, docs_in, cents_in, ids_in, near_out, chosen_out,
                 own, raw, ends, buf, docs, flat, ids, turned, acc, idb, mx, ch, csq, scale, res, got,
                 local_sem, send_sem, c_recv, last_recv, d_recv, i_recv, r_recv):
    width = cents_in.shape[1]
    rows_dev, depth = docs_in.shape
    half = width // 2
    count, extra = half // 128, half % 128
    small = count // 2 * 128
    wide = small + extra
    turn_at = (count + 1) * 128
    full = width // 128 * 128
    rest = width - full
    late = -(-4 * feat // 256) * 256
    k1 = 8 * feat // 256 * 256
    k2 = depth - late - k1
    a = rows_dev * 5 // 16 // 16 * 16
    b = (rows_dev - a) // 32 * 16
    spans = ((0, a), (a, b), (a + b, rows_dev - a - b))
    cuts = {w: (0, 256, (w - 1) // 256 * 256, w) for w in (small, wide)}

    clu, doc = lax.axis_index("clu"), lax.axis_index("doc")
    core, chip = lax.rem(clu, 2), lax.div(clu, 2)
    z, x = lax.div(chip, 2), lax.rem(chip, 2)
    upper = z >= nz // 2
    out = jnp.where(upper, 1, -1)
    end = (z == 0) | (z == nz - 1)
    inner = jnp.logical_not(end)

    def device(r, dz=0):
        dx, dy, dc = r // 4, r // 2 % 2, r % 2
        there = ((z + dz) * 2 + (1 - x if dx else x)) * 2 + (1 - core if dc else core)
        return {"clu": there, "doc": 1 - doc if dy else doc}

    def when(cond, body):
        if cond is None:
            body()
        else:
            pl.when(cond)(body)

    def both(p, q):
        return q if p is None else p if q is None else p & q

    def sized(c, cond, body):
        for value, w in ((1, wide), (0, small)):
            when(both(cond, c == value), functools.partial(body, w))

    own_copy = pltpu.make_async_copy(cents_in.at[:, pl.ds(0, full)], own.at[:, pl.ds(0, full)], local_sem.at[0])
    docs_copy = pltpu.make_async_copy(docs_in, docs.at[0], local_sem.at[1])
    ids_copy = pltpu.make_async_copy(ids_in, ids.at[0], local_sem.at[2])
    own_copy.start()
    raw_copy = pltpu.make_async_copy(cents_in.at[:, pl.ds(full, rest)], raw, local_sem.at[3])
    raw_copy.start()
    end_copies = [pltpu.make_async_copy(cents_in.at[:, pl.ds(k * turn_at + small, small)],
                                        ends.at[k, :, pl.ds(0, small)], local_sem.at[4 + k]) for k in (0, 1)]
    for copy in end_copies:
        copy.start()
    docs_copy.start()
    ids_copy.start()

    barrier = pltpu.get_barrier_semaphore()

    def greet(to):
        pl.semaphore_signal(barrier, inc=1, device_id=to, device_id_type=MESH)

    pl.when(inner)(lambda: greet(device(0, out)))
    greet(device(0, -out))
    for r in (4, 5, 2, 1):
        greet(device(r))

    @pl.when(core == 0)
    def _():
        buf[:, pl.ds(small, extra)] = jnp.zeros((buf.shape[0], extra), buf.dtype)

    own_copy.wait()
    raw_copy.wait()
    middle = own[:, pl.ds(turn_at - 128, 128)]
    ends[0, :, pl.ds(small, extra)] = middle[:, 0:extra]
    ends[1, :, pl.ds(small, extra)] = jnp.concatenate([raw[...], middle[:, extra:128]], axis=1)
    for copy in end_copies:
        copy.wait()
    docs_copy.wait()
    ids_copy.wait()
    pl.semaphore_wait(barrier, 5 + inner.astype(jnp.int32))

    outward, inward, doc_sent, id_sent, result_sent, traded, traded_wide = (send_sem.at[i] for i in range(7))

    def start(make, cond=None):
        when(cond, lambda: make().start())

    def start_sized(make, c, cond=None):
        sized(c, cond, lambda w: make(w).start())

    def remote(src, dst, ss, rs, to):
        return pltpu.make_async_remote_copy(
            src_ref=src, dst_ref=dst, send_sem=ss, recv_sem=rs, device_id=to, device_id_type=MESH)

    near = (0, 1, 4, 5)

    def source(layer, j):
        r = near[j]
        there = (layer * 2 + (1 - x if r // 4 else x)) * 2 + (1 - core if r % 2 else core)
        return pl.ds(pl.multiple_of(there * feat, 16), feat)

    def piece(r, w):
        xd = 1 - x if r // 4 else x
        if w == wide:
            return ends.at[xd]
        return own.at[:, pl.ds(pl.multiple_of(xd * turn_at, 128), w)]

    mine = source(z, 0)

    def exchange(j):
        r = near[j]
        start_sized(lambda w: remote(piece(r, w), buf.at[mine, pl.ds(0, w)],
                                     traded_wide if w == wide else traded, c_recv.at[z, j], device(r)),
                    1 - core if r % 2 else core)

    def landed(layer, j, cond=None):
        rows = source(layer, j)
        sized(core, cond, lambda w: remote(
            buf.at[rows, pl.ds(0, w)], buf.at[rows, pl.ds(0, w)], traded, c_recv.at[layer, j],
            device(1)).wait_recv())

    def carry(layer, j, way, s, cond=None):
        rows = source(layer, j)
        src = (lambda w: piece(0, w)) if s == 0 and j == 0 else (lambda w: buf.at[rows, pl.ds(0, w)])
        start_sized(lambda w: remote(src(w), buf.at[rows, pl.ds(0, w)], inward if way else outward,
                                     c_recv.at[layer, j], device(0, -out if way else out)), core, cond)

    def spread(j):
        if j:
            landed(z, j)
        carry(z, j, 0, 0, inner)
        carry(z, j, 1, 0)

    def relay(j):
        landed(z - out, j)
        carry(z - out, j, 0, 1, inner)
        landed(z + out, j, inner)
        carry(z + out, j, 1, 1, inner)

    def pair(layer, k, w):
        rows = pl.ds(pl.multiple_of((layer * 2 + 1 - x) * 2 * feat, 16), 2 * feat)
        return buf.at[rows, pl.ds(cuts[w][k], cuts[w][k + 1] - cuts[w][k])]

    def relay_far(j):
        landed(z - 2 * out, j)
        if j < 2:
            carry(z - 2 * out, j, 0, 2, inner)

    def send_last(cond):
        for k in range(3):
            start_sized(lambda w, k=k: remote(
                pair(z - 2 * out, k, w), pair(z - 2 * out, k, w), outward, last_recv.at[k],
                device(0, out)), core, inner & cond)

    def last_landed(k):
        sized(core, end, lambda w: remote(
            pair(z - 3 * out, k, w), pair(z - 3 * out, k, w), outward, last_recv.at[k],
            device(1)).wait_recv())

    ahead = {(1, 0): 0, (1, 1): 0, (1, 2): 0, (3, 0): 1, (3, 1): 1, (3, 2): 1, (5, 0): 2, (5, 1): 2, (5, 2): 2,
             (7, 0): 3, (7, 1): 3, (7, 2): 3, (2, 0): 4, (2, 1): 5, (2, 2): 5, (4, 0): 6, (4, 1): 7, (4, 2): 8,
             (6, 0): 9, (6, 1): 10, (6, 2): 11}
    id_at = {1: 0, 3: 0, 5: 0, 7: 0, 2: 1, 4: 2, 6: 3}

    def part(slot, *parts):
        first, last = spans[parts[0]], spans[parts[-1]]
        return docs.at[slot, pl.ds(first[0], last[0] + last[1] - first[0]), :]

    def send_docs(src_slot, dst_slot, r, *parts):
        start(lambda: remote(part(src_slot, *parts), part(dst_slot, *parts), doc_sent,
                             d_recv.at[ahead[dst_slot, parts[0]]], device(r)))

    def send_ids(src_slot, dst_slot, r):
        start(lambda: remote(ids.at[src_slot], ids.at[dst_slot], id_sent, i_recv.at[id_at[dst_slot]], device(r)))

    def have_docs(slot, *parts):
        remote(part(slot, *parts), part(slot, *parts), doc_sent, d_recv.at[ahead[slot, parts[0]]],
               device(1)).wait_recv()

    def have_ids(slot):
        some = ids.at[pl.ds(0, 4)] if slot % 2 else ids.at[slot]
        remote(some, some, id_sent, i_recv.at[id_at[slot]], device(1)).wait_recv()

    def share(slot, *parts):
        send_docs(slot, slot + 1, 1, *parts)

    spread(0)
    for j in (1, 2, 3):
        exchange(j)
    send_ids(0, 2, 2)
    send_docs(0, 2, 2, 0)
    send_docs(0, 2, 2, 1, 2)
    send_ids(0, 1, 1)
    send_docs(0, 1, 1, 0, 1, 2)

    first = x * turn_at + core * small
    reach = small + jnp.where(core == 0, 0, jnp.where(x == 0, extra, rest))
    tail = (core == 1) & (x == 1)
    lines = lax.broadcasted_iota(jnp.int32, (GROUP, rows_dev), 0)

    def prepare_ids(slot):
        local = ids[slot] - doc * width
        rel = jnp.where((local >= first) & (local < first + reach), local - first, -(2**20))
        rel = jnp.where((local >= half) & (local < turn_at) & tail, local - half + small + rest, rel)
        idb[:, pl.ds(slot * rows_dev, rows_dev)] = jnp.broadcast_to(rel, (GROUP, rows_dev)) - lines

    def place(w):
        buf[mine, pl.ds(0, w)] = ends[x] if w == wide else piece(0, w)[...]

    sized(core, None, place)

    k1_at = pl.multiple_of(jnp.where(upper, depth - k1, 0), 256)
    k2_at = pl.multiple_of(jnp.where(upper, late, k1), 256)
    late_at = pl.multiple_of(jnp.where(upper, 0, depth - late), 256)
    starts = (k1_at, k2_at, late_at)

    def squares(i, c, w):
        w32 = buf[pl.ds(starts[i], 256), pl.ds(c, w)].astype(jnp.float32)
        return jnp.sum((w32 * w32).reshape(32, 8, w), 0)

    def turn(i, c, w):
        turned[i, pl.ds(c, w), :] = buf[pl.ds(starts[i], 256), pl.ds(c, w)].T

    def gather(i):
        for c in range(0, wide, 256):
            turn(i, c, min(256, wide - c))
        csq[...] = squares(i, 0, wide) + (csq[...] if i else 0.0)

    def flatten(*slots):
        for slot in slots:
            flat[:, pl.ds(slot * rows_dev, rows_dev)] = docs[slot].T

    def times(i, c, w, slot, count):
        return jnp.dot(turned[i, pl.ds(c, w), :],
                       flat[pl.ds(starts[i], 256), pl.ds(slot * rows_dev, count * rows_dev)],
                       preferred_element_type=jnp.float32)

    def begin(slot, count, *phases):
        where_docs = pl.ds(slot * rows_dev, count * rows_dev)

        def add(w):
            cut_at = w if count > 1 else w // 32 * 16
            for c, h in ((0, cut_at), (cut_at, w - cut_at)):
                if not h:
                    continue
                prod = times(phases[0], c, h, slot, count)
                for i in phases[1:]:
                    prod = prod + times(i, c, h, slot, count)
                if phases[0]:
                    acc[pl.ds(c, h), where_docs] += prod
                else:
                    acc[pl.ds(c, h), where_docs] = prod

        sized(core, None, add)

    def cross_docs():
        send_ids(0, 4, 4)
        for p in (1, 2, 0):
            send_docs(0, 4, 4, p)

    spread(1)
    pl.when(core == 0)(cross_docs)
    prepare_ids(0)
    flatten(0)
    spread(2)
    pl.when(core == 1)(cross_docs)
    relay(0)
    spread(3)
    relay(1)
    have_docs(2, 0)
    send_docs(2, 6, 4, 0)
    share(2, 0)
    have_ids(4)
    send_ids(4, 6, 2)
    send_ids(4, 5, 1)
    have_ids(2)
    send_ids(2, 3, 1)
    relay(2)
    have_docs(4, 1)
    send_docs(4, 6, 2, 1)
    share(4, 1)
    have_docs(1, 0, 1, 2)
    flatten(1)
    relay(3)
    relay_far(0)
    have_docs(4, 2)
    send_docs(4, 6, 2, 2)
    share(4, 2)
    have_docs(2, 1, 2)
    share(2, 1, 2)
    have_ids(6)
    send_ids(6, 7, 1)
    relay_far(1)
    gather(0)
    begin(0, 2, 0)
    flatten(2)
    have_ids(1)
    for slot in (1, 2, 3, 4, 5, 6, 7):
        prepare_ids(slot)
    relay_far(2)
    have_docs(3, 0, 1, 2)
    flatten(3)
    begin(2, 2, 0)
    have_docs(4, 0)
    share(4, 0)
    flatten(4)
    relay_far(3)
    send_last(core == 0)
    gather(1)
    begin(0, 2, 1)
    begin(2, 2, 1)

    def share_far():
        for p in (1, 2, 0):
            have_docs(6, p)
            share(6, p)

    have_docs(5, 0, 1, 2)
    flatten(5)
    pl.when(core == 0)(share_far)
    begin(4, 2, 0, 1)
    send_last(core == 1)
    pl.when(core == 1)(share_far)
    flatten(6)
    begin(6, 1, 0, 1)

    def scales(c, w):
        total = jnp.sum(csq[:, pl.ds(c, w)] + squares(2, c, w), 0, keepdims=True)
        scale[pl.ds(c, w), :] = jnp.broadcast_to(lax.rsqrt(total + epsilon), (128, w)).T

    def stage(c0, w, slot, count):
        prod = times(2, c0, w, slot, count)
        spots = [pl.ds(slot * rows_dev + d, 128) for d in range(0, count * rows_dev, 128)]
        if c0:
            tops, hits = [mx[:, at] for at in spots], [ch[:, at] for at in spots]
        else:
            tops = [jnp.full((GROUP, 128), -3.0e38, jnp.float32)] * len(spots)
            hits = [jnp.zeros((GROUP, 128), jnp.float32)] * len(spots)
        for c in range(0, w, GROUP):
            rows = pl.ds(c0 + c, GROUP)
            by = scale[rows, :]
            for n, at in enumerate(spots):
                v = (acc[rows, at] + prod[c:c + GROUP, n * 128:n * 128 + 128]) * by
                hits[n] = jnp.where(idb[:, at] == c0 + c, v, hits[n])
                tops[n] = jnp.maximum(tops[n], v)
        for n, at in enumerate(spots):
            mx[:, at], ch[:, at] = tops[n], hits[n]

    def reduced(slot):
        at = pl.ds(slot * rows_dev, rows_dev)
        return jnp.max(mx[:, at], 0, keepdims=True), jnp.sum(ch[:, at], 0, keepdims=True)

    def give(slot):
        best, chosen = reduced(slot)
        res[slot, 0:1, :] = best
        res[slot, 1:2, :] = chosen
        remote(res.at[slot], got.at[slot], result_sent, r_recv, device(slot)).start()

    x32 = docs[0].astype(jnp.float32)
    sq = x32 * x32
    total = sq[:, 0:128]
    for c in range(128, depth, 128):
        total = total + sq[:, c:c + 128]
    scale_x = lax.rsqrt(jnp.sum(total.T, 0, keepdims=True) + epsilon)

    landed(z - 3 * out, 0, end)
    landed(z - 3 * out, 1, end)
    have_docs(7, 0, 1, 2)
    flatten(7)
    begin(7, 1, 0, 1)

    def advance(k, have):
        c, w = cuts[have][k], cuts[have][k + 1] - cuts[have][k]
        turn(2, c, w)
        scales(c, w)
        for slot in (6, 2, 4, 0):
            stage(c, w, slot, 2)
            if k == 2:
                give(slot + 1)
                if slot:
                    give(slot)

    for k in range(3):
        last_landed(k)
        sized(core, None, functools.partial(advance, k))
    best, chosen = reduced(0)
    everyone = pl.ds(1, 7)
    remote(got.at[everyone], got.at[everyone], result_sent, r_recv, device(1)).wait_recv()
    for slot in range(1, 8):
        best = jnp.maximum(best, got[slot, 0:1, :])
        chosen = chosen + got[slot, 1:2, :]
    near_out[...] = best * scale_x
    chosen_out[...] = chosen * scale_x

    def sent(ref, sem):
        remote(ref, ref, sem, r_recv, device(1)).wait_send()

    sent(res.at[everyone], result_sent)
    sent(docs.at[everyone], doc_sent)
    sent(ids.at[everyone], id_sent)
    layer = 4 * feat
    sized(core, inner, lambda w: sent(buf.at[pl.ds(0, 3 * layer), pl.ds(0, w)], outward))
    sized(core, inner, lambda w: sent(buf.at[pl.ds(0, 2 * layer), pl.ds(0, w)], inward))
    sized(core, end, lambda w: sent(buf.at[pl.ds(0, layer), pl.ds(0, w)], inward))
    for w, sem, two in ((wide, traded_wide, 0), (small, traded, 1)):
        pl.when(core == two)(lambda: sent(buf.at[pl.ds(0, 2 * feat), pl.ds(0, w)], sem))
        pl.when(core != two)(lambda: sent(buf.at[pl.ds(0, feat), pl.ds(0, w)], sem))


def by_layers(docs, centroids, assigned):
    nz = lax.axis_size("clu") // 4
    rows_dev, depth = docs.shape
    width, feat = centroids.shape
    wide = width // 512 * 128 + width // 2 % 128
    any_space = pl.BlockSpec(memory_space=pl.ANY)
    vmem = pl.BlockSpec(memory_space=pltpu.VMEM)
    dma = pltpu.SemaphoreType.DMA
    line = pltpu.VMEM((1, rows_dev), jnp.float32)
    near, chosen = pl.pallas_call(
        functools.partial(layer_kernel, nz, feat),
        out_shape=(line, line),
        in_specs=[any_space] * 3,
        out_specs=(vmem, vmem),
        scratch_shapes=[
            pltpu.VMEM((feat, width // 128 * 128), jnp.bfloat16),
            pltpu.VMEM((feat, width % 128), jnp.bfloat16),
            pltpu.VMEM((2, feat, wide), jnp.bfloat16),
            pltpu.VMEM((depth, wide), jnp.bfloat16),
            pltpu.VMEM((8, rows_dev, depth), jnp.bfloat16),
            pltpu.VMEM((depth, 8 * rows_dev), jnp.bfloat16),
            pltpu.VMEM((8, 1, rows_dev), jnp.int32),
            pltpu.VMEM((3, wide, 256), jnp.bfloat16),
            pltpu.VMEM((wide, 8 * rows_dev), jnp.float32),
            pltpu.VMEM((GROUP, 8 * rows_dev), jnp.int32),
            pltpu.VMEM((GROUP, 8 * rows_dev), jnp.float32),
            pltpu.VMEM((GROUP, 8 * rows_dev), jnp.float32),
            pltpu.VMEM((8, wide), jnp.float32),
            pltpu.VMEM((wide, 128), jnp.float32),
            pltpu.VMEM((8, 2, rows_dev), jnp.float32),
            pltpu.VMEM((8, 2, rows_dev), jnp.float32),
            dma((6,)), dma((7,)), dma((nz, 4)), dma((3,)), dma((12,)), dma((4,)), dma,
        ],
        compiler_params=pltpu.CompilerParams(collective_id=0, has_side_effects=True),
        name="layer_distances",
    )(docs, centroids.T, assigned.reshape(1, rows_dev))
    return 1.0 - near.reshape(rows_dev), 1.0 - chosen.reshape(rows_dev)


def fits_layers(docs, centroids):
    n_clu, feat = lax.axis_size("clu"), centroids.shape[1]
    width = centroids.shape[0]
    count, extra = width // 2 // 128, width // 2 % 128
    return (lax.axis_size("doc") == 2 and n_clu == 16 and feat % 16 == 0
            and width % 2 == 0 and count % 2 == 0 and count >= 10 and extra > 64 and extra % GROUP == 0
            and docs.shape[0] % 128 == 0 and docs.shape[1] == n_clu * feat == 3 * 256)


def on_device(docs, centroids, assigned):
    if fits_layers(docs, centroids):
        return by_layers(docs, centroids, assigned)
    n_clu, nd = lax.axis_size("clu"), lax.axis_size("doc")
    n = n_clu // 2
    rows_dev, depth = docs.shape
    width, feat = centroids.shape
    fp = (feat + 15) // 16 * 16
    cents = centroids.T
    if fp != feat:
        cents = jnp.pad(cents, ((0, fp - feat), (0, 0)))
    rows = nd * rows_dev
    any_space = pl.BlockSpec(memory_space=pl.ANY)
    vmem = pl.BlockSpec(memory_space=pltpu.VMEM)
    dma = pltpu.SemaphoreType.DMA
    hops = n // 2
    line = jax.ShapeDtypeStruct((1, rows_dev), jnp.float32)
    near, chosen = pl.pallas_call(
        functools.partial(kernel, n, nd, feat),
        out_shape=(line, line),
        in_specs=[any_space] * 3,
        out_specs=(vmem, vmem),
        scratch_shapes=[
            pltpu.VMEM((n_clu * fp, width), jnp.bfloat16),
            pltpu.VMEM((nd, rows_dev, depth), jnp.bfloat16),
            pltpu.VMEM((nd, 1, rows_dev), jnp.int32),
            pltpu.VMEM((rows, (n - 3) * 2 * fp), jnp.bfloat16),
            pltpu.VMEM((rows, 4 * fp), jnp.bfloat16),
            pltpu.VMEM((rows, 2 * fp), jnp.bfloat16),
            pltpu.VMEM((rows, width), jnp.float32),
            pltpu.VMEM((rows, 128), jnp.int32),
            pltpu.VMEM((rows, 128), jnp.float32),
            pltpu.VMEM((rows, 128), jnp.float32),
            pltpu.VMEM((8, width), jnp.float32),
            pltpu.VMEM((1, width), jnp.float32),
            pltpu.VMEM((nd, 2, rows_dev), jnp.float32),
            pltpu.VMEM((nd, 2, rows_dev), jnp.float32),
            dma((3,)),
            dma((2, hops, PIECES)),
            dma((n, PIECES)),
            dma((n, 2, PIECES)),
            dma((nd,)), dma((nd,)), dma((nd,)), dma((nd,)), dma((nd,)), dma((nd,)),
        ],
        compiler_params=pltpu.CompilerParams(collective_id=0, has_side_effects=True),
        name="ring_distances",
    )(docs, cents, assigned.reshape(1, rows_dev))
    return 1.0 - near.reshape(rows_dev), 1.0 - chosen.reshape(rows_dev)


def solution(mesh):
    placed = (P(("clu", "doc"), None), P("doc", "clu"), P(("clu", "doc")))
    return jax.shard_map(
        on_device,
        mesh=mesh,
        in_specs=placed,
        out_specs=(P(("clu", "doc")), P(("clu", "doc"))),
        check_vma=False,
    )
```

```python
import functools

import jax
import jax.numpy as jnp
from jax import lax
from jax.experimental import pallas as pl
from jax.experimental.pallas import tpu as pltpu
from jax.sharding import PartitionSpec as P

epsilon = 1e-06
PIECES = 4
ROWS = 64
GROUP = 16
MESH = pl.DeviceIdType.MESH


def chip_at(pos, n):
    half = n // 2
    return jnp.where(pos < half, 2 * pos, 2 * (n - 1 - pos) + 1)


def cut(width):
    tiles = (width + 127) // 128
    ends = [min(-(-tiles * (c + 1) // PIECES) * 128, width) for c in range(PIECES)]
    return tuple((a, b - a) for a, b in zip([0] + ends[:-1], ends))


def kernel(n, nd, feat, docs_in, cents_in, ids_in, near_out, chosen_out,
           buf, docs_all, ids_all, dp_a, dp_b, dp_c, acc, idb, mx, ch, csq, scale, res, got,
           local_sem, ring_send, pair_send, recv, docs_send, docs_recv, ids_send, ids_recv,
           res_send, res_recv):
    hops = n // 2
    fp = cents_in.shape[0]
    width = cents_in.shape[1]
    rows_dev = docs_in.shape[0]
    chunks = cut(width)
    half = len(chunks) // 2

    clu, doc = lax.axis_index("clu"), lax.axis_index("doc")
    core, chip = lax.rem(clu, 2), lax.div(clu, 2)
    z, x = lax.div(chip, 2), lax.rem(chip, 2)
    pos = jnp.where(x == 0, z, n - 1 - z)
    right = chip_at(lax.rem(pos + 1, n), n) * 2 + core
    left = chip_at(lax.rem(pos + n - 1, n), n) * 2 + core
    partner = chip * 2 + (1 - core)

    own_c = pltpu.make_async_copy(cents_in, buf.at[pl.ds(0, fp), :], local_sem.at[0])
    own_d = pltpu.make_async_copy(docs_in, docs_all.at[0], local_sem.at[1])
    own_i = pltpu.make_async_copy(ids_in, ids_all.at[0], local_sem.at[2])
    own_c.start()
    own_d.start()
    own_i.start()

    barrier = pltpu.get_barrier_semaphore()
    for peer in (left, right, partner):
        pl.semaphore_signal(barrier, inc=1, device_id={"clu": peer}, device_id_type=MESH)
    for k in range(1, nd):
        pl.semaphore_signal(barrier, inc=1, device_id={"doc": lax.rem(doc + k, nd)}, device_id_type=MESH)
    pl.semaphore_wait(barrier, 3 + nd - 1)

    def slot(way, h):
        if h == 0:
            return 0
        if h == hops:
            return n - 1
        return 2 * h - 1 if way == 0 else 2 * h

    def piece(s, m, c):
        return buf.at[pl.ds((2 * s + m) * fp, fp), pl.ds(*chunks[c])]

    def reach(way, c):
        return hops if way == c // half else hops - 1

    sent = []

    def ring(way, h, c):
        s, t = slot(way, h), slot(way, h + 1)
        copy = pltpu.make_async_remote_copy(
            src_ref=piece(s, 0, c), dst_ref=piece(t, 0, c),
            send_sem=ring_send.at[way, h, c], recv_sem=recv.at[t, 0, c],
            device_id={"clu": right if way == 0 else left}, device_id_type=MESH)
        copy.start()
        sent.append(copy)

    def share(s, c):
        copy = pltpu.make_async_remote_copy(
            src_ref=piece(s, 0, c), dst_ref=piece(s, 1, c),
            send_sem=pair_send.at[s, c], recv_sem=recv.at[s, 1, c],
            device_id={"clu": partner}, device_id_type=MESH)
        copy.start()
        sent.append(copy)

    def landed(s, m, c):
        pltpu.make_async_remote_copy(
            src_ref=piece(s, m, c), dst_ref=piece(s, m, c),
            send_sem=pair_send.at[s, c], recv_sem=recv.at[s, m, c],
            device_id={"clu": partner}, device_id_type=MESH).wait_recv()

    own_c.wait()
    for i in range(PIECES):
        ring(0, 0, i)
        ring(1, 0, (i + half) % PIECES)
    for c in range(PIECES):
        share(0, c)
    own_d.wait()
    own_i.wait()
    doc_copies = []
    for k in range(1, nd):
        mate = lax.rem(doc + k, nd)
        for ref, ss, rs in ((ids_all, ids_send, ids_recv), (docs_all, docs_send, docs_recv)):
            copy = pltpu.make_async_remote_copy(
                src_ref=ref.at[0], dst_ref=ref.at[k], send_sem=ss.at[k], recv_sem=rs.at[k],
                device_id={"doc": mate}, device_id_type=MESH)
            copy.start()
            doc_copies.append(copy)

    def owner(s):
        if s == 0:
            p = pos
        elif s == n - 1:
            p = pos + hops
        elif s % 2:
            p = pos + n - (s + 1) // 2
        else:
            p = pos + s // 2
        return chip_at(lax.rem(p, n), n)

    ranges = ((0, n - 3), (n - 3, n - 1), (n - 1, n))
    spread = (dp_a, dp_b, dp_c)

    def permute(k):
        rows = docs_all[k]
        for (first, last), out in zip(ranges, spread):
            wide = out.shape[1]
            lane = lax.broadcasted_iota(jnp.int32, (1, wide), 1)
            target = jnp.full((1, wide), -1, jnp.int32)
            for s in range(first, last):
                chip_s = owner(s)
                for m in (0, 1):
                    part = chip_s * 2 + (core if m == 0 else 1 - core)
                    start = (2 * (s - first) + m) * fp
                    inside = (lane >= start) & (lane < start + feat)
                    target = jnp.where(inside, lane - start + part * feat, target)
            source = lax.broadcasted_iota(jnp.int32, (rows.shape[1], wide), 0)
            mover = jnp.where(source == target, 1.0, 0.0).astype(jnp.bfloat16)
            out[pl.ds(k * rows_dev, rows_dev), :] = jnp.dot(
                rows, mover, preferred_element_type=jnp.float32).astype(jnp.bfloat16)

    def prepare_ids(k):
        base = doc * width
        ids = ids_all[k] - base
        ids = jnp.where((ids >= 0) & (ids < width), ids, -1)
        full = jnp.broadcast_to(ids, (128, rows_dev)).T
        lanes = lax.broadcasted_iota(jnp.int32, (rows_dev, 128), 1)
        idb[pl.ds(k * rows_dev, rows_dev), :] = jnp.where(full >= 0, full - lanes, -(2**20))

    def phase(index, c):
        first, last = ranges[index]
        start, depth = 2 * first * fp, 2 * (last - first) * fp
        cols = pl.ds(*chunks[c])
        block = buf[pl.ds(start, depth), cols]
        prod = jnp.dot(spread[index][...], block, preferred_element_type=jnp.float32)
        w32 = block.astype(jnp.float32)
        sq = jnp.sum((w32 * w32).reshape(depth // 8, 8, chunks[c][1]), 0)
        if index == 0:
            acc[:, cols] = prod
            csq[:, cols] = sq
        else:
            acc[:, cols] += prod
            csq[:, cols] += sq

    tail = pl.ds(2 * (n - 1) * fp, 2 * fp)

    def finish_scale(c):
        cols = pl.ds(*chunks[c])
        w32 = buf[tail, cols].astype(jnp.float32)
        sq = jnp.sum((w32 * w32).reshape(2 * fp // 8, 8, chunks[c][1]), 0) + csq[:, cols]
        scale[:, cols] = lax.rsqrt(jnp.sum(sq, 0, keepdims=True) + epsilon)

    def final(k, c):
        start, wide = chunks[c]
        prod = jnp.dot(dp_c[pl.ds(k * rows_dev, rows_dev), :], buf[tail, pl.ds(start, wide)],
                       preferred_element_type=jnp.float32)
        for r in range(0, rows_dev, ROWS):
            rs = pl.ds(k * rows_dev + r, ROWS)
            top, hit = mx[rs, :], ch[rs, :]
            ids = idb[rs, :]
            for a in range(0, wide, 128):
                w = min(128, wide - a)
                cols = pl.ds(start + a, w)
                v = (acc[rs, cols] + prod[r:r + ROWS, a:a + w]) * scale[:, cols]
                if w == 128:
                    top = jnp.maximum(top, v)
                    hit = jnp.where(ids == start + a, v, hit)
                else:
                    mx[rs, :] = top
                    ch[rs, :] = hit
                    mx[rs, pl.ds(0, w)] = jnp.maximum(mx[rs, pl.ds(0, w)], v)
                    ch[rs, pl.ds(0, w)] = jnp.where(idb[rs, pl.ds(0, w)] == start + a, v, ch[rs, pl.ds(0, w)])
            if wide % 128 == 0:
                mx[rs, :] = top
                ch[rs, :] = hit

    def reduced(k):
        rs = pl.ds(k * rows_dev, rows_dev)
        return (jnp.max(mx[rs, :].T, 0, keepdims=True), jnp.sum(ch[rs, :].T, 0, keepdims=True))

    mx[...] = jnp.full(mx.shape, -3.0e38, jnp.float32)
    ch[...] = jnp.zeros(ch.shape, jnp.float32)
    permute(0)
    prepare_ids(0)
    wide = docs_all[0].astype(jnp.float32)
    squares = wide * wide
    total = squares[:, 0:128]
    for a in range(128, wide.shape[1], 128):
        total = total + squares[:, a:a + 128]
    scale_x = lax.rsqrt(jnp.sum(total.T, 0, keepdims=True) + epsilon)

    def step(way, h, c):
        s = slot(way, h)
        landed(s, 0, c)
        if h < reach(way, c):
            ring(way, h, c)
        share(s, c)

    def pair(h, i):
        step(0, h, i)
        step(1, h, (i + half) % PIECES)

    def partners(slots, c):
        for s in slots:
            landed(s, 1, c)

    early, late = range(n - 3), (n - 3, n - 2)
    order = [j // 2 + half * (j % 2) for j in range(PIECES)]
    for h in range(1, hops):
        for i in range(PIECES):
            pair(h, i)
            if h == hops - 2 and i == half:
                for copy in doc_copies:
                    copy.wait()
                for k in range(1, nd):
                    permute(k)
                    prepare_ids(k)
            if h == hops - 1:
                c = order[i]
                partners(early, c)
                phase(0, c)
    for c in order[:half]:
        partners(late, c)
        phase(1, c)
    for i in range(half):
        for way in (0, 1):
            c = i + half * way
            landed(n - 1, 0, c)
            share(n - 1, c)
    for c in order[half:]:
        partners(late, c)
        phase(1, c)
    for c in order[:-2]:
        landed(n - 1, 1, c)
        finish_scale(c)
        for k in range(nd):
            final(k, c)
    for c in order[-2:]:
        landed(n - 1, 1, c)
        finish_scale(c)

    returns = []
    for k in range(1, nd):
        for c in order[-2:]:
            final(k, c)
        best, chosen = reduced(k)
        res[k, 0:1, :] = best
        res[k, 1:2, :] = chosen
        copy = pltpu.make_async_remote_copy(
            src_ref=res.at[k], dst_ref=got.at[k], send_sem=res_send.at[k], recv_sem=res_recv.at[k],
            device_id={"doc": lax.rem(doc + nd - k, nd)}, device_id_type=MESH)
        copy.start()
        returns.append(copy)
    for c in order[-2:]:
        final(0, c)
    best, chosen = reduced(0)
    for k in range(1, nd):
        returns[k - 1].wait()
        best = jnp.maximum(best, got[k, 0:1, :])
        chosen = chosen + got[k, 1:2, :]
    near_out[...] = best * scale_x
    chosen_out[...] = chosen * scale_x
    for copy in sent:
        copy.wait_send()


def layer_kernel(nz, feat, docs_in, cents_in, ids_in, near_out, chosen_out,
                 own, raw, ends, buf, docs, flat, ids, turned, acc, idb, mx, ch, csq, scale, res, got,
                 local_sem, send_sem, c_recv, last_recv, d_recv, i_recv, r_recv):
    width = cents_in.shape[1]
    rows_dev, depth = docs_in.shape
    half = width // 2
    count, extra = half // 128, half % 128
    small = count // 2 * 128
    wide = small + extra
    turn_at = (count + 1) * 128
    full = width // 128 * 128
    rest = width - full
    late = -(-4 * feat // 256) * 256
    k1 = 8 * feat // 256 * 256
    k2 = depth - late - k1
    a = rows_dev * 3 // 8 // 16 * 16
    b = (rows_dev - a) // 32 * 16
    spans = ((0, a), (a, b), (a + b, rows_dev - a - b))
    cuts = {w: (0, 256, (w - 1) // 256 * 256, w) for w in (small, wide)}

    clu, doc = lax.axis_index("clu"), lax.axis_index("doc")
    core, chip = lax.rem(clu, 2), lax.div(clu, 2)
    z, x = lax.div(chip, 2), lax.rem(chip, 2)
    upper = z >= nz // 2
    out = jnp.where(upper, 1, -1)
    end = (z == 0) | (z == nz - 1)
    inner = jnp.logical_not(end)

    def device(r, dz=0):
        dx, dy, dc = r // 4, r // 2 % 2, r % 2
        there = ((z + dz) * 2 + (1 - x if dx else x)) * 2 + (1 - core if dc else core)
        return {"clu": there, "doc": 1 - doc if dy else doc}

    def when(cond, body):
        if cond is None:
            body()
        else:
            pl.when(cond)(body)

    def both(p, q):
        return q if p is None else p if q is None else p & q

    def sized(c, cond, body):
        for value, w in ((1, wide), (0, small)):
            when(both(cond, c == value), functools.partial(body, w))

    own_copy = pltpu.make_async_copy(cents_in.at[:, pl.ds(0, full)], own.at[:, pl.ds(0, full)], local_sem.at[0])
    docs_copy = pltpu.make_async_copy(docs_in, docs.at[0], local_sem.at[1])
    ids_copy = pltpu.make_async_copy(ids_in, ids.at[0], local_sem.at[2])
    own_copy.start()
    raw_copy = pltpu.make_async_copy(cents_in.at[:, pl.ds(full, rest)], raw, local_sem.at[3])
    raw_copy.start()
    end_copies = [pltpu.make_async_copy(cents_in.at[:, pl.ds(k * turn_at + small, small)],
                                        ends.at[k, :, pl.ds(0, small)], local_sem.at[4 + k]) for k in (0, 1)]
    for copy in end_copies:
        copy.start()
    docs_copy.start()
    ids_copy.start()

    barrier = pltpu.get_barrier_semaphore()

    def greet(to):
        pl.semaphore_signal(barrier, inc=1, device_id=to, device_id_type=MESH)

    pl.when(inner)(lambda: greet(device(0, out)))
    greet(device(0, -out))
    for r in (4, 5, 2, 1):
        greet(device(r))

    @pl.when(core == 0)
    def _():
        buf[:, pl.ds(small, extra)] = jnp.zeros((buf.shape[0], extra), buf.dtype)

    own_copy.wait()
    raw_copy.wait()
    middle = own[:, pl.ds(turn_at - 128, 128)]
    ends[0, :, pl.ds(small, extra)] = middle[:, 0:extra]
    ends[1, :, pl.ds(small, extra)] = jnp.concatenate([raw[...], middle[:, extra:128]], axis=1)
    for copy in end_copies:
        copy.wait()
    docs_copy.wait()
    ids_copy.wait()
    pl.semaphore_wait(barrier, 5 + inner.astype(jnp.int32))

    outward, inward, doc_sent, id_sent, result_sent, traded, traded_wide = (send_sem.at[i] for i in range(7))

    def start(make, cond=None):
        when(cond, lambda: make().start())

    def start_sized(make, c, cond=None):
        sized(c, cond, lambda w: make(w).start())

    def remote(src, dst, ss, rs, to):
        return pltpu.make_async_remote_copy(
            src_ref=src, dst_ref=dst, send_sem=ss, recv_sem=rs, device_id=to, device_id_type=MESH)

    near = (0, 1, 4, 5)

    def source(layer, j):
        r = near[j]
        there = (layer * 2 + (1 - x if r // 4 else x)) * 2 + (1 - core if r % 2 else core)
        return pl.ds(pl.multiple_of(there * feat, 16), feat)

    def piece(r, w):
        xd = 1 - x if r // 4 else x
        if w == wide:
            return ends.at[xd]
        return own.at[:, pl.ds(pl.multiple_of(xd * turn_at, 128), w)]

    mine = source(z, 0)

    def exchange(j):
        r = near[j]
        start_sized(lambda w: remote(piece(r, w), buf.at[mine, pl.ds(0, w)],
                                     traded_wide if w == wide else traded, c_recv.at[z, j], device(r)),
                    1 - core if r % 2 else core)

    def landed(layer, j, cond=None):
        rows = source(layer, j)
        sized(core, cond, lambda w: remote(
            buf.at[rows, pl.ds(0, w)], buf.at[rows, pl.ds(0, w)], traded, c_recv.at[layer, j],
            device(1)).wait_recv())

    def carry(layer, j, way, s, cond=None):
        rows = source(layer, j)
        src = (lambda w: piece(0, w)) if s == 0 and j == 0 else (lambda w: buf.at[rows, pl.ds(0, w)])
        start_sized(lambda w: remote(src(w), buf.at[rows, pl.ds(0, w)], inward if way else outward,
                                     c_recv.at[layer, j], device(0, -out if way else out)), core, cond)

    def spread(j):
        if j:
            landed(z, j)
        carry(z, j, 0, 0, inner)
        carry(z, j, 1, 0)

    def relay(j):
        landed(z - out, j)
        carry(z - out, j, 0, 1, inner)
        landed(z + out, j, inner)
        carry(z + out, j, 1, 1, inner)

    def pair(layer, k, w):
        rows = pl.ds(pl.multiple_of((layer * 2 + 1 - x) * 2 * feat, 16), 2 * feat)
        return buf.at[rows, pl.ds(cuts[w][k], cuts[w][k + 1] - cuts[w][k])]

    def relay_far(j):
        landed(z - 2 * out, j)
        if j < 2:
            carry(z - 2 * out, j, 0, 2, inner)

    def send_last(cond):
        for k in range(3):
            start_sized(lambda w, k=k: remote(
                pair(z - 2 * out, k, w), pair(z - 2 * out, k, w), outward, last_recv.at[k],
                device(0, out)), core, inner & cond)

    def last_landed(k):
        sized(core, end, lambda w: remote(
            pair(z - 3 * out, k, w), pair(z - 3 * out, k, w), outward, last_recv.at[k],
            device(1)).wait_recv())

    ahead = {(1, 0): 0, (1, 1): 0, (1, 2): 0, (3, 0): 1, (3, 1): 1, (3, 2): 1, (5, 0): 2, (5, 1): 2, (5, 2): 2,
             (7, 0): 3, (7, 1): 3, (7, 2): 3, (2, 0): 4, (2, 1): 5, (2, 2): 5, (4, 0): 6, (4, 1): 7, (4, 2): 8,
             (6, 0): 9, (6, 1): 10, (6, 2): 11}
    id_at = {1: 0, 3: 0, 5: 0, 7: 0, 2: 1, 4: 2, 6: 3}

    def part(slot, *parts):
        first, last = spans[parts[0]], spans[parts[-1]]
        return docs.at[slot, pl.ds(first[0], last[0] + last[1] - first[0]), :]

    def send_docs(src_slot, dst_slot, r, *parts):
        start(lambda: remote(part(src_slot, *parts), part(dst_slot, *parts), doc_sent,
                             d_recv.at[ahead[dst_slot, parts[0]]], device(r)))

    def send_ids(src_slot, dst_slot, r):
        start(lambda: remote(ids.at[src_slot], ids.at[dst_slot], id_sent, i_recv.at[id_at[dst_slot]], device(r)))

    def have_docs(slot, *parts):
        remote(part(slot, *parts), part(slot, *parts), doc_sent, d_recv.at[ahead[slot, parts[0]]],
               device(1)).wait_recv()

    def have_ids(slot):
        some = ids.at[pl.ds(0, 4)] if slot % 2 else ids.at[slot]
        remote(some, some, id_sent, i_recv.at[id_at[slot]], device(1)).wait_recv()

    def share(slot, *parts):
        send_docs(slot, slot + 1, 1, *parts)

    spread(0)
    for j in (1, 2, 3):
        exchange(j)
    send_ids(0, 2, 2)
    send_docs(0, 2, 2, 0)
    send_docs(0, 2, 2, 1, 2)
    send_ids(0, 1, 1)
    send_docs(0, 1, 1, 0, 1, 2)

    first = x * turn_at + core * small
    reach = small + jnp.where(core == 0, 0, jnp.where(x == 0, extra, rest))
    tail = (core == 1) & (x == 1)
    lines = lax.broadcasted_iota(jnp.int32, (GROUP, rows_dev), 0)

    def prepare_ids(slot):
        local = ids[slot] - doc * width
        rel = jnp.where((local >= first) & (local < first + reach), local - first, -(2**20))
        rel = jnp.where((local >= half) & (local < turn_at) & tail, local - half + small + rest, rel)
        idb[:, pl.ds(slot * rows_dev, rows_dev)] = jnp.broadcast_to(rel, (GROUP, rows_dev)) - lines

    def place(w):
        buf[mine, pl.ds(0, w)] = ends[x] if w == wide else piece(0, w)[...]

    sized(core, None, place)

    k1_at = pl.multiple_of(jnp.where(upper, depth - k1, 0), 256)
    k2_at = pl.multiple_of(jnp.where(upper, late, k1), 256)
    late_at = pl.multiple_of(jnp.where(upper, 0, depth - late), 256)
    starts = (k1_at, k2_at, late_at)

    def squares(i, c, w):
        w32 = buf[pl.ds(starts[i], 256), pl.ds(c, w)].astype(jnp.float32)
        return jnp.sum((w32 * w32).reshape(32, 8, w), 0)

    def turn(i, c, w):
        turned[i, pl.ds(c, w), :] = buf[pl.ds(starts[i], 256), pl.ds(c, w)].T

    def gather(i):
        for c in range(0, wide, 256):
            turn(i, c, min(256, wide - c))
        csq[...] = squares(i, 0, wide) + (csq[...] if i else 0.0)

    def flatten(*slots):
        for slot in slots:
            flat[:, pl.ds(slot * rows_dev, rows_dev)] = docs[slot].T

    def times(i, c, w, slot, count):
        return jnp.dot(turned[i, pl.ds(c, w), :],
                       flat[pl.ds(starts[i], 256), pl.ds(slot * rows_dev, count * rows_dev)],
                       preferred_element_type=jnp.float32)

    def begin(slot, count, *phases):
        where_docs = pl.ds(slot * rows_dev, count * rows_dev)

        def add(w):
            cut_at = w if count > 1 else w // 32 * 16
            for c, h in ((0, cut_at), (cut_at, w - cut_at)):
                if not h:
                    continue
                prod = times(phases[0], c, h, slot, count)
                for i in phases[1:]:
                    prod = prod + times(i, c, h, slot, count)
                if phases[0]:
                    acc[pl.ds(c, h), where_docs] += prod
                else:
                    acc[pl.ds(c, h), where_docs] = prod

        sized(core, None, add)

    def cross_docs():
        send_ids(0, 4, 4)
        for p in (1, 2, 0):
            send_docs(0, 4, 4, p)

    spread(1)
    pl.when(core == 0)(cross_docs)
    prepare_ids(0)
    flatten(0)
    spread(2)
    pl.when(core == 1)(cross_docs)
    relay(0)
    spread(3)
    relay(1)
    have_docs(2, 0)
    send_docs(2, 6, 4, 0)
    share(2, 0)
    have_ids(4)
    send_ids(4, 6, 2)
    send_ids(4, 5, 1)
    have_ids(2)
    send_ids(2, 3, 1)
    relay(2)
    have_docs(4, 1)
    send_docs(4, 6, 2, 1)
    share(4, 1)
    have_docs(1, 0, 1, 2)
    flatten(1)
    relay(3)
    relay_far(0)
    have_docs(4, 2)
    send_docs(4, 6, 2, 2)
    share(4, 2)
    have_docs(2, 1, 2)
    share(2, 1, 2)
    have_ids(6)
    send_ids(6, 7, 1)
    relay_far(1)
    gather(0)
    begin(0, 2, 0)
    flatten(2)
    have_ids(1)
    for slot in (1, 2, 3, 4, 5, 6, 7):
        prepare_ids(slot)
    relay_far(2)
    have_docs(3, 0, 1, 2)
    flatten(3)
    begin(2, 2, 0)
    have_docs(4, 0)
    share(4, 0)
    flatten(4)
    relay_far(3)
    send_last(core == 0)
    gather(1)
    begin(0, 2, 1)
    begin(2, 2, 1)

    def share_far():
        for p in (1, 2, 0):
            have_docs(6, p)
            share(6, p)

    have_docs(5, 0, 1, 2)
    flatten(5)
    pl.when(core == 0)(share_far)
    begin(4, 2, 0, 1)
    send_last(core == 1)
    pl.when(core == 1)(share_far)
    flatten(6)
    begin(6, 1, 0, 1)

    def scales(c, w):
        total = jnp.sum(csq[:, pl.ds(c, w)] + squares(2, c, w), 0, keepdims=True)
        scale[pl.ds(c, w), :] = jnp.broadcast_to(lax.rsqrt(total + epsilon), (128, w)).T

    def stage(c0, w, slot, count):
        prod = times(2, c0, w, slot, count)
        spots = [pl.ds(slot * rows_dev + d, 128) for d in range(0, count * rows_dev, 128)]
        if c0:
            tops, hits = [mx[:, at] for at in spots], [ch[:, at] for at in spots]
        else:
            tops = [jnp.full((GROUP, 128), -3.0e38, jnp.float32)] * len(spots)
            hits = [jnp.zeros((GROUP, 128), jnp.float32)] * len(spots)
        for c in range(0, w, GROUP):
            rows = pl.ds(c0 + c, GROUP)
            by = scale[rows, :]
            for n, at in enumerate(spots):
                v = (acc[rows, at] + prod[c:c + GROUP, n * 128:n * 128 + 128]) * by
                hits[n] = jnp.where(idb[:, at] == c0 + c, v, hits[n])
                tops[n] = jnp.maximum(tops[n], v)
        for n, at in enumerate(spots):
            mx[:, at], ch[:, at] = tops[n], hits[n]

    def reduced(slot):
        at = pl.ds(slot * rows_dev, rows_dev)
        return jnp.max(mx[:, at], 0, keepdims=True), jnp.sum(ch[:, at], 0, keepdims=True)

    def give(slot):
        best, chosen = reduced(slot)
        res[slot, 0:1, :] = best
        res[slot, 1:2, :] = chosen
        remote(res.at[slot], got.at[slot], result_sent, r_recv, device(slot)).start()

    x32 = docs[0].astype(jnp.float32)
    sq = x32 * x32
    total = sq[:, 0:128]
    for c in range(128, depth, 128):
        total = total + sq[:, c:c + 128]
    scale_x = lax.rsqrt(jnp.sum(total.T, 0, keepdims=True) + epsilon)

    landed(z - 3 * out, 0, end)
    landed(z - 3 * out, 1, end)
    have_docs(7, 0, 1, 2)
    flatten(7)
    begin(7, 1, 0, 1)

    def advance(k, have):
        c, w = cuts[have][k], cuts[have][k + 1] - cuts[have][k]
        turn(2, c, w)
        scales(c, w)
        for slot in (6, 2, 4, 0):
            stage(c, w, slot, 2)
            if k == 2:
                give(slot + 1)
                if slot:
                    give(slot)

    for k in range(3):
        last_landed(k)
        sized(core, None, functools.partial(advance, k))
    best, chosen = reduced(0)
    everyone = pl.ds(1, 7)
    remote(got.at[everyone], got.at[everyone], result_sent, r_recv, device(1)).wait_recv()
    for slot in range(1, 8):
        best = jnp.maximum(best, got[slot, 0:1, :])
        chosen = chosen + got[slot, 1:2, :]
    near_out[...] = best * scale_x
    chosen_out[...] = chosen * scale_x

    def sent(ref, sem):
        remote(ref, ref, sem, r_recv, device(1)).wait_send()

    sent(res.at[everyone], result_sent)
    sent(docs.at[everyone], doc_sent)
    sent(ids.at[everyone], id_sent)
    layer = 4 * feat
    sized(core, inner, lambda w: sent(buf.at[pl.ds(0, 3 * layer), pl.ds(0, w)], outward))
    sized(core, inner, lambda w: sent(buf.at[pl.ds(0, 2 * layer), pl.ds(0, w)], inward))
    sized(core, end, lambda w: sent(buf.at[pl.ds(0, layer), pl.ds(0, w)], inward))
    for w, sem, two in ((wide, traded_wide, 0), (small, traded, 1)):
        pl.when(core == two)(lambda: sent(buf.at[pl.ds(0, 2 * feat), pl.ds(0, w)], sem))
        pl.when(core != two)(lambda: sent(buf.at[pl.ds(0, feat), pl.ds(0, w)], sem))


def by_layers(docs, centroids, assigned):
    nz = lax.axis_size("clu") // 4
    rows_dev, depth = docs.shape
    width, feat = centroids.shape
    wide = width // 512 * 128 + width // 2 % 128
    any_space = pl.BlockSpec(memory_space=pl.ANY)
    vmem = pl.BlockSpec(memory_space=pltpu.VMEM)
    dma = pltpu.SemaphoreType.DMA
    line = pltpu.VMEM((1, rows_dev), jnp.float32)
    near, chosen = pl.pallas_call(
        functools.partial(layer_kernel, nz, feat),
        out_shape=(line, line),
        in_specs=[any_space] * 3,
        out_specs=(vmem, vmem),
        scratch_shapes=[
            pltpu.VMEM((feat, width // 128 * 128), jnp.bfloat16),
            pltpu.VMEM((feat, width % 128), jnp.bfloat16),
            pltpu.VMEM((2, feat, wide), jnp.bfloat16),
            pltpu.VMEM((depth, wide), jnp.bfloat16),
            pltpu.VMEM((8, rows_dev, depth), jnp.bfloat16),
            pltpu.VMEM((depth, 8 * rows_dev), jnp.bfloat16),
            pltpu.VMEM((8, 1, rows_dev), jnp.int32),
            pltpu.VMEM((3, wide, 256), jnp.bfloat16),
            pltpu.VMEM((wide, 8 * rows_dev), jnp.float32),
            pltpu.VMEM((GROUP, 8 * rows_dev), jnp.int32),
            pltpu.VMEM((GROUP, 8 * rows_dev), jnp.float32),
            pltpu.VMEM((GROUP, 8 * rows_dev), jnp.float32),
            pltpu.VMEM((8, wide), jnp.float32),
            pltpu.VMEM((wide, 128), jnp.float32),
            pltpu.VMEM((8, 2, rows_dev), jnp.float32),
            pltpu.VMEM((8, 2, rows_dev), jnp.float32),
            dma((6,)), dma((7,)), dma((nz, 4)), dma((3,)), dma((12,)), dma((4,)), dma,
        ],
        compiler_params=pltpu.CompilerParams(collective_id=0, has_side_effects=True),
        name="layer_distances",
    )(docs, centroids.T, assigned.reshape(1, rows_dev))
    return 1.0 - near.reshape(rows_dev), 1.0 - chosen.reshape(rows_dev)


def fits_layers(docs, centroids):
    n_clu, feat = lax.axis_size("clu"), centroids.shape[1]
    width = centroids.shape[0]
    count, extra = width // 2 // 128, width // 2 % 128
    return (lax.axis_size("doc") == 2 and n_clu == 16 and feat % 16 == 0
            and width % 2 == 0 and count % 2 == 0 and count >= 10 and extra > 64 and extra % GROUP == 0
            and docs.shape[0] % 128 == 0 and docs.shape[1] == n_clu * feat == 3 * 256)


def on_device(docs, centroids, assigned):
    if fits_layers(docs, centroids):
        return by_layers(docs, centroids, assigned)
    n_clu, nd = lax.axis_size("clu"), lax.axis_size("doc")
    n = n_clu // 2
    rows_dev, depth = docs.shape
    width, feat = centroids.shape
    fp = (feat + 15) // 16 * 16
    cents = centroids.T
    if fp != feat:
        cents = jnp.pad(cents, ((0, fp - feat), (0, 0)))
    rows = nd * rows_dev
    any_space = pl.BlockSpec(memory_space=pl.ANY)
    vmem = pl.BlockSpec(memory_space=pltpu.VMEM)
    dma = pltpu.SemaphoreType.DMA
    hops = n // 2
    line = jax.ShapeDtypeStruct((1, rows_dev), jnp.float32)
    near, chosen = pl.pallas_call(
        functools.partial(kernel, n, nd, feat),
        out_shape=(line, line),
        in_specs=[any_space] * 3,
        out_specs=(vmem, vmem),
        scratch_shapes=[
            pltpu.VMEM((n_clu * fp, width), jnp.bfloat16),
            pltpu.VMEM((nd, rows_dev, depth), jnp.bfloat16),
            pltpu.VMEM((nd, 1, rows_dev), jnp.int32),
            pltpu.VMEM((rows, (n - 3) * 2 * fp), jnp.bfloat16),
            pltpu.VMEM((rows, 4 * fp), jnp.bfloat16),
            pltpu.VMEM((rows, 2 * fp), jnp.bfloat16),
            pltpu.VMEM((rows, width), jnp.float32),
            pltpu.VMEM((rows, 128), jnp.int32),
            pltpu.VMEM((rows, 128), jnp.float32),
            pltpu.VMEM((rows, 128), jnp.float32),
            pltpu.VMEM((8, width), jnp.float32),
            pltpu.VMEM((1, width), jnp.float32),
            pltpu.VMEM((nd, 2, rows_dev), jnp.float32),
            pltpu.VMEM((nd, 2, rows_dev), jnp.float32),
            dma((3,)),
            dma((2, hops, PIECES)),
            dma((n, PIECES)),
            dma((n, 2, PIECES)),
            dma((nd,)), dma((nd,)), dma((nd,)), dma((nd,)), dma((nd,)), dma((nd,)),
        ],
        compiler_params=pltpu.CompilerParams(collective_id=0, has_side_effects=True),
        name="ring_distances",
    )(docs, cents, assigned.reshape(1, rows_dev))
    return 1.0 - near.reshape(rows_dev), 1.0 - chosen.reshape(rows_dev)


def solution(mesh):
    placed = (P(("clu", "doc"), None), P("doc", "clu"), P(("clu", "doc")))
    return jax.shard_map(
        on_device,
        mesh=mesh,
        in_specs=placed,
        out_specs=(P(("clu", "doc")), P(("clu", "doc"))),
        check_vma=False,
    )
```
